8 devices in a mesh: hp: 4 (over z, y, x), cp: 2 (over core).
Axes of the slice: x: 2, y: 2, z: 1, core: 2. Of those that a mesh axis runs over, the one named last changes fastest.
Arguments:
- hidden: bfloat16 [2048, 2048], P(('cp', 'hp'))
- grad_out: bfloat16 [2048, 2048], P(('cp', 'hp'))
- positions: int32 [2048], P(('cp', 'hp'))
- norm_gain: bfloat16 [2048], replicated
- w_q: bfloat16 [2048, 2048], replicated
- w_k: bfloat16 [2048, 256], replicated
- w_v: bfloat16 [2048, 256], replicated
- w_o: bfloat16 [2048, 2048], replicated
- inv_freq: float32 [32], replicated
Outputs:
- output 1: bfloat16 [2048, 2048], P(('cp', 'hp'))
- output 2: bfloat16 [2048, 2048], P(('cp', 'hp'))
- output 3: float32 [2048, 2048], replicated
- output 4: float32 [2048, 256], replicated
- output 5: float32 [2048, 256], replicated
- output 6: float32 [2048, 2048], replicated
- output 7: float32 [2048], replicated
All inputs are finite; a program needn't handle non-finite values.
Results may differ from the reference program's by a relative error of at most 0.00983856.
Values are sent between devices in bfloat16 or wider.
A program may use at most 1 GiB of HBM per device.

```python
import math
import jax
import jax.numpy as jnp
from jax import lax

D_MODEL = 2048
Q_HEADS = 32
KV_HEADS = 4
HEAD_DIM = 64
TOKENS_DEV = 256
CP_SIZE = 2
HP_SIZE = 4

SEQ_LEN = TOKENS_DEV * CP_SIZE * HP_SIZE
NORM_EPS = 1e-5


def true_index():
    block_len = SEQ_LEN // (2 * CP_SIZE)
    rows_idx = jnp.arange(SEQ_LEN, dtype=jnp.int32)
    pair_id = rows_idx // (2 * block_len)
    within = rows_idx % (2 * block_len)
    return jnp.where(within < block_len, pair_id * block_len + within, (2 * CP_SIZE - 1 - pair_id) * block_len + within - block_len)


def draw_positions(key):
    doc_starts = jax.random.randint(key, (8,), 1, SEQ_LEN)
    seq_idx = jnp.arange(SEQ_LEN, dtype=jnp.int32)
    start_flags = jnp.zeros((SEQ_LEN,), jnp.int32).at[doc_starts].set(1)
    start_marks = jnp.where(start_flags > 0, seq_idx, 0)
    return (seq_idx - lax.cummax(start_marks, axis=0))[true_index()]


def setup_inputs(seed: int = 0) -> dict:
    key_list = jax.random.split(jax.random.key(seed), 10)
    half_dim = HEAD_DIM // 2
    in_scale = D_MODEL ** -0.5
    hidden = jax.random.normal(key_list[0], (SEQ_LEN, D_MODEL), jnp.float32).astype(jnp.bfloat16)
    grad_out = jax.random.normal(key_list[1], (SEQ_LEN, D_MODEL), jnp.float32).astype(jnp.bfloat16)
    positions = draw_positions(key_list[2])
    norm_gain = (1.0 + 0.3 * jax.random.normal(key_list[3], (D_MODEL,), jnp.float32)).astype(jnp.bfloat16)
    w_q = (jax.random.normal(key_list[4], (D_MODEL, Q_HEADS * HEAD_DIM), jnp.float32) * in_scale).astype(jnp.bfloat16)
    w_k = (jax.random.normal(key_list[5], (D_MODEL, KV_HEADS * HEAD_DIM), jnp.float32) * in_scale).astype(jnp.bfloat16)
    w_v = (jax.random.normal(key_list[6], (D_MODEL, KV_HEADS * HEAD_DIM), jnp.float32) * in_scale).astype(jnp.bfloat16)
    w_o = (jax.random.normal(key_list[7], (Q_HEADS * HEAD_DIM, D_MODEL), jnp.float32) * (Q_HEADS * HEAD_DIM) ** -0.5).astype(jnp.bfloat16)
    rope_base = jnp.exp(jax.random.uniform(key_list[8], (), jnp.float32, math.log(1.0e4), math.log(5.0e5)))
    jitter = jax.random.uniform(key_list[9], (half_dim,), jnp.float32, 0.7, 1.3)
    inv_freq = rope_base ** (-jnp.arange(half_dim, dtype=jnp.float32) / half_dim) * jitter
    return dict(hidden=hidden, grad_out=grad_out, positions=positions, norm_gain=norm_gain, w_q=w_q, w_k=w_k, w_v=w_v, w_o=w_o, inv_freq=inv_freq)


def rope_apply(vectors, cos_t, sin_t):
    half_dim = vectors.shape[-1] // 2
    lo_half = vectors[..., :half_dim]
    hi_half = vectors[..., half_dim:]
    return jnp.concatenate([lo_half * cos_t - hi_half * sin_t, hi_half * cos_t + lo_half * sin_t], axis=-1)


def rope_undo(vectors, cos_t, sin_t):
    half_dim = vectors.shape[-1] // 2
    lo_half = vectors[..., :half_dim]
    hi_half = vectors[..., half_dim:]
    return jnp.concatenate([lo_half * cos_t + hi_half * sin_t, hi_half * cos_t - lo_half * sin_t], axis=-1)


def reference(hidden, grad_out, positions, norm_gain, w_q, w_k, w_v, w_o, inv_freq):
    group_size = Q_HEADS // KV_HEADS
    score_scale = HEAD_DIM ** -0.5
    q_block = min(TOKENS_DEV, 64)
    n_blocks = SEQ_LEN // q_block
    x_f32 = hidden.astype(jnp.float32)
    inv_rms = lax.rsqrt(jnp.mean(x_f32 * x_f32, axis=-1, keepdims=True) + NORM_EPS)
    x_hat = x_f32 * inv_rms
    normed = (x_hat * norm_gain.astype(jnp.float32)).astype(jnp.bfloat16)
    angles = positions.astype(jnp.float32)[:, None] * inv_freq[None, :]
    cos_t = jnp.cos(angles)[:, None, :]
    sin_t = jnp.sin(angles)[:, None, :]
    q_rot = rope_apply(jnp.dot(normed, w_q, preferred_element_type=jnp.float32).reshape(SEQ_LEN, Q_HEADS, HEAD_DIM), cos_t, sin_t).astype(jnp.bfloat16)
    k_rot = rope_apply(jnp.dot(normed, w_k, preferred_element_type=jnp.float32).reshape(SEQ_LEN, KV_HEADS, HEAD_DIM), cos_t, sin_t).astype(jnp.bfloat16)
    v_val = jnp.dot(normed, w_v, preferred_element_type=jnp.float32).astype(jnp.bfloat16).reshape(SEQ_LEN, KV_HEADS, HEAD_DIM)
    d_out = jnp.dot(grad_out, w_o.T, preferred_element_type=jnp.float32).astype(jnp.bfloat16)
    seq_idx = true_index()
    k_f32 = k_rot.astype(jnp.float32)
    v_f32 = v_val.astype(jnp.float32)
    q_blocks = q_rot.reshape(n_blocks, q_block, KV_HEADS, group_size, HEAD_DIM)
    do_blocks = d_out.reshape(n_blocks, q_block, KV_HEADS, group_size, HEAD_DIM)
    idx_blocks = seq_idx.reshape(n_blocks, q_block)

    def block_step(acc_pair, block_in):
        dk_acc, dv_acc = acc_pair
        q_part, do_part, idx_part = block_in
        q_f32 = q_part.astype(jnp.float32)
        do_f32 = do_part.astype(jnp.float32)
        scores = jnp.einsum('qkgd,tkd->kgqt', q_f32, k_f32) * score_scale
        visible = idx_part[:, None] >= seq_idx[None, :]
        scores = jnp.where(visible, scores, -1e30)
        prob_f32 = jnp.exp(scores - jnp.max(scores, axis=-1, keepdims=True))
        prob_f32 = prob_f32 / jnp.sum(prob_f32, axis=-1, keepdims=True)
        prob_b16 = prob_f32.astype(jnp.bfloat16).astype(jnp.float32)
        out_part = jnp.einsum('kgqt,tkd->qkgd', prob_b16, v_f32).astype(jnp.bfloat16)
        row_delta = jnp.einsum('qkgd,qkgd->kgq', do_f32, out_part.astype(jnp.float32))
        d_prob = jnp.einsum('qkgd,tkd->kgqt', do_f32, v_f32)
        d_score = (prob_f32 * (d_prob - row_delta[..., None])).astype(jnp.bfloat16).astype(jnp.float32)
        dq_part = (jnp.einsum('kgqt,tkd->qkgd', d_score, k_f32) * score_scale).astype(jnp.bfloat16)
        dk_acc = dk_acc + jnp.einsum('kgqt,qkgd->tkd', d_score, q_f32) * score_scale
        dv_acc = dv_acc + jnp.einsum('kgqt,qkgd->tkd', prob_b16, do_f32)
        return (dk_acc, dv_acc), (out_part, dq_part)

    zeros_kv = jnp.zeros((SEQ_LEN, KV_HEADS, HEAD_DIM), jnp.float32)
    (dk_sum, dv_sum), (out_blocks, dq_blocks) = lax.scan(block_step, (zeros_kv, zeros_kv), (q_blocks, do_blocks, idx_blocks))
    attn_out = out_blocks.reshape(SEQ_LEN, Q_HEADS * HEAD_DIM)
    output = (x_f32 + jnp.dot(attn_out, w_o, preferred_element_type=jnp.float32)).astype(jnp.bfloat16)
    grad_wo = jnp.dot(attn_out.T, grad_out, preferred_element_type=jnp.float32)
    g_q = rope_undo(dq_blocks.reshape(SEQ_LEN, Q_HEADS, HEAD_DIM).astype(jnp.float32), cos_t, sin_t).astype(jnp.bfloat16).reshape(SEQ_LEN, Q_HEADS * HEAD_DIM)
    g_k = rope_undo(dk_sum.astype(jnp.bfloat16).astype(jnp.float32), cos_t, sin_t).astype(jnp.bfloat16).reshape(SEQ_LEN, KV_HEADS * HEAD_DIM)
    g_v = dv_sum.astype(jnp.bfloat16).reshape(SEQ_LEN, KV_HEADS * HEAD_DIM)
    grad_wq = jnp.dot(normed.T, g_q, preferred_element_type=jnp.float32)
    grad_wk = jnp.dot(normed.T, g_k, preferred_element_type=jnp.float32)
    grad_wv = jnp.dot(normed.T, g_v, preferred_element_type=jnp.float32)
    d_norm = jnp.dot(g_q, w_q.T, preferred_element_type=jnp.float32) + jnp.dot(g_k, w_k.T, preferred_element_type=jnp.float32) + jnp.dot(g_v, w_v.T, preferred_element_type=jnp.float32)
    grad_gain = jnp.sum(d_norm * x_hat, axis=0)
    d_hat = d_norm * norm_gain.astype(jnp.float32)
    grad_hidden = (grad_out.astype(jnp.float32) + inv_rms * (d_hat - x_hat * jnp.mean(d_hat * x_hat, axis=-1, keepdims=True))).astype(jnp.bfloat16)
    return (output, grad_hidden, grad_wq, grad_wk, grad_wv, grad_wo, grad_gain)
```

```python
import functools
import math

import jax
import jax.numpy as jnp
from jax import lax
from jax.experimental import pallas as pl
from jax.experimental.pallas import tpu as pltpu
from jax.sharding import PartitionSpec as P

NORM_EPS = 1e-5
BLK = 256
HEADS = 4
DH = 64
NB = 8
CW = HEADS * BLK
EXP2_SCALE = (DH ** -0.5) * math.log2(math.e)
F32 = jnp.float32
BF16 = jnp.bfloat16


def seq_block(d):
    cp, half, sub = d // 4, (d // 2) % 2, d % 2
    return 2 * ((1 - half) * cp + half * (3 - cp)) + sub


def stored_block(j):
    b, sub = j // 2, j % 2
    half = b // 2
    cp = (1 - half) * b + half * (3 - b)
    return cp * 4 + half * 2 + sub


def nt_dot(a, b):
    return lax.dot_general(a, b, (((1,), (1,)), ((), ())), preferred_element_type=F32)


def dot(a, b):
    return jnp.dot(a, b, preferred_element_type=F32)


def rope_pairs(t, cos_t, sin_t):
    lane = lax.broadcasted_iota(jnp.int32, t.shape, 1)
    partner = jnp.where(lane % DH < DH // 2, pltpu.roll(t, 128 - DH // 2, 1), pltpu.roll(t, DH // 2, 1))
    return t * cos_t + partner * sin_t


def rows_of(b):
    return pl.ds(pl.multiple_of(b * BLK, BLK), BLK)


def causal_tile():
    row = lax.broadcasted_iota(jnp.int32, (BLK, CW), 0)
    col = lax.broadcasted_iota(jnp.int32, (BLK, CW), 1)
    return row <= col % BLK


def project_block(d, x, gain, w_ref, cos_ref, sin_ref, ht_ref, q_ref, k_ref, v_ref):
    xf = x.astype(F32)
    inv = lax.rsqrt(jnp.mean(xf * xf, axis=-1, keepdims=True) + NORM_EPS)
    h = (xf * inv * gain).astype(BF16)
    ht_ref[:, rows_of(d)] = h.T
    y = dot(h, w_ref[...])
    dst = rows_of(seq_block(d))
    cos_t, sin_t = cos_ref[rows_of(d), :], sin_ref[rows_of(d), :]
    for p in range(HEADS // 2):
        qr = rope_pairs(y[:, 128 * p:128 * (p + 1)], cos_t, sin_t).astype(BF16)
        q_ref[2 * p, dst, :] = qr[:, :DH]
        q_ref[2 * p + 1, dst, :] = qr[:, DH:]
    kv = y[:, 128 * (HEADS // 2):]
    k_ref[dst, :] = rope_pairs(kv, cos_t, sin_t).astype(BF16)[:, :DH]
    v_ref[dst, :] = kv.astype(BF16)[:, DH:]


def attend_block(j, q_ref, k_ref, vt_ref, e_ref, m_ref, ot_ref, lse_ref):
    q4 = q_ref[:, rows_of(j), :].reshape(CW, DH)

    def score_tile(kb, carry, masked):
        m_old, l_old = carry
        s = nt_dot(k_ref[rows_of(kb), :], q4) * EXP2_SCALE
        if masked:
            s = jnp.where(causal_tile(), s, -1e30)
        m_new = jnp.maximum(m_old, jnp.max(s, axis=0, keepdims=True))
        e = jnp.exp2(s - m_new)
        e_ref[rows_of(kb), :] = e
        m_ref[pl.ds(kb, 1), :] = m_new
        return m_new, l_old * jnp.exp2(m_old - m_new) + jnp.sum(e, axis=0, keepdims=True)

    carry = (jnp.full((1, CW), -1e30, F32), jnp.zeros((1, CW), F32))
    carry = score_tile(j, carry, True)
    m_fin, l_fin = lax.fori_loop(0, j, functools.partial(score_tile, masked=False), carry)
    inv_l = 1.0 / l_fin
    lse = m_fin + jnp.log2(l_fin)

    def out_tile(kb, acc):
        f = jnp.exp2(m_ref[pl.ds(kb, 1), :] - m_fin) * inv_l
        p = (e_ref[rows_of(kb), :] * f).astype(BF16)
        return acc + dot(vt_ref[:, rows_of(kb)], p)

    acc = lax.fori_loop(0, j + 1, out_tile, jnp.zeros((DH, CW), F32)).astype(BF16)
    dst = rows_of(stored_block(j))
    for h in range(HEADS):
        ot_ref[DH * h:DH * (h + 1), dst] = acc[:, BLK * h:BLK * (h + 1)]
        lse_ref[h:h + 1, rows_of(j)] = lse[:, BLK * h:BLK * (h + 1)]


def forward_kernel(x_ref, gain_ref, w_ref, cos_ref, sin_ref, ht_ref, q_ref, k_ref, v_ref, ot_ref, lse_ref, e_ref, m_ref, vt_ref):
    def project(d, _):
        project_block(d, x_ref[rows_of(d), :], gain_ref[...], w_ref, cos_ref, sin_ref, ht_ref, q_ref, k_ref, v_ref)
        return 0

    lax.fori_loop(0, NB, project, 0)
    vt_ref[...] = v_ref[...].T

    def attend(j, _):
        attend_block(j, q_ref, k_ref, vt_ref, e_ref, m_ref, ot_ref, lse_ref)
        return 0

    lax.fori_loop(0, NB, attend, 0)


def backward_kernel(dy_ref, wo_ref, q_ref, k_ref, v_ref, ot_ref, lse_ref, cos_ref, sin_ref, gq_ref, dk_ref, dv_ref, do_ref, kt_ref):
    def project(d, _):
        do = nt_dot(dy_ref[rows_of(d), :], wo_ref[...]).astype(BF16)
        dst = rows_of(seq_block(d))
        for h in range(HEADS):
            do_ref[h, dst, :] = do[:, DH * h:DH * (h + 1)]
        return 0

    lax.fori_loop(0, NB, project, 0)
    kt_ref[...] = k_ref[...].T
    dk_ref[...] = jnp.zeros_like(dk_ref)
    dv_ref[...] = jnp.zeros_like(dv_ref)

    def attend(j, _):
        src = rows_of(stored_block(j))
        q4 = q_ref[:, rows_of(j), :].reshape(CW, DH)
        do4 = do_ref[:, rows_of(j), :].reshape(CW, DH)
        o4t = jnp.concatenate([ot_ref[DH * h:DH * (h + 1), src] for h in range(HEADS)], axis=1)
        lse = jnp.concatenate([lse_ref[h:h + 1, rows_of(j)] for h in range(HEADS)], axis=1)
        delta = jnp.sum(do4.astype(F32).T * o4t.astype(F32), axis=0, keepdims=True)

        def tile(kb, dqt, masked):
            keys = rows_of(kb)
            p = jnp.exp2(nt_dot(k_ref[keys, :], q4) * EXP2_SCALE - lse)
            if masked:
                p = jnp.where(causal_tile(), p, 0.0)
            dp = nt_dot(v_ref[keys, :], do4)
            dv_ref[keys, :] += dot(p.astype(BF16), do4)
            ds = (p * (dp - delta)).astype(BF16)
            dk_ref[keys, :] += dot(ds, q4)
            return dqt + dot(kt_ref[:, keys], ds)

        dqt = tile(j, jnp.zeros((DH, CW), F32), True)
        dqt = lax.fori_loop(0, j, functools.partial(tile, masked=False), dqt) * (DH ** -0.5)
        cos_t, sin_t = cos_ref[src, :], sin_ref[src, :]
        for p in range(HEADS // 2):
            pair = jnp.concatenate([dqt[:, BLK * (2 * p):BLK * (2 * p + 1)], dqt[:, BLK * (2 * p + 1):BLK * (2 * p + 2)]], axis=0)
            dq = pair.T.astype(BF16).astype(F32)
            gq_ref[src, 128 * p:128 * (p + 1)] = rope_pairs(dq, cos_t, -sin_t).astype(BF16)
        return 0

    lax.fori_loop(0, NB, attend, 0)


VMEM_SPEC = pl.BlockSpec(memory_space=pltpu.VMEM)


def run_forward(x_all, gain, w_qkv, cos_t, sin_t):
    toks, width = x_all.shape
    return pl.pallas_call(
        forward_kernel,
        out_shape=(
            jax.ShapeDtypeStruct((width, toks), BF16),
            jax.ShapeDtypeStruct((HEADS, toks, DH), BF16),
            jax.ShapeDtypeStruct((toks, DH), BF16),
            jax.ShapeDtypeStruct((toks, DH), BF16),
            jax.ShapeDtypeStruct((HEADS * DH, toks), BF16),
            jax.ShapeDtypeStruct((HEADS, toks), F32),
        ),
        in_specs=[VMEM_SPEC] * 5,
        out_specs=(VMEM_SPEC,) * 6,
        scratch_shapes=[pltpu.VMEM((toks, CW), F32), pltpu.VMEM((NB, CW), F32), pltpu.VMEM((DH, toks), BF16)],
        compiler_params=pltpu.CompilerParams(vmem_limit_bytes=60 * 1024 * 1024),
        cost_estimate=pl.CostEstimate(flops=30_000_000_000, bytes_accessed=20_000_000, transcendentals=0),
        name="attn_forward",
    )(x_all, gain, w_qkv, cos_t, sin_t)


def run_backward(dy_all, w_o, q, k, v, o_t, lse, cos_t, sin_t):
    toks = dy_all.shape[0]
    return pl.pallas_call(
        backward_kernel,
        out_shape=(
            jax.ShapeDtypeStruct((toks, HEADS * DH), BF16),
            jax.ShapeDtypeStruct((toks, DH), F32),
            jax.ShapeDtypeStruct((toks, DH), F32),
        ),
        in_specs=[VMEM_SPEC] * 9,
        out_specs=(VMEM_SPEC,) * 3,
        scratch_shapes=[pltpu.VMEM((HEADS, toks, DH), BF16), pltpu.VMEM((DH, toks), BF16)],
        compiler_params=pltpu.CompilerParams(vmem_limit_bytes=60 * 1024 * 1024),
        cost_estimate=pl.CostEstimate(flops=40_000_000_000, bytes_accessed=20_000_000, transcendentals=0),
        name="attn_backward",
    )(dy_all, w_o, q, k, v, o_t, lse, cos_t, sin_t)


def seq_to_stored(a):
    return jnp.concatenate([a[0:512], a[1536:2048], a[512:1536]], axis=0)


def rope_undo(vectors, cos_t, sin_t):
    half_dim = vectors.shape[-1] // 2
    lo_half = vectors[..., :half_dim]
    hi_half = vectors[..., half_dim:]
    return jnp.concatenate([lo_half * cos_t + hi_half * sin_t, hi_half * cos_t - lo_half * sin_t], axis=-1)


def solution(mesh):
    def device_step(hidden, grad_out, positions, norm_gain, w_q, w_k, w_v, w_o, inv_freq):
        rows = hidden.shape[0]
        hp, cp = lax.axis_index('hp'), lax.axis_index('cp')
        me_tok, me_head = cp * 4 + hp, hp * 2 + cp
        x_all = lax.all_gather(hidden, ('cp', 'hp'), axis=0, tiled=True)
        dy_all = lax.all_gather(grad_out, ('cp', 'hp'), axis=0, tiled=True)
        pos_all = lax.all_gather(positions, ('cp', 'hp'), axis=0, tiled=True)
        angles = pos_all.astype(F32)[:, None] * inv_freq[None, :]
        cos_h, sin_h = jnp.cos(angles), jnp.sin(angles)
        cos_t = jnp.concatenate([cos_h] * 4, axis=1)
        sin_t = jnp.concatenate([-sin_h, sin_h] * 2, axis=1)
        gain = norm_gain.astype(F32)[None, :]
        hw = HEADS * DH
        w_qkv = jnp.concatenate([
            lax.dynamic_slice_in_dim(w_q, me_head * hw, hw, 1),
            lax.dynamic_slice_in_dim(w_k, hp * DH, DH, 1),
            lax.dynamic_slice_in_dim(w_v, hp * DH, DH, 1)], axis=1)
        wo_my = lax.dynamic_slice_in_dim(w_o, me_head * hw, hw, 0)
        h_t, q, k, v, o_t, lse = run_forward(x_all, gain, w_qkv, cos_t, sin_t)
        ot_all = lax.all_gather(o_t, ('hp', 'cp'), axis=0, tiled=True)
        g_q, dk_part, dv_part = run_backward(dy_all, wo_my, q, k, v, o_t, lse, cos_t, sin_t)
        gq_all = lax.all_gather(g_q, ('hp', 'cp'), axis=0)
        part = seq_to_stored(jnp.concatenate([dk_part * (DH ** -0.5), dv_part], axis=1)).astype(BF16)
        pair = lax.all_gather(part, 'cp', axis=0).astype(F32)
        dkv = (pair[0] + pair[1]).astype(BF16)
        g_k = rope_undo(dkv[:, :DH].astype(F32), cos_h, sin_h).astype(BF16)
        gkv_all = lax.all_gather(jnp.concatenate([g_k, dkv[:, DH:]], axis=1), 'hp', axis=0)
        x_f32 = hidden.astype(F32)
        inv_rms = lax.rsqrt(jnp.mean(x_f32 * x_f32, axis=-1, keepdims=True) + NORM_EPS)
        x_hat = x_f32 * inv_rms
        o_mine = lax.dynamic_slice_in_dim(ot_all, me_tok * rows, rows, 1)
        output = (x_f32 + jnp.einsum('at,ab->tb', o_mine, w_o, preferred_element_type=F32)).astype(BF16)
        grad_wo = jnp.dot(ot_all, dy_all, preferred_element_type=F32)
        gq_cols = gq_all.transpose(1, 0, 2).reshape(NB * rows, NB * hw)
        gk_cols = gkv_all[:, :, :DH].transpose(1, 0, 2).reshape(NB * rows, 4 * DH)
        gv_cols = gkv_all[:, :, DH:].transpose(1, 0, 2).reshape(NB * rows, 4 * DH)
        grad_wq = jnp.dot(h_t, gq_cols, preferred_element_type=F32)
        grad_wk = jnp.dot(h_t, gk_cols, preferred_element_type=F32)
        grad_wv = jnp.dot(h_t, gv_cols, preferred_element_type=F32)
        mine = lambda a: lax.dynamic_slice_in_dim(a, me_tok * rows, rows, 0)
        d_norm = (jnp.einsum('tb,ab->ta', mine(gq_cols), w_q, preferred_element_type=F32)
                  + jnp.einsum('tb,ab->ta', mine(gk_cols), w_k, preferred_element_type=F32)
                  + jnp.einsum('tb,ab->ta', mine(gv_cols), w_v, preferred_element_type=F32))
        gain_part = jnp.sum(d_norm * x_hat, axis=0, keepdims=True)
        grad_gain = jnp.sum(lax.all_gather(gain_part, ('cp', 'hp'), axis=0, tiled=True), axis=0)
        d_hat = d_norm * gain
        grad_hidden = (grad_out.astype(F32) + inv_rms * (d_hat - x_hat * jnp.mean(d_hat * x_hat, axis=-1, keepdims=True))).astype(BF16)
        return output, grad_hidden, grad_wq, grad_wk, grad_wv, grad_wo, grad_gain

    seq_spec = P(('cp', 'hp'), None)
    whole = P()
    return jax.shard_map(device_step, mesh=mesh, in_specs=(seq_spec, seq_spec, P(('cp', 'hp')), whole, whole, whole, whole, whole, whole), out_specs=(seq_spec, seq_spec, whole, whole, whole, whole, whole), check_vma=False)
```

```python
import functools
import math

import jax
import jax.numpy as jnp
from jax import lax
from jax.experimental import pallas as pl
from jax.experimental.pallas import tpu as pltpu
from jax.sharding import PartitionSpec as P

NORM_EPS = 1e-5
BLK = 256
HEADS = 4
DH = 64
NB = 8
CW = HEADS * BLK
EXP2_SCALE = (DH ** -0.5) * math.log2(math.e)
F32 = jnp.float32
BF16 = jnp.bfloat16


def seq_block(d):
    cp, half, sub = d // 4, (d // 2) % 2, d % 2
    return 2 * ((1 - half) * cp + half * (3 - cp)) + sub


def stored_block(j):
    b, sub = j // 2, j % 2
    half = b // 2
    cp = (1 - half) * b + half * (3 - b)
    return cp * 4 + half * 2 + sub


def nt_dot(a, b):
    return lax.dot_general(a, b, (((1,), (1,)), ((), ())), preferred_element_type=F32)


def dot(a, b):
    return jnp.dot(a, b, preferred_element_type=F32)


def rope_pairs(t, cos_t, sin_t):
    lane = lax.broadcasted_iota(jnp.int32, t.shape, 1)
    partner = jnp.where(lane % DH < DH // 2, pltpu.roll(t, 128 - DH // 2, 1), pltpu.roll(t, DH // 2, 1))
    return t * cos_t + partner * sin_t


def rows_of(b):
    return pl.ds(pl.multiple_of(b * BLK, BLK), BLK)


def causal_tile():
    row = lax.broadcasted_iota(jnp.int32, (BLK, CW), 0)
    col = lax.broadcasted_iota(jnp.int32, (BLK, CW), 1)
    return row <= col % BLK


MESH = pl.DeviceIdType.MESH
CHUNKS = 4


def neighbours():
    hp, cp = lax.axis_index('hp'), lax.axis_index('cp')
    flip = 1 - 2 * (hp % 2)
    y_hp = (hp + 2) % 4
    return hp, cp, hp + flip, y_hp, y_hp + flip


def tok_slot(hp, cp):
    return cp * 4 + hp


def head_slot(hp, cp):
    return hp * 2 + cp


def enter_barrier():
    hp, cp = lax.axis_index('hp'), lax.axis_index('cp')
    barrier = pltpu.get_barrier_semaphore()
    for m in range(1, 8):
        pl.semaphore_signal(barrier, inc=1, device_id=((hp + m // 2) % 4, (cp + m % 2) % 2), device_id_type=MESH)
    pl.semaphore_wait(barrier, 7)


class Gather:
    def __init__(self, src, dst, slot, send, recv, rows):
        self.src, self.dst, self.slot, self.send, self.recv = src, dst, slot, send, recv
        self.step = rows // CHUNKS
        self.hp, self.cp, self.xn, self.yn, self.dn = neighbours()

    def part(self, ref, c):
        return ref.at[pl.ds(c * self.step, self.step)]

    def place(self, hp, cp, c):
        return self.part(self.dst.at[self.slot(hp, cp)], c)

    def copy(self, kind, c):
        hp, cp, xn, yn, dn = self.hp, self.cp, self.xn, self.yn, self.dn
        origin, lands, to = {
            'own_x': (hp, 0, (xn, cp)), 'own_y': (hp, 1, (yn, cp)), 'own_s': (hp, 3, (hp, 1 - cp)),
            'x_s': (xn, 4, (hp, 1 - cp)), 'y_s': (yn, 5, (hp, 1 - cp)), 'd_s': (dn, 6, (hp, 1 - cp)),
            'x_y': (xn, 2, (yn, cp)), 'y_x': (yn, 2, (xn, cp)),
        }[kind]
        number = ('own_x', 'own_y', 'own_s', 'x_s', 'y_s', 'd_s', 'x_y', 'y_x').index(kind)
        src = self.part(self.src, c) if kind.startswith('own') else self.place(origin, cp, c)
        return pltpu.make_async_remote_copy(
            src_ref=src, dst_ref=self.place(origin, cp, c), send_sem=self.send.at[number, c],
            recv_sem=self.recv.at[lands, c], device_id=to, device_id_type=MESH)

    def await_from(self, number, c):
        hp, cp = ((self.xn, self.cp), (self.yn, self.cp), (self.dn, self.cp), (self.hp, 1 - self.cp),
                  (self.xn, 1 - self.cp), (self.yn, 1 - self.cp), (self.dn, 1 - self.cp))[number]
        ref = self.place(hp, cp, c)
        pltpu.make_async_remote_copy(
            src_ref=ref, dst_ref=ref, send_sem=self.send.at[0, c], recv_sem=self.recv.at[number, c],
            device_id=(self.hp, 1 - self.cp), device_id_type=MESH).wait_recv()

    def start_own(self):
        for c in range(CHUNKS):
            for kind in ('own_x', 'own_y', 'own_s'):
                self.copy(kind, c).start()

    def relay_near(self, chunks=range(CHUNKS)):
        for c in chunks:
            self.await_from(0, c)
            self.copy('x_s', c).start()
            if c < CHUNKS // 2:
                self.copy('x_y', c).start()
            self.await_from(1, c)
            self.copy('y_s', c).start()
            if c >= CHUNKS // 2:
                self.copy('y_x', c).start()

    def relay_diagonal(self):
        for c in range(CHUNKS):
            self.await_from(2, c)
            self.copy('d_s', c).start()

    def await_sibling(self, number):
        for c in range(CHUNKS):
            self.await_from(number, c)

    def finish_sends(self):
        for c in range(CHUNKS):
            for kind in ('own_x', 'own_y', 'own_s', 'x_s', 'y_s', 'd_s'):
                self.copy(kind, c).wait_send()
            self.copy('x_y' if c < CHUNKS // 2 else 'y_x', c).wait_send()


def gather_sems():
    return [pltpu.SemaphoreType.DMA((8, CHUNKS)), pltpu.SemaphoreType.DMA((7, CHUNKS))]


def unpack_table(tab):
    group = lax.broadcasted_iota(jnp.int32, tab.shape, 1) // (DH // 2)
    turned = [tab] + [pltpu.roll(tab, 32 * i, 1) for i in (1, 2, 3)]

    def pick(order):
        out = turned[order[3]]
        for g in range(3):
            out = jnp.where(group == g, turned[order[g]], out)
        return out

    sign = jnp.where(group % 2 == 0, -1.0, 1.0)
    cos_t = jnp.concatenate([pick((0, 1, 2, 3)), pick((2, 3, 0, 1))], axis=0)
    sin_t = jnp.concatenate([pick((3, 0, 1, 2)) * sign, pick((1, 2, 3, 0)) * sign], axis=0)
    return cos_t, sin_t


def project_block(d, x, gain, wq_ref, wkv_ref, tab, ht_ref, q_ref, k_ref, v_ref):
    xf = x.astype(F32)
    inv = lax.rsqrt(jnp.mean(xf * xf, axis=-1, keepdims=True) + NORM_EPS)
    h = (xf * inv * gain).astype(BF16)
    ht_ref[:, rows_of(d)] = h.T
    dst = rows_of(seq_block(d))
    cos_t, sin_t = unpack_table(tab)
    y = dot(h, wq_ref[...])
    for p in range(HEADS // 2):
        qr = rope_pairs(y[:, 128 * p:128 * (p + 1)], cos_t, sin_t).astype(BF16)
        q_ref[2 * p, dst, :] = qr[:, :DH]
        q_ref[2 * p + 1, dst, :] = qr[:, DH:]
    kv = dot(h, wkv_ref[...])
    k_ref[dst, :] = rope_pairs(kv, cos_t, sin_t).astype(BF16)[:, :DH]
    v_ref[dst, :] = kv.astype(BF16)[:, DH:]


def attend_block(j, q_ref, k_ref, vt_ref, e_ref, m_ref, ot_ref, lse_ref):
    q4 = q_ref[:, rows_of(j), :].reshape(CW, DH)

    def score_tile(kb, carry, masked):
        m_old, l_old = carry
        s = nt_dot(k_ref[rows_of(kb), :], q4) * EXP2_SCALE
        if masked:
            s = jnp.where(causal_tile(), s, -1e30)
        m_new = jnp.maximum(m_old, jnp.max(s, axis=0, keepdims=True))
        e = jnp.exp2(s - m_new)
        e_ref[rows_of(kb), :] = e
        m_ref[pl.ds(kb, 1), :] = m_new
        return m_new, l_old * jnp.exp2(m_old - m_new) + jnp.sum(e, axis=0, keepdims=True)

    carry = (jnp.full((1, CW), -1e30, F32), jnp.zeros((1, CW), F32))
    carry = score_tile(j, carry, True)
    m_fin, l_fin = lax.fori_loop(0, j, functools.partial(score_tile, masked=False), carry)
    inv_l = 1.0 / l_fin
    lse = m_fin + jnp.log2(l_fin)

    def out_tile(kb, acc):
        f = jnp.exp2(m_ref[pl.ds(kb, 1), :] - m_fin) * inv_l
        p = (e_ref[rows_of(kb), :] * f).astype(BF16)
        return acc + dot(vt_ref[:, rows_of(kb)], p)

    acc = lax.fori_loop(0, j + 1, out_tile, jnp.zeros((DH, CW), F32)).astype(BF16)
    dst = rows_of(stored_block(j))
    for h in range(HEADS):
        ot_ref[DH * h:DH * (h + 1), dst] = acc[:, BLK * h:BLK * (h + 1)]
        lse_ref[h:h + 1, rows_of(j)] = lse[:, BLK * h:BLK * (h + 1)]


def forward_kernel(x_own, dy_own, gain_ref, wq_hbm, wk_hbm, wv_hbm, tab_own,
                   dy_all, ht_out, q_ref, k_ref, v_ref, ot_ref, lse_ref, tabs,
                   xg, ht, e_ref, m_ref, vt_ref, wq, wk, wv, wkv, stage,
                   local_sem, tab_send, tab_recv, x_send, x_recv, dy_send, dy_recv):
    hp, cp, xn, yn, dn = neighbours()
    mine = tok_slot(hp, cp)
    hw = HEADS * DH
    loads = [
        pltpu.make_async_copy(x_own, xg.at[mine], local_sem.at[0]),
        pltpu.make_async_copy(wq_hbm.at[:, pl.ds(pl.multiple_of(head_slot(hp, cp) * hw, hw), hw)], wq, local_sem.at[1]),
        pltpu.make_async_copy(wk_hbm.at[:, pl.ds(pl.multiple_of((hp // 2) * 128, 128), 128)], wk, local_sem.at[2]),
        pltpu.make_async_copy(wv_hbm.at[:, pl.ds(pl.multiple_of((hp // 2) * 128, 128), 128)], wv, local_sem.at[3]),
        pltpu.make_async_copy(dy_own, stage, local_sem.at[4]),
        pltpu.make_async_copy(tab_own, tabs.at[mine], local_sem.at[5]),
    ]
    for load in loads:
        load.start()
    enter_barrier()
    gx = Gather(x_own, xg, tok_slot, x_send, x_recv, BLK)
    gdy = Gather(dy_own, dy_all, tok_slot, dy_send, dy_recv, BLK)

    def table_copy(m):
        to = ((hp + m // 2) % 4, (cp + m % 2) % 2)
        return pltpu.make_async_remote_copy(
            src_ref=tab_own, dst_ref=tabs.at[mine], send_sem=tab_send.at[m - 1], recv_sem=tab_recv.at[m - 1],
            device_id=to, device_id_type=MESH)

    for m in range(1, NB):
        table_copy(m).start()
    gx.start_own()
    for load in loads[1:4]:
        load.wait()
    lane = lax.broadcasted_iota(jnp.int32, wk.shape, 1)
    swap = hp % 2 == 1
    kf, vf = wk[...].astype(F32), wv[...].astype(F32)
    k_sel = jnp.where(swap, pltpu.roll(kf, DH, 1), kf)
    v_sel = jnp.where(swap, vf, pltpu.roll(vf, DH, 1))
    wkv[...] = jnp.where(lane < DH, k_sel, v_sel).astype(BF16)
    for i in (0, 4, 5):
        loads[i].wait()
    dy_mine = pltpu.make_async_copy(stage, dy_all.at[mine], local_sem.at[6])
    dy_mine.start()
    for m in range(1, NB):
        src_slot = tok_slot((hp + 4 - m // 2) % 4, (cp + m % 2) % 2)
        ref = tabs.at[src_slot]
        pltpu.make_async_remote_copy(
            src_ref=ref, dst_ref=ref, send_sem=tab_send.at[m - 1], recv_sem=tab_recv.at[m - 1],
            device_id=(hp, 1 - cp), device_id_type=MESH).wait_recv()

    def project(e, _):
        @pl.when(e == 1)
        def _():
            gx.await_sibling(3)

        @pl.when(e == 2)
        def _():
            gx.relay_near()
            gdy.start_own()

        @pl.when(e == 3)
        def _():
            gx.await_sibling(4)

        @pl.when(e == 5)
        def _():
            gx.await_sibling(5)

        @pl.when(e == 6)
        def _():
            gx.relay_diagonal()

        @pl.when(e == 7)
        def _():
            gx.await_sibling(6)

        m, b = e // 2, e % 2
        px = (hp % 2 + m % 2) % 2
        py = (hp // 2 + m // 2) % 2
        d = tok_slot(py * 2 + px, (cp + b) % 2)
        project_block(d, xg[d], gain_ref[...], wq, wkv, tabs[d], ht, q_ref, k_ref, v_ref)
        return 0

    lax.fori_loop(0, NB, project, 0)
    ht_copy = pltpu.make_async_copy(ht, ht_out, local_sem.at[7])
    ht_copy.start()
    vt_ref[...] = v_ref[...].T

    def attend(j, _):
        @pl.when(j == 5)
        def _():
            gdy.relay_near(range(0, CHUNKS // 2))

        @pl.when(j == 6)
        def _():
            gdy.relay_near(range(CHUNKS // 2, CHUNKS))

        attend_block(j, q_ref, k_ref, vt_ref, e_ref, m_ref, ot_ref, lse_ref)
        return 0

    lax.fori_loop(0, NB, attend, 0)
    gdy.relay_diagonal()
    for number in (3, 4, 5, 6):
        gdy.await_sibling(number)
    for m in range(1, NB):
        table_copy(m).wait_send()
    gx.finish_sends()
    gdy.finish_sends()
    dy_mine.wait()
    ht_copy.wait()


def backward_kernel(dy_all, wo_hbm, q_ref, k_ref, v_ref, ot_ref, lse_ref, tabs,
                    gq_ref, ot_all,
                    dyv, wo, do_ref, kt_ref, dk_ref, dv_ref, give, take,
                    local_sem, o_send, o_recv, pair_send, pair_recv):
    hp, cp, xn, yn, dn = neighbours()
    mine = head_slot(hp, cp)
    hw = HEADS * DH
    wo_load = pltpu.make_async_copy(wo_hbm.at[pl.ds(pl.multiple_of(mine * hw, hw), hw)], wo, local_sem.at[NB])
    wo_load.start()
    for d in range(NB):
        pltpu.make_async_copy(dy_all.at[d], dyv.at[d], local_sem.at[d]).start()
    ot_mine = pltpu.make_async_copy(ot_ref, ot_all.at[mine], local_sem.at[NB + 1])
    ot_mine.start()
    enter_barrier()
    go = Gather(ot_ref, ot_all, head_slot, o_send, o_recv, hw)
    go.start_own()
    kt_ref[...] = k_ref[...].T
    dk_ref[...] = jnp.zeros_like(dk_ref)
    dv_ref[...] = jnp.zeros_like(dv_ref)
    wo_load.wait()

    def project(d, _):
        pltpu.make_async_copy(dy_all.at[d], dyv.at[d], local_sem.at[d]).wait()
        do = nt_dot(dyv[d], wo[...]).astype(BF16)
        dst = rows_of(seq_block(d))
        for h in range(HEADS):
            do_ref[h, dst, :] = do[:, DH * h:DH * (h + 1)]
        return 0

    lax.fori_loop(0, NB, project, 0)

    def attend(j, _):
        @pl.when(j == 5)
        def _():
            go.relay_near(range(0, CHUNKS // 2))

        @pl.when(j == 6)
        def _():
            go.relay_near(range(CHUNKS // 2, CHUNKS))

        slot = stored_block(j)
        src = rows_of(slot)
        q4 = q_ref[:, rows_of(j), :].reshape(CW, DH)
        do4 = do_ref[:, rows_of(j), :].reshape(CW, DH)
        o4t = jnp.concatenate([ot_ref[DH * h:DH * (h + 1), src] for h in range(HEADS)], axis=1)
        lse = jnp.concatenate([lse_ref[h:h + 1, rows_of(j)] for h in range(HEADS)], axis=1)
        delta = jnp.sum(do4.astype(F32).T * o4t.astype(F32), axis=0, keepdims=True)

        def tile(kb, dqt, masked):
            keys = rows_of(kb)
            p = jnp.exp2(nt_dot(k_ref[keys, :], q4) * EXP2_SCALE - lse)
            if masked:
                p = jnp.where(causal_tile(), p, 0.0)
            dp = nt_dot(v_ref[keys, :], do4)
            dv_ref[keys, :] += dot(p.astype(BF16), do4)
            ds = (p * (dp - delta)).astype(BF16)
            dk_ref[keys, :] += dot(ds, q4)
            return dqt + dot(kt_ref[:, keys], ds)

        dqt = tile(j, jnp.zeros((DH, CW), F32), True)
        dqt = lax.fori_loop(0, j, functools.partial(tile, masked=False), dqt) * (DH ** -0.5)
        cos_t, sin_t = unpack_table(tabs[slot])
        for p in range(HEADS // 2):
            pair = jnp.concatenate([dqt[:, BLK * (2 * p):BLK * (2 * p + 1)], dqt[:, BLK * (2 * p + 1):BLK * (2 * p + 2)]], axis=0)
            dq = pair.T.astype(BF16).astype(F32)
            gq_ref[src, 128 * p:128 * (p + 1)] = rope_pairs(dq, cos_t, -sin_t).astype(BF16)
        return 0

    lax.fori_loop(0, NB, attend, 0)
    give[:, :DH] = (dk_ref[...] * (DH ** -0.5)).astype(BF16)
    give[:, DH:] = dv_ref[...].astype(BF16)
    swap = pltpu.make_async_remote_copy(
        src_ref=give, dst_ref=take, send_sem=pair_send, recv_sem=pair_recv, device_id=(hp, 1 - cp), device_id_type=MESH)
    swap.start()
    go.relay_diagonal()
    swap.wait_recv()
    lane = lax.broadcasted_iota(jnp.int32, (BLK, 2 * DH), 1)
    for i in range(NB // 2):
        slot = cp * 4 + i
        src = rows_of(seq_block(slot))
        total = (give[src, :].astype(F32) + take[src, :].astype(F32)).astype(BF16).astype(F32)
        cos_t, sin_t = unpack_table(tabs[slot])
        turned = rope_pairs(total, cos_t, -sin_t)
        gq_ref[pl.ds(NB * BLK + (i % 2) * BLK, BLK), 128 * (i // 2):128 * (i // 2 + 1)] = jnp.where(lane < DH, turned, total).astype(BF16)
    for number in (3, 4, 5, 6):
        go.await_sibling(number)
    swap.wait_send()
    go.finish_sends()
    ot_mine.wait()


VMEM_SPEC = pl.BlockSpec(memory_space=pltpu.VMEM)
ANY_SPEC = pl.BlockSpec(memory_space=pl.ANY)


def run_forward(x_own, dy_own, gain, w_q, w_k, w_v, tab):
    rows, width = x_own.shape
    toks = rows * NB
    hw = HEADS * DH
    return pl.pallas_call(
        forward_kernel,
        out_shape=(
            jax.ShapeDtypeStruct((NB, rows, width), BF16),
            jax.ShapeDtypeStruct((width, toks), BF16),
            jax.ShapeDtypeStruct((HEADS, toks, DH), BF16),
            jax.ShapeDtypeStruct((toks, DH), BF16),
            jax.ShapeDtypeStruct((toks, DH), BF16),
            jax.ShapeDtypeStruct((hw, toks), BF16),
            jax.ShapeDtypeStruct((HEADS, toks), F32),
            jax.ShapeDtypeStruct((NB, 128, 128), F32),
        ),
        in_specs=[ANY_SPEC, ANY_SPEC, VMEM_SPEC, ANY_SPEC, ANY_SPEC, ANY_SPEC, ANY_SPEC],
        out_specs=(ANY_SPEC, ANY_SPEC) + (VMEM_SPEC,) * 6,
        scratch_shapes=[
            pltpu.VMEM((NB, rows, width), BF16), pltpu.VMEM((width, toks), BF16),
            pltpu.VMEM((toks, CW), F32), pltpu.VMEM((NB, CW), F32), pltpu.VMEM((DH, toks), BF16),
            pltpu.VMEM((width, hw), BF16), pltpu.VMEM((width, 128), BF16), pltpu.VMEM((width, 128), BF16),
            pltpu.VMEM((width, 128), BF16), pltpu.VMEM((rows, width), BF16),
            pltpu.SemaphoreType.DMA((8,)), pltpu.SemaphoreType.DMA((7,)), pltpu.SemaphoreType.DMA((7,)),
        ] + gather_sems() + gather_sems(),
        compiler_params=pltpu.CompilerParams(vmem_limit_bytes=60 * 1024 * 1024, collective_id=0, has_side_effects=True),
        cost_estimate=pl.CostEstimate(flops=30_000_000_000, bytes_accessed=20_000_000, transcendentals=0),
        name="attn_forward",
    )(x_own, dy_own, gain, w_q, w_k, w_v, tab)


def run_backward(dy_all, w_o, q, k, v, o_t, lse, tabs):
    _, rows, width = dy_all.shape
    toks = rows * NB
    hw = HEADS * DH
    return pl.pallas_call(
        backward_kernel,
        out_shape=(
            jax.ShapeDtypeStruct((toks + 2 * BLK, hw), BF16),
            jax.ShapeDtypeStruct((NB, hw, toks), BF16),
        ),
        in_specs=[ANY_SPEC, ANY_SPEC] + [VMEM_SPEC] * 6,
        out_specs=(VMEM_SPEC, ANY_SPEC),
        scratch_shapes=[
            pltpu.VMEM((NB, rows, width), BF16), pltpu.VMEM((hw, width), BF16),
            pltpu.VMEM((HEADS, toks, DH), BF16), pltpu.VMEM((DH, toks), BF16),
            pltpu.VMEM((toks, DH), F32), pltpu.VMEM((toks, DH), F32),
            pltpu.VMEM((toks, 2 * DH), BF16), pltpu.VMEM((toks, 2 * DH), BF16),
            pltpu.SemaphoreType.DMA((NB + 2,)),
        ] + gather_sems() + [pltpu.SemaphoreType.DMA, pltpu.SemaphoreType.DMA],
        compiler_params=pltpu.CompilerParams(vmem_limit_bytes=60 * 1024 * 1024, collective_id=1, has_side_effects=True),
        cost_estimate=pl.CostEstimate(flops=40_000_000_000, bytes_accessed=20_000_000, transcendentals=0),
        name="attn_backward",
    )(dy_all, w_o, q, k, v, o_t, lse, tabs)


def solution(mesh):
    def device_step(hidden, grad_out, positions, norm_gain, w_q, w_k, w_v, w_o, inv_freq):
        rows = hidden.shape[0]
        toks = rows * NB
        hw = HEADS * DH
        hp, cp = lax.axis_index('hp'), lax.axis_index('cp')
        me_tok = tok_slot(hp, cp)
        angles = positions.astype(F32)[:, None] * inv_freq[None, :]
        cos_h, sin_h = jnp.cos(angles), jnp.sin(angles)
        tab = jnp.concatenate([cos_h[:128], sin_h[:128], cos_h[128:], sin_h[128:]], axis=1)
        gain = norm_gain.astype(F32)[None, :]
        dy_all, h_t, q, k, v, o_t, lse, tabs = run_forward(hidden, grad_out, gain, w_q, w_k, w_v, tab)
        gq_ext, ot_all = run_backward(dy_all, w_o, q, k, v, o_t, lse, tabs)
        ot_all = ot_all.reshape(NB * hw, toks)
        ext = lax.all_gather(gq_ext, ('hp', 'cp'), axis=0)
        gq_cols = ext[:, :toks].transpose(1, 0, 2).reshape(toks, NB * hw)
        gkv = ext[:, toks:].reshape(4, 2, 2 * BLK, 2, 2 * DH).transpose(0, 1, 3, 2, 4).reshape(4, toks, 2 * DH)
        gk_cols = gkv[:, :, :DH].transpose(1, 0, 2).reshape(toks, 4 * DH)
        gv_cols = gkv[:, :, DH:].transpose(1, 0, 2).reshape(toks, 4 * DH)
        x_f32 = hidden.astype(F32)
        inv_rms = lax.rsqrt(jnp.mean(x_f32 * x_f32, axis=-1, keepdims=True) + NORM_EPS)
        x_hat = x_f32 * inv_rms
        o_mine = lax.dynamic_slice_in_dim(ot_all, me_tok * rows, rows, 1)
        output = (x_f32 + jnp.einsum('at,ab->tb', o_mine, w_o, preferred_element_type=F32)).astype(BF16)
        grad_wo = jnp.dot(ot_all, dy_all.reshape(toks, -1), preferred_element_type=F32)
        grad_wq = jnp.dot(h_t, gq_cols, preferred_element_type=F32)
        grad_wk = jnp.dot(h_t, gk_cols, preferred_element_type=F32)
        grad_wv = jnp.dot(h_t, gv_cols, preferred_element_type=F32)
        mine = lambda a: lax.dynamic_slice_in_dim(a, me_tok * rows, rows, 0)
        d_norm = (jnp.einsum('tb,ab->ta', mine(gq_cols), w_q, preferred_element_type=F32)
                  + jnp.einsum('tb,ab->ta', mine(gk_cols), w_k, preferred_element_type=F32)
                  + jnp.einsum('tb,ab->ta', mine(gv_cols), w_v, preferred_element_type=F32))
        gain_part = jnp.sum(d_norm * x_hat, axis=0, keepdims=True)
        grad_gain = jnp.sum(lax.all_gather(gain_part, ('cp', 'hp'), axis=0, tiled=True), axis=0)
        d_hat = d_norm * gain
        grad_hidden = (grad_out.astype(F32) + inv_rms * (d_hat - x_hat * jnp.mean(d_hat * x_hat, axis=-1, keepdims=True))).astype(BF16)
        return output, grad_hidden, grad_wq, grad_wk, grad_wv, grad_wo, grad_gain

    seq_spec = P(('cp', 'hp'), None)
    whole = P()
    return jax.shard_map(device_step, mesh=mesh, in_specs=(seq_spec, seq_spec, P(('cp', 'hp')), whole, whole, whole, whole, whole, whole), out_specs=(seq_spec, seq_spec, whole, whole, whole, whole, whole), check_vma=False)
```

```python
import functools
import math

import jax
import jax.numpy as jnp
from jax import lax
from jax.experimental import pallas as pl
from jax.experimental.pallas import tpu as pltpu
from jax.sharding import PartitionSpec as P

NORM_EPS = 1e-5
BLK = 256
HEADS = 4
DH = 64
NB = 8
CW = HEADS * BLK
EXP2_SCALE = (DH ** -0.5) * math.log2(math.e)
F32 = jnp.float32
BF16 = jnp.bfloat16


def seq_block(d):
    cp, half, sub = d // 4, (d // 2) % 2, d % 2
    return 2 * ((1 - half) * cp + half * (3 - cp)) + sub


def stored_block(j):
    b, sub = j // 2, j % 2
    half = b // 2
    cp = (1 - half) * b + half * (3 - b)
    return cp * 4 + half * 2 + sub


def nt_dot(a, b):
    return lax.dot_general(a, b, (((1,), (1,)), ((), ())), preferred_element_type=F32)


def dot(a, b):
    return jnp.dot(a, b, preferred_element_type=F32)


def rope_pairs(t, cos_t, sin_t):
    lane = lax.broadcasted_iota(jnp.int32, t.shape, 1)
    partner = jnp.where(lane % DH < DH // 2, pltpu.roll(t, 128 - DH // 2, 1), pltpu.roll(t, DH // 2, 1))
    return t * cos_t + partner * sin_t


def rows_of(b):
    return pl.ds(pl.multiple_of(b * BLK, BLK), BLK)


def causal_tile():
    row = lax.broadcasted_iota(jnp.int32, (BLK, CW), 0)
    col = lax.broadcasted_iota(jnp.int32, (BLK, CW), 1)
    return row <= col % BLK


MESH = pl.DeviceIdType.MESH
CHUNKS = 4


def neighbours():
    hp, cp = lax.axis_index('hp'), lax.axis_index('cp')
    flip = 1 - 2 * (hp % 2)
    y_hp = (hp + 2) % 4
    return hp, cp, hp + flip, y_hp, y_hp + flip


def tok_slot(hp, cp):
    return cp * 4 + hp


def head_slot(hp, cp):
    return hp * 2 + cp


def enter_barrier():
    hp, cp = lax.axis_index('hp'), lax.axis_index('cp')
    barrier = pltpu.get_barrier_semaphore()
    for m in range(1, 8):
        pl.semaphore_signal(barrier, inc=1, device_id=((hp + m // 2) % 4, (cp + m % 2) % 2), device_id_type=MESH)
    pl.semaphore_wait(barrier, 7)


class Gather:
    def __init__(self, src, dst, slot, send, recv, rows):
        self.src, self.dst, self.slot, self.send, self.recv = src, dst, slot, send, recv
        self.step = rows // CHUNKS
        self.hp, self.cp, self.xn, self.yn, self.dn = neighbours()

    def part(self, ref, c):
        return ref.at[pl.ds(c * self.step, self.step)]

    def place(self, hp, cp, c):
        return self.part(self.dst.at[self.slot(hp, cp)], c)

    def copy(self, kind, c):
        hp, cp, xn, yn, dn = self.hp, self.cp, self.xn, self.yn, self.dn
        origin, lands, to = {
            'own_x': (hp, 0, (xn, cp)), 'own_y': (hp, 1, (yn, cp)), 'own_s': (hp, 3, (hp, 1 - cp)),
            'x_s': (xn, 4, (hp, 1 - cp)), 'y_s': (yn, 5, (hp, 1 - cp)), 'd_s': (dn, 6, (hp, 1 - cp)),
            'x_y': (xn, 2, (yn, cp)), 'y_x': (yn, 2, (xn, cp)),
        }[kind]
        number = ('own_x', 'own_y', 'own_s', 'x_s', 'y_s', 'd_s', 'x_y', 'y_x').index(kind)
        src = self.part(self.src, c) if kind.startswith('own') else self.place(origin, cp, c)
        return pltpu.make_async_remote_copy(
            src_ref=src, dst_ref=self.place(origin, cp, c), send_sem=self.send.at[number, c],
            recv_sem=self.recv.at[lands, c], device_id=to, device_id_type=MESH)

    def await_from(self, number, c):
        hp, cp = ((self.xn, self.cp), (self.yn, self.cp), (self.dn, self.cp), (self.hp, 1 - self.cp),
                  (self.xn, 1 - self.cp), (self.yn, 1 - self.cp), (self.dn, 1 - self.cp))[number]
        ref = self.place(hp, cp, c)
        pltpu.make_async_remote_copy(
            src_ref=ref, dst_ref=ref, send_sem=self.send.at[0, c], recv_sem=self.recv.at[number, c],
            device_id=(self.hp, 1 - self.cp), device_id_type=MESH).wait_recv()

    def start_own(self):
        for c in range(CHUNKS):
            for kind in ('own_x', 'own_y', 'own_s'):
                self.copy(kind, c).start()

    def relay_near(self, chunks=range(CHUNKS)):
        for c in chunks:
            self.await_from(0, c)
            self.copy('x_s', c).start()
            if c < CHUNKS // 2:
                self.copy('x_y', c).start()
            self.await_from(1, c)
            self.copy('y_s', c).start()
            if c >= CHUNKS // 2:
                self.copy('y_x', c).start()

    def relay_diagonal(self):
        for c in range(CHUNKS):
            self.await_from(2, c)
            self.copy('d_s', c).start()

    def await_sibling(self, number):
        for c in range(CHUNKS):
            self.await_from(number, c)

    def finish_sends(self):
        for c in range(CHUNKS):
            for kind in ('own_x', 'own_y', 'own_s', 'x_s', 'y_s', 'd_s'):
                self.copy(kind, c).wait_send()
            self.copy('x_y' if c < CHUNKS // 2 else 'y_x', c).wait_send()


def gather_sems():
    return [pltpu.SemaphoreType.DMA((8, CHUNKS)), pltpu.SemaphoreType.DMA((7, CHUNKS))]


def unpack_table(tab):
    group = lax.broadcasted_iota(jnp.int32, tab.shape, 1) // (DH // 2)
    turned = [tab] + [pltpu.roll(tab, 32 * i, 1) for i in (1, 2, 3)]

    def pick(order):
        out = turned[order[3]]
        for g in range(3):
            out = jnp.where(group == g, turned[order[g]], out)
        return out

    sign = jnp.where(group % 2 == 0, -1.0, 1.0)
    cos_t = jnp.concatenate([pick((0, 1, 2, 3)), pick((2, 3, 0, 1))], axis=0)
    sin_t = jnp.concatenate([pick((3, 0, 1, 2)) * sign, pick((1, 2, 3, 0)) * sign], axis=0)
    return cos_t, sin_t


def project_block(d, x, gain, wq_ref, wkv_ref, tab, ht_ref, q_ref, k_ref, v_ref):
    xf = x.astype(F32)
    inv = lax.rsqrt(jnp.mean(xf * xf, axis=-1, keepdims=True) + NORM_EPS)
    h = (xf * inv * gain).astype(BF16)
    ht_ref[:, rows_of(d)] = h.T
    dst = rows_of(seq_block(d))
    cos_t, sin_t = unpack_table(tab)
    y = dot(h, wq_ref[...])
    for p in range(HEADS // 2):
        qr = rope_pairs(y[:, 128 * p:128 * (p + 1)], cos_t, sin_t).astype(BF16)
        q_ref[2 * p, dst, :] = qr[:, :DH]
        q_ref[2 * p + 1, dst, :] = qr[:, DH:]
    kv = dot(h, wkv_ref[...])
    k_ref[dst, :] = rope_pairs(kv, cos_t, sin_t).astype(BF16)[:, :DH]
    v_ref[dst, :] = kv.astype(BF16)[:, DH:]


def attend_block(j, q_ref, k_ref, vt_ref, e_ref, m_ref, ot_ref, lse_ref):
    q4 = q_ref[:, rows_of(j), :].reshape(CW, DH)

    def score_tile(kb, carry, masked):
        m_old, l_old = carry
        s = nt_dot(k_ref[rows_of(kb), :], q4) * EXP2_SCALE
        if masked:
            s = jnp.where(causal_tile(), s, -1e30)
        m_new = jnp.maximum(m_old, jnp.max(s, axis=0, keepdims=True))
        e = jnp.exp2(s - m_new)
        e_ref[rows_of(kb), :] = e
        m_ref[pl.ds(kb, 1), :] = m_new
        return m_new, l_old * jnp.exp2(m_old - m_new) + jnp.sum(e, axis=0, keepdims=True)

    carry = (jnp.full((1, CW), -1e30, F32), jnp.zeros((1, CW), F32))
    carry = score_tile(j, carry, True)
    m_fin, l_fin = lax.fori_loop(0, j, functools.partial(score_tile, masked=False), carry)
    inv_l = 1.0 / l_fin
    lse = m_fin + jnp.log2(l_fin)

    def out_tile(kb, acc):
        f = jnp.exp2(m_ref[pl.ds(kb, 1), :] - m_fin) * inv_l
        p = (e_ref[rows_of(kb), :] * f).astype(BF16)
        return acc + dot(vt_ref[:, rows_of(kb)], p)

    acc = lax.fori_loop(0, j + 1, out_tile, jnp.zeros((DH, CW), F32)).astype(BF16)
    dst = rows_of(stored_block(j))
    for h in range(HEADS):
        ot_ref[DH * h:DH * (h + 1), dst] = acc[:, BLK * h:BLK * (h + 1)]
        lse_ref[h:h + 1, rows_of(j)] = lse[:, BLK * h:BLK * (h + 1)]


def forward_kernel(x_own, dy_own, gain_ref, wq_hbm, wk_hbm, wv_hbm, tab_own,
                   dy_all, ht_out, q_ref, k_ref, v_ref, ot_ref, lse_ref, tabs,
                   xg, ht, e_ref, m_ref, vt_ref, wq, wk, wv, wkv, stage,
                   local_sem, tab_send, tab_recv, x_send, x_recv, dy_send, dy_recv):
    hp, cp, xn, yn, dn = neighbours()
    mine = tok_slot(hp, cp)
    hw = HEADS * DH
    loads = [
        pltpu.make_async_copy(x_own, xg.at[mine], local_sem.at[0]),
        pltpu.make_async_copy(wq_hbm.at[:, pl.ds(pl.multiple_of(head_slot(hp, cp) * hw, hw), hw)], wq, local_sem.at[1]),
        pltpu.make_async_copy(wk_hbm.at[:, pl.ds(pl.multiple_of((hp // 2) * 128, 128), 128)], wk, local_sem.at[2]),
        pltpu.make_async_copy(wv_hbm.at[:, pl.ds(pl.multiple_of((hp // 2) * 128, 128), 128)], wv, local_sem.at[3]),
        pltpu.make_async_copy(dy_own, stage, local_sem.at[4]),
        pltpu.make_async_copy(tab_own, tabs.at[mine], local_sem.at[5]),
    ]
    for load in loads:
        load.start()
    enter_barrier()
    gx = Gather(x_own, xg, tok_slot, x_send, x_recv, BLK)
    gdy = Gather(dy_own, dy_all, tok_slot, dy_send, dy_recv, BLK)

    def table_copy(m):
        to = ((hp + m // 2) % 4, (cp + m % 2) % 2)
        return pltpu.make_async_remote_copy(
            src_ref=tab_own, dst_ref=tabs.at[mine], send_sem=tab_send.at[m - 1], recv_sem=tab_recv.at[m - 1],
            device_id=to, device_id_type=MESH)

    for m in range(1, NB):
        table_copy(m).start()
    gx.start_own()
    for load in loads[1:4]:
        load.wait()
    lane = lax.broadcasted_iota(jnp.int32, wk.shape, 1)
    swap = hp % 2 == 1
    kf, vf = wk[...].astype(F32), wv[...].astype(F32)
    k_sel = jnp.where(swap, pltpu.roll(kf, DH, 1), kf)
    v_sel = jnp.where(swap, vf, pltpu.roll(vf, DH, 1))
    wkv[...] = jnp.where(lane < DH, k_sel, v_sel).astype(BF16)
    for i in (0, 4, 5):
        loads[i].wait()
    dy_mine = pltpu.make_async_copy(stage, dy_all.at[mine], local_sem.at[6])
    dy_mine.start()
    for m in range(1, NB):
        src_slot = tok_slot((hp + 4 - m // 2) % 4, (cp + m % 2) % 2)
        ref = tabs.at[src_slot]
        pltpu.make_async_remote_copy(
            src_ref=ref, dst_ref=ref, send_sem=tab_send.at[m - 1], recv_sem=tab_recv.at[m - 1],
            device_id=(hp, 1 - cp), device_id_type=MESH).wait_recv()

    def project(e, _):
        @pl.when(e == 1)
        def _():
            gx.await_sibling(3)

        @pl.when(e == 2)
        def _():
            gx.relay_near()
            gdy.start_own()

        @pl.when(e == 3)
        def _():
            gx.await_sibling(4)

        @pl.when(e == 5)
        def _():
            gx.await_sibling(5)

        @pl.when(e == 6)
        def _():
            gx.relay_diagonal()

        @pl.when(e == 7)
        def _():
            gx.await_sibling(6)

        m, b = e // 2, e % 2
        px = (hp % 2 + m % 2) % 2
        py = (hp // 2 + m // 2) % 2
        d = tok_slot(py * 2 + px, (cp + b) % 2)
        project_block(d, xg[d], gain_ref[...], wq, wkv, tabs[d], ht, q_ref, k_ref, v_ref)
        return 0

    lax.fori_loop(0, NB, project, 0)
    ht_copy = pltpu.make_async_copy(ht, ht_out, local_sem.at[7])
    ht_copy.start()
    vt_ref[...] = v_ref[...].T

    def attend(j, _):
        @pl.when(j == 5)
        def _():
            gdy.relay_near(range(0, CHUNKS // 2))

        @pl.when(j == 6)
        def _():
            gdy.relay_near(range(CHUNKS // 2, CHUNKS))

        attend_block(j, q_ref, k_ref, vt_ref, e_ref, m_ref, ot_ref, lse_ref)
        return 0

    lax.fori_loop(0, NB, attend, 0)
    gdy.relay_diagonal()
    for number in (3, 4, 5, 6):
        gdy.await_sibling(number)
    for m in range(1, NB):
        table_copy(m).wait_send()
    gx.finish_sends()
    gdy.finish_sends()
    dy_mine.wait()
    ht_copy.wait()


def backward_kernel(dy_all, wo_hbm, q_ref, k_ref, v_ref, ot_ref, lse_ref, tabs,
                    gq_ref, gkv_ref, ot_all,
                    dyv, wo, do_ref, kt_ref, dk_ref, dv_ref, give, take,
                    local_sem, o_send, o_recv, pair_send, pair_recv):
    hp, cp, xn, yn, dn = neighbours()
    mine = head_slot(hp, cp)
    hw = HEADS * DH
    wo_load = pltpu.make_async_copy(wo_hbm.at[pl.ds(pl.multiple_of(mine * hw, hw), hw)], wo, local_sem.at[NB])
    wo_load.start()
    for d in range(NB):
        pltpu.make_async_copy(dy_all.at[d], dyv.at[d], local_sem.at[d]).start()
    ot_mine = pltpu.make_async_copy(ot_ref, ot_all.at[mine], local_sem.at[NB + 1])
    ot_mine.start()
    enter_barrier()
    go = Gather(ot_ref, ot_all, head_slot, o_send, o_recv, hw)
    go.start_own()
    kt_ref[...] = k_ref[...].T
    dk_ref[...] = jnp.zeros_like(dk_ref)
    dv_ref[...] = jnp.zeros_like(dv_ref)
    wo_load.wait()

    def project(d, _):
        pltpu.make_async_copy(dy_all.at[d], dyv.at[d], local_sem.at[d]).wait()
        do = nt_dot(dyv[d], wo[...]).astype(BF16)
        dst = rows_of(seq_block(d))
        for h in range(HEADS):
            do_ref[h, dst, :] = do[:, DH * h:DH * (h + 1)]
        return 0

    lax.fori_loop(0, NB, project, 0)

    def attend(j, _):
        @pl.when(j == 5)
        def _():
            go.relay_near(range(0, CHUNKS // 2))

        @pl.when(j == 6)
        def _():
            go.relay_near(range(CHUNKS // 2, CHUNKS))

        slot = stored_block(j)
        src = rows_of(slot)
        q4 = q_ref[:, rows_of(j), :].reshape(CW, DH)
        do4 = do_ref[:, rows_of(j), :].reshape(CW, DH)
        o4t = jnp.concatenate([ot_ref[DH * h:DH * (h + 1), src] for h in range(HEADS)], axis=1)
        lse = jnp.concatenate([lse_ref[h:h + 1, rows_of(j)] for h in range(HEADS)], axis=1)
        delta = jnp.sum(do4.astype(F32).T * o4t.astype(F32), axis=0, keepdims=True)

        def tile(kb, dqt, masked):
            keys = rows_of(kb)
            p = jnp.exp2(nt_dot(k_ref[keys, :], q4) * EXP2_SCALE - lse)
            if masked:
                p = jnp.where(causal_tile(), p, 0.0)
            dp = nt_dot(v_ref[keys, :], do4)
            dv_ref[keys, :] += dot(p.astype(BF16), do4)
            ds = (p * (dp - delta)).astype(BF16)
            dk_ref[keys, :] += dot(ds, q4)
            return dqt + dot(kt_ref[:, keys], ds)

        dqt = tile(j, jnp.zeros((DH, CW), F32), True)
        dqt = lax.fori_loop(0, j, functools.partial(tile, masked=False), dqt) * (DH ** -0.5)
        cos_t, sin_t = unpack_table(tabs[slot])
        for p in range(HEADS // 2):
            pair = jnp.concatenate([dqt[:, BLK * (2 * p):BLK * (2 * p + 1)], dqt[:, BLK * (2 * p + 1):BLK * (2 * p + 2)]], axis=0)
            dq = pair.T.astype(BF16).astype(F32)
            gq_ref[src, 128 * p:128 * (p + 1)] = rope_pairs(dq, cos_t, -sin_t).astype(BF16)
        return 0

    lax.fori_loop(0, NB, attend, 0)
    give[:, :DH] = (dk_ref[...] * (DH ** -0.5)).astype(BF16)
    give[:, DH:] = dv_ref[...].astype(BF16)
    swap = pltpu.make_async_remote_copy(
        src_ref=give, dst_ref=take, send_sem=pair_send, recv_sem=pair_recv, device_id=(hp, 1 - cp), device_id_type=MESH)
    swap.start()
    go.relay_diagonal()
    swap.wait_recv()
    lane = lax.broadcasted_iota(jnp.int32, (BLK, 2 * DH), 1)
    for i in range(NB // 2):
        slot = cp * 4 + i
        src = rows_of(seq_block(slot))
        total = (give[src, :].astype(F32) + take[src, :].astype(F32)).astype(BF16).astype(F32)
        cos_t, sin_t = unpack_table(tabs[slot])
        turned = rope_pairs(total, cos_t, -sin_t)
        gkv_ref[(i % 2) * BLK:(i % 2 + 1) * BLK, 128 * (i // 2):128 * (i // 2 + 1)] = jnp.where(lane < DH, turned, total).astype(BF16)
    for number in (3, 4, 5, 6):
        go.await_sibling(number)
    swap.wait_send()
    go.finish_sends()
    ot_mine.wait()


def nth_peer(e):
    hp, cp = lax.axis_index('hp'), lax.axis_index('cp')
    m, b = e // 2, e % 2
    px = (hp % 2 + m % 2) % 2
    py = (hp // 2 + m // 2) % 2
    return py * 2 + px, (cp + b) % 2


def weight_grad(a_ref, b, stage):
    def rows(i, _):
        a = a_ref[pl.ds(2 * i, 2)].reshape(2 * BLK, NB * BLK)
        stage[pl.ds(pl.multiple_of(i * 2 * BLK, 2 * BLK), 2 * BLK), :] = dot(a, b)
        return 0

    lax.fori_loop(0, NB // 2, rows, 0)


def grads_kernel(gq_own, gkv_own, ot_hbm, dy_hbm, ht_hbm, wo_hbm, wq_hbm, wk_hbm, wv_hbm, x_ref, dy_ref, gain_ref,
                 out_ref, gh_ref, gq_all, gwo_hbm, gwk_ref, gwv_ref, gg_ref,
                 gkvg, ot, dya, wbuf, wk, wv, stage, acc, o_mine, gq_mine, bk, bv, pass_gq, gains,
                 local_sem, stage_sem, mine_sem, q_send, q_recv, kv_send, kv_recv, gain_send, gain_recv):
    hp, cp, xn, yn, dn = neighbours()
    me_tok, me_head = tok_slot(hp, cp), head_slot(hp, cp)
    my_rows = rows_of(me_tok)
    copy = pltpu.make_async_copy
    loads = dict(
        ot=copy(ot_hbm, ot, local_sem.at[0]), wo=copy(wo_hbm, wbuf, local_sem.at[1]),
        dy=copy(dy_hbm, dya, local_sem.at[2]), gq=copy(gq_own, pass_gq, local_sem.at[3]),
        gkv=copy(gkv_own, gkvg.at[me_head], local_sem.at[4]),
        wk=copy(wk_hbm, wk, local_sem.at[5]), wv=copy(wv_hbm, wv, local_sem.at[6]))
    for name in ('gkv', 'ot', 'wo', 'gq', 'dy', 'wk', 'wv'):
        loads[name].start()
    enter_barrier()
    gkv = Gather(gkv_own, gkvg, head_slot, kv_send, kv_recv, 2 * BLK)
    ggq = Gather(gq_own, gq_all, head_slot, q_send, q_recv, NB * BLK)
    gkv.start_own()
    ggq.start_own()
    loads['gq'].wait()
    keep_gq = copy(pass_gq, gq_all.at[me_head], local_sem.at[7])
    keep_gq.start()

    loads['ot'].wait()

    def turn(d, _):
        o_mine[:, rows_of(d)] = ot[d, :, my_rows].T
        return 0

    lax.fori_loop(0, NB, turn, 0)
    loads['wo'].wait()

    def out_cols(n, _):
        cols = rows_of(n)
        out_ref[:, cols] = (x_ref[:, cols].astype(F32) + dot(o_mine[...], wbuf[:, cols])).astype(BF16)
        return 0

    lax.fori_loop(0, NB, out_cols, 0)
    wq_load = copy(wq_hbm, wbuf, local_sem.at[8])
    wq_load.start()
    gkv.relay_near()
    loads['dy'].wait()

    def stage_out(n, slot):
        return copy(stage.at[slot], gwo_hbm.at[:, rows_of(n)], stage_sem.at[slot])

    def wo_cols(n, _):
        @pl.when(n == 1)
        def _():
            gkv.relay_diagonal()

        @pl.when(n == 3)
        def _():
            ggq.relay_near(range(0, CHUNKS // 2))

        slot = n % 2

        @pl.when(n >= 2)
        def _():
            stage_out(n - 2, slot).wait()

        weight_grad(ot, dya[:, :, rows_of(n)].reshape(NB * BLK, BLK), stage.at[slot])
        stage_out(n, slot).start()
        return 0

    lax.fori_loop(0, NB, wo_cols, 0)
    ht_load = copy(ht_hbm, dya, local_sem.at[9])
    ht_load.start()
    ggq.relay_near(range(CHUNKS // 2, CHUNKS))

    for number in (3, 4, 5, 6):
        gkv.await_sibling(number)
    loads['gkv'].wait()
    for c in range(2):
        for r in range(2):
            dst = pl.ds((c * 2 + r) * 2 * BLK, 2 * BLK)
            for p in range(2):
                even = gkvg[4 * p + c, :, 128 * r:128 * (r + 1)]
                odd = gkvg[4 * p + 2 + c, :, 128 * r:128 * (r + 1)]
                bk[dst, 128 * p:128 * (p + 1)] = jnp.concatenate([even[:, :DH], odd[:, :DH]], axis=1)
                bv[dst, 128 * p:128 * (p + 1)] = jnp.concatenate([even[:, DH:], odd[:, DH:]], axis=1)
    ht_load.wait()
    weight_grad(dya, bk[...], gwk_ref)
    weight_grad(dya, bv[...], gwv_ref)

    loads['wk'].wait()
    loads['wv'].wait()
    acc[...] = nt_dot(bk[my_rows, :], wk[...]) + nt_dot(bv[my_rows, :], wv[...])
    wq_load.wait()
    keep_gq.wait()
    for number in (3, 4, 5):
        ggq.await_sibling(number)

    def fetch(e):
        return copy(gq_all.at[head_slot(*nth_peer(e)), my_rows], gq_mine.at[e], mine_sem.at[e])

    def add_head(e, _):
        fetch(e).wait()
        cols = rows_of(head_slot(*nth_peer(e)))
        acc[...] += nt_dot(gq_mine[e], wbuf[:, cols])
        return 0

    for e in range(6):
        fetch(e).start()
    lax.fori_loop(0, 6, add_head, 0)
    ggq.relay_diagonal()
    fetch(6).start()
    ggq.await_sibling(6)
    fetch(7).start()
    lax.fori_loop(6, NB, add_head, 0)

    x = x_ref[...].astype(F32)
    inv = lax.rsqrt(jnp.mean(x * x, axis=-1, keepdims=True) + NORM_EPS)
    x_hat = x * inv
    d_norm = acc[...]
    gains[me_tok] = jnp.sum(d_norm * x_hat, axis=0, keepdims=True)

    def gain_copy(m):
        return pltpu.make_async_remote_copy(
            src_ref=gains.at[me_tok], dst_ref=gains.at[me_tok], send_sem=gain_send.at[m - 1], recv_sem=gain_recv.at[m - 1],
            device_id=((hp + m // 2) % 4, (cp + m % 2) % 2), device_id_type=MESH)

    d_hat = d_norm * gain_ref[...]
    row_mean = jnp.mean(d_hat * x_hat, axis=-1, keepdims=True)
    for m in range(1, NB):
        gain_copy(m).start()
    gh_ref[...] = (dy_ref[...].astype(F32) + inv * (d_hat - x_hat * row_mean)).astype(BF16)
    for m in range(1, NB):
        ref = gains.at[tok_slot((hp + 4 - m // 2) % 4, (cp + m % 2) % 2)]
        pltpu.make_async_remote_copy(
            src_ref=ref, dst_ref=ref, send_sem=gain_send.at[m - 1], recv_sem=gain_recv.at[m - 1],
            device_id=(hp, 1 - cp), device_id_type=MESH).wait_recv()
    total = gains[0]
    for d in range(1, NB):
        total = total + gains[d]
    gg_ref[...] = total
    for m in range(1, NB):
        gain_copy(m).wait_send()
    for n in (NB - 2, NB - 1):
        stage_out(n, n % 2).wait()
    gkv.finish_sends()
    ggq.finish_sends()


def wq_kernel(ht_ref, gq_ref, gwo_in, gwq_ref, gwo_ref):
    gwo_ref[...] = gwo_in[...]
    b = gq_ref[0]

    def rows(i, _):
        r = pl.ds(pl.multiple_of(i * 2 * BLK, 2 * BLK), 2 * BLK)
        gwq_ref[r, :] = dot(ht_ref[r, :], b)
        return 0

    lax.fori_loop(0, NB // 2, rows, 0)


VMEM_SPEC = pl.BlockSpec(memory_space=pltpu.VMEM)
ANY_SPEC = pl.BlockSpec(memory_space=pl.ANY)


def run_forward(x_own, dy_own, gain, w_q, w_k, w_v, tab):
    rows, width = x_own.shape
    toks = rows * NB
    hw = HEADS * DH
    return pl.pallas_call(
        forward_kernel,
        out_shape=(
            jax.ShapeDtypeStruct((NB, rows, width), BF16),
            jax.ShapeDtypeStruct((width, toks), BF16),
            jax.ShapeDtypeStruct((HEADS, toks, DH), BF16),
            jax.ShapeDtypeStruct((toks, DH), BF16),
            jax.ShapeDtypeStruct((toks, DH), BF16),
            jax.ShapeDtypeStruct((hw, toks), BF16),
            jax.ShapeDtypeStruct((HEADS, toks), F32),
            jax.ShapeDtypeStruct((NB, 128, 128), F32),
        ),
        in_specs=[ANY_SPEC, ANY_SPEC, VMEM_SPEC, ANY_SPEC, ANY_SPEC, ANY_SPEC, ANY_SPEC],
        out_specs=(ANY_SPEC, ANY_SPEC) + (VMEM_SPEC,) * 6,
        scratch_shapes=[
            pltpu.VMEM((NB, rows, width), BF16), pltpu.VMEM((width, toks), BF16),
            pltpu.VMEM((toks, CW), F32), pltpu.VMEM((NB, CW), F32), pltpu.VMEM((DH, toks), BF16),
            pltpu.VMEM((width, hw), BF16), pltpu.VMEM((width, 128), BF16), pltpu.VMEM((width, 128), BF16),
            pltpu.VMEM((width, 128), BF16), pltpu.VMEM((rows, width), BF16),
            pltpu.SemaphoreType.DMA((8,)), pltpu.SemaphoreType.DMA((7,)), pltpu.SemaphoreType.DMA((7,)),
        ] + gather_sems() + gather_sems(),
        compiler_params=pltpu.CompilerParams(vmem_limit_bytes=60 * 1024 * 1024, collective_id=0, has_side_effects=True),
        cost_estimate=pl.CostEstimate(flops=30_000_000_000, bytes_accessed=20_000_000, transcendentals=0),
        name="attn_forward",
    )(x_own, dy_own, gain, w_q, w_k, w_v, tab)


def run_backward(dy_all, w_o, q, k, v, o_t, lse, tabs):
    _, rows, width = dy_all.shape
    toks = rows * NB
    hw = HEADS * DH
    return pl.pallas_call(
        backward_kernel,
        out_shape=(
            jax.ShapeDtypeStruct((toks, hw), BF16),
            jax.ShapeDtypeStruct((2 * BLK, hw), BF16),
            jax.ShapeDtypeStruct((NB, hw, toks), BF16),
        ),
        in_specs=[ANY_SPEC, ANY_SPEC] + [VMEM_SPEC] * 6,
        out_specs=(VMEM_SPEC, VMEM_SPEC, ANY_SPEC),
        scratch_shapes=[
            pltpu.VMEM((NB, rows, width), BF16), pltpu.VMEM((hw, width), BF16),
            pltpu.VMEM((HEADS, toks, DH), BF16), pltpu.VMEM((DH, toks), BF16),
            pltpu.VMEM((toks, DH), F32), pltpu.VMEM((toks, DH), F32),
            pltpu.VMEM((toks, 2 * DH), BF16), pltpu.VMEM((toks, 2 * DH), BF16),
            pltpu.SemaphoreType.DMA((NB + 2,)),
        ] + gather_sems() + [pltpu.SemaphoreType.DMA, pltpu.SemaphoreType.DMA],
        compiler_params=pltpu.CompilerParams(vmem_limit_bytes=60 * 1024 * 1024, collective_id=1, has_side_effects=True),
        cost_estimate=pl.CostEstimate(flops=40_000_000_000, bytes_accessed=20_000_000, transcendentals=0),
        name="attn_backward",
    )(dy_all, w_o, q, k, v, o_t, lse, tabs)


def run_grads(gq, gkv, ot_all, dy_all, h_t, w_o, w_q, w_k, w_v, x_own, dy_own, gain):
    rows, width = x_own.shape
    toks = rows * NB
    hw = HEADS * DH
    kv = w_k.shape[1]
    dma = pltpu.SemaphoreType.DMA
    return pl.pallas_call(
        grads_kernel,
        out_shape=(
            jax.ShapeDtypeStruct((rows, width), BF16), jax.ShapeDtypeStruct((rows, width), BF16),
            jax.ShapeDtypeStruct((NB, toks, hw), BF16), jax.ShapeDtypeStruct((NB * hw, width), F32),
            jax.ShapeDtypeStruct((width, kv), F32), jax.ShapeDtypeStruct((width, kv), F32),
            jax.ShapeDtypeStruct((1, width), F32),
        ),
        in_specs=[ANY_SPEC] * 9 + [VMEM_SPEC] * 3,
        out_specs=(VMEM_SPEC, VMEM_SPEC, ANY_SPEC, ANY_SPEC, VMEM_SPEC, VMEM_SPEC, VMEM_SPEC),
        scratch_shapes=[
            pltpu.VMEM((NB, 2 * BLK, hw), BF16), pltpu.VMEM((NB, hw, toks), BF16), pltpu.VMEM((NB, rows, width), BF16),
            pltpu.VMEM((NB * hw, width), BF16), pltpu.VMEM((width, kv), BF16), pltpu.VMEM((width, kv), BF16),
            pltpu.VMEM((2, NB * hw, BLK), F32), pltpu.VMEM((rows, width), F32), pltpu.VMEM((rows, NB * hw), BF16),
            pltpu.VMEM((NB, rows, hw), BF16), pltpu.VMEM((toks, kv), BF16), pltpu.VMEM((toks, kv), BF16),
            pltpu.VMEM((toks, hw), BF16), pltpu.VMEM((NB, 1, width), F32),
            dma((10,)), dma((2,)), dma((NB,)),
        ] + gather_sems() + gather_sems() + [dma((7,)), dma((7,))],
        compiler_params=pltpu.CompilerParams(vmem_limit_bytes=60 * 1024 * 1024, collective_id=2, has_side_effects=True),
        cost_estimate=pl.CostEstimate(flops=40_000_000_000, bytes_accessed=60_000_000, transcendentals=0),
        name="grads",
    )(gq, gkv, ot_all, dy_all, h_t.reshape(NB, BLK, toks), w_o, w_q, w_k, w_v, x_own, dy_own, gain)


def run_wq(h_t, gq_all, gwo):
    width, toks = h_t.shape
    hw = HEADS * DH
    cols = pl.BlockSpec((width, hw), lambda n: (0, n))
    return pl.pallas_call(
        wq_kernel,
        grid=(NB,),
        out_shape=(jax.ShapeDtypeStruct((width, NB * hw), F32), jax.ShapeDtypeStruct(gwo.shape, F32)),
        in_specs=[VMEM_SPEC, pl.BlockSpec((1, toks, hw), lambda n: (n, 0, 0)), cols],
        out_specs=(cols, cols),
        compiler_params=pltpu.CompilerParams(vmem_limit_bytes=60 * 1024 * 1024),
        cost_estimate=pl.CostEstimate(flops=17_000_000_000, bytes_accessed=67_000_000, transcendentals=0),
        name="wq_grad",
    )(h_t, gq_all, gwo)


def solution(mesh):
    def device_step(hidden, grad_out, positions, norm_gain, w_q, w_k, w_v, w_o, inv_freq):
        angles = positions.astype(F32)[:, None] * inv_freq[None, :]
        cos_h, sin_h = jnp.cos(angles), jnp.sin(angles)
        tab = jnp.concatenate([cos_h[:128], sin_h[:128], cos_h[128:], sin_h[128:]], axis=1)
        gain = norm_gain.astype(F32)[None, :]
        dy_all, h_t, q, k, v, o_t, lse, tabs = run_forward(hidden, grad_out, gain, w_q, w_k, w_v, tab)
        g_q, g_kv, ot_all = run_backward(dy_all, w_o, q, k, v, o_t, lse, tabs)
        output, grad_hidden, gq_all, gwo, grad_wk, grad_wv, grad_gain = run_grads(
            g_q, g_kv, ot_all, dy_all, h_t, w_o, w_q, w_k, w_v, hidden, grad_out, gain)
        grad_wq, grad_wo = run_wq(h_t, gq_all, gwo)
        return output, grad_hidden, grad_wq, grad_wk, grad_wv, grad_wo, grad_gain[0]

    seq_spec = P(('cp', 'hp'), None)
    whole = P()
    return jax.shard_map(device_step, mesh=mesh, in_specs=(seq_spec, seq_spec, P(('cp', 'hp')), whole, whole, whole, whole, whole, whole), out_specs=(seq_spec, seq_spec, whole, whole, whole, whole, whole), check_vma=False)
```

```python
import functools
import math

import jax
import jax.numpy as jnp
from jax import lax
from jax.experimental import pallas as pl
from jax.experimental.pallas import tpu as pltpu
from jax.sharding import PartitionSpec as P

NORM_EPS = 1e-5
BLK = 256
HEADS = 4
DH = 64
NB = 8
CW = HEADS * BLK
EXP2_SCALE = (DH ** -0.5) * math.log2(math.e)
F32 = jnp.float32
BF16 = jnp.bfloat16


def seq_block(d):
    cp, half, sub = d // 4, (d // 2) % 2, d % 2
    return 2 * ((1 - half) * cp + half * (3 - cp)) + sub


def stored_block(j):
    b, sub = j // 2, j % 2
    half = b // 2
    cp = (1 - half) * b + half * (3 - b)
    return cp * 4 + half * 2 + sub


def nt_dot(a, b):
    return lax.dot_general(a, b, (((1,), (1,)), ((), ())), preferred_element_type=F32)


def dot(a, b):
    return jnp.dot(a, b, preferred_element_type=F32)


def rope_pairs(t, cos_t, sin_t):
    lane = lax.broadcasted_iota(jnp.int32, t.shape, 1)
    partner = jnp.where(lane % DH < DH // 2, pltpu.roll(t, 128 - DH // 2, 1), pltpu.roll(t, DH // 2, 1))
    return t * cos_t + partner * sin_t


def rows_of(b):
    return pl.ds(pl.multiple_of(b * BLK, BLK), BLK)


def causal_tile():
    row = lax.broadcasted_iota(jnp.int32, (BLK, CW), 0)
    col = lax.broadcasted_iota(jnp.int32, (BLK, CW), 1)
    return row <= col % BLK


MESH = pl.DeviceIdType.MESH
CHUNKS = 4


def neighbours():
    hp, cp = lax.axis_index('hp'), lax.axis_index('cp')
    flip = 1 - 2 * (hp % 2)
    y_hp = (hp + 2) % 4
    return hp, cp, hp + flip, y_hp, y_hp + flip


def tok_slot(hp, cp):
    return cp * 4 + hp


def head_slot(hp, cp):
    return hp * 2 + cp


def enter_barrier():
    hp, cp = lax.axis_index('hp'), lax.axis_index('cp')
    barrier = pltpu.get_barrier_semaphore()
    for m in range(1, 8):
        pl.semaphore_signal(barrier, inc=1, device_id=((hp + m // 2) % 4, (cp + m % 2) % 2), device_id_type=MESH)
    pl.semaphore_wait(barrier, 7)


class Gather:
    def __init__(self, src, dst, slot, send, recv, rows):
        self.src, self.dst, self.slot, self.send, self.recv = src, dst, slot, send, recv
        self.step = rows // CHUNKS
        self.hp, self.cp, self.xn, self.yn, self.dn = neighbours()

    def part(self, ref, c):
        return ref.at[pl.ds(c * self.step, self.step)]

    def place(self, hp, cp, c):
        return self.part(self.dst.at[self.slot(hp, cp)], c)

    def copy(self, kind, c):
        hp, cp, xn, yn, dn = self.hp, self.cp, self.xn, self.yn, self.dn
        origin, lands, to = {
            'own_x': (hp, 0, (xn, cp)), 'own_y': (hp, 1, (yn, cp)), 'own_s': (hp, 3, (hp, 1 - cp)),
            'x_s': (xn, 4, (hp, 1 - cp)), 'y_s': (yn, 5, (hp, 1 - cp)), 'd_s': (dn, 6, (hp, 1 - cp)),
            'x_y': (xn, 2, (yn, cp)), 'y_x': (yn, 2, (xn, cp)),
        }[kind]
        number = ('own_x', 'own_y', 'own_s', 'x_s', 'y_s', 'd_s', 'x_y', 'y_x').index(kind)
        src = self.part(self.src, c) if kind.startswith('own') else self.place(origin, cp, c)
        return pltpu.make_async_remote_copy(
            src_ref=src, dst_ref=self.place(origin, cp, c), send_sem=self.send.at[number, c],
            recv_sem=self.recv.at[lands, c], device_id=to, device_id_type=MESH)

    def await_from(self, number, c):
        hp, cp = ((self.xn, self.cp), (self.yn, self.cp), (self.dn, self.cp), (self.hp, 1 - self.cp),
                  (self.xn, 1 - self.cp), (self.yn, 1 - self.cp), (self.dn, 1 - self.cp))[number]
        ref = self.place(hp, cp, c)
        pltpu.make_async_remote_copy(
            src_ref=ref, dst_ref=ref, send_sem=self.send.at[0, c], recv_sem=self.recv.at[number, c],
            device_id=(self.hp, 1 - self.cp), device_id_type=MESH).wait_recv()

    def start_own(self):
        for c in range(CHUNKS):
            for kind in ('own_x', 'own_y', 'own_s'):
                self.copy(kind, c).start()

    def relay_near(self, chunks=range(CHUNKS)):
        for c in chunks:
            self.await_from(0, c)
            self.copy('x_s', c).start()
            if c < CHUNKS // 2:
                self.copy('x_y', c).start()
            self.await_from(1, c)
            self.copy('y_s', c).start()
            if c >= CHUNKS // 2:
                self.copy('y_x', c).start()

    def relay_diagonal(self):
        for c in range(CHUNKS):
            self.await_from(2, c)
            self.copy('d_s', c).start()

    def await_sibling(self, number):
        for c in range(CHUNKS):
            self.await_from(number, c)

    def finish_sends(self):
        for c in range(CHUNKS):
            for kind in ('own_x', 'own_y', 'own_s', 'x_s', 'y_s', 'd_s'):
                self.copy(kind, c).wait_send()
            self.copy('x_y' if c < CHUNKS // 2 else 'y_x', c).wait_send()


def gather_sems():
    return [pltpu.SemaphoreType.DMA((8, CHUNKS)), pltpu.SemaphoreType.DMA((7, CHUNKS))]


def unpack_table(tab):
    group = lax.broadcasted_iota(jnp.int32, tab.shape, 1) // (DH // 2)
    turned = [tab] + [pltpu.roll(tab, 32 * i, 1) for i in (1, 2, 3)]

    def pick(order):
        out = turned[order[3]]
        for g in range(3):
            out = jnp.where(group == g, turned[order[g]], out)
        return out

    sign = jnp.where(group % 2 == 0, -1.0, 1.0)
    cos_t = jnp.concatenate([pick((0, 1, 2, 3)), pick((2, 3, 0, 1))], axis=0)
    sin_t = jnp.concatenate([pick((3, 0, 1, 2)) * sign, pick((1, 2, 3, 0)) * sign], axis=0)
    return cos_t, sin_t


def project_block(d, x, gain, wq_ref, wkv_ref, tab, ht_ref, q_ref, k_ref, v_ref):
    xf = x.astype(F32)
    inv = lax.rsqrt(jnp.mean(xf * xf, axis=-1, keepdims=True) + NORM_EPS)
    h = (xf * inv * gain).astype(BF16)
    ht_ref[:, rows_of(d)] = h.T
    dst = rows_of(seq_block(d))
    cos_t, sin_t = unpack_table(tab)
    y = dot(h, wq_ref[...])
    for p in range(HEADS // 2):
        qr = rope_pairs(y[:, 128 * p:128 * (p + 1)], cos_t, sin_t).astype(BF16)
        q_ref[2 * p, dst, :] = qr[:, :DH]
        q_ref[2 * p + 1, dst, :] = qr[:, DH:]
    kv = dot(h, wkv_ref[...])
    k_ref[dst, :] = rope_pairs(kv, cos_t, sin_t).astype(BF16)[:, :DH]
    v_ref[dst, :] = kv.astype(BF16)[:, DH:]


def attend_block(j, q_ref, k_ref, vt_ref, e_ref, m_ref, ot_ref, lse_ref):
    q4 = q_ref[:, rows_of(j), :].reshape(CW, DH)

    def score_tile(kb, carry, masked):
        m_old, l_old = carry
        s = nt_dot(k_ref[rows_of(kb), :], q4) * EXP2_SCALE
        if masked:
            s = jnp.where(causal_tile(), s, -1e30)
        m_new = jnp.maximum(m_old, jnp.max(s, axis=0, keepdims=True))
        e = jnp.exp2(s - m_new)
        e_ref[rows_of(kb), :] = e
        m_ref[pl.ds(kb, 1), :] = m_new
        return m_new, l_old * jnp.exp2(m_old - m_new) + jnp.sum(e, axis=0, keepdims=True)

    carry = (jnp.full((1, CW), -1e30, F32), jnp.zeros((1, CW), F32))
    carry = score_tile(j, carry, True)
    m_fin, l_fin = lax.fori_loop(0, j, functools.partial(score_tile, masked=False), carry)
    inv_l = 1.0 / l_fin
    lse = m_fin + jnp.log2(l_fin)

    def out_tile(kb, acc):
        f = jnp.exp2(m_ref[pl.ds(kb, 1), :] - m_fin) * inv_l
        p = (e_ref[rows_of(kb), :] * f).astype(BF16)
        return acc + dot(vt_ref[:, rows_of(kb)], p)

    acc = lax.fori_loop(0, j + 1, out_tile, jnp.zeros((DH, CW), F32)).astype(BF16)
    dst = rows_of(stored_block(j))
    for h in range(HEADS):
        ot_ref[DH * h:DH * (h + 1), dst] = acc[:, BLK * h:BLK * (h + 1)]
        lse_ref[h:h + 1, rows_of(j)] = lse[:, BLK * h:BLK * (h + 1)]


def forward_kernel(x_own, dy_own, gain_ref, wq_hbm, wk_hbm, wv_hbm, tab_own,
                   dy_all, ht_out, q_ref, k_ref, v_ref, ot_ref, lse_ref, tabs,
                   xg, ht, e_ref, m_ref, vt_ref, wq, wk, wv, wkv, stage,
                   local_sem, t_send, t_recv, x_send, x_recv, dy_send, dy_recv):
    hp, cp, xn, yn, dn = neighbours()
    mine = tok_slot(hp, cp)
    hw = HEADS * DH
    loads = [
        pltpu.make_async_copy(x_own, xg.at[mine], local_sem.at[0]),
        pltpu.make_async_copy(wq_hbm.at[:, pl.ds(pl.multiple_of(head_slot(hp, cp) * hw, hw), hw)], wq, local_sem.at[1]),
        pltpu.make_async_copy(wk_hbm.at[:, pl.ds(pl.multiple_of((hp // 2) * 128, 128), 128)], wk, local_sem.at[2]),
        pltpu.make_async_copy(wv_hbm.at[:, pl.ds(pl.multiple_of((hp // 2) * 128, 128), 128)], wv, local_sem.at[3]),
        pltpu.make_async_copy(dy_own, stage, local_sem.at[4]),
        pltpu.make_async_copy(tab_own, tabs.at[mine], local_sem.at[5]),
    ]
    for load in loads:
        load.start()
    enter_barrier()
    gx = Gather(x_own, xg, tok_slot, x_send, x_recv, BLK)
    gdy = Gather(dy_own, dy_all, tok_slot, dy_send, dy_recv, BLK)

    gt = Gather(tab_own, tabs, tok_slot, t_send, t_recv, 128)
    gt.start_own()
    gx.start_own()
    for load in loads[1:4]:
        load.wait()
    lane = lax.broadcasted_iota(jnp.int32, wk.shape, 1)
    swap = hp % 2 == 1
    kf, vf = wk[...].astype(F32), wv[...].astype(F32)
    k_sel = jnp.where(swap, pltpu.roll(kf, DH, 1), kf)
    v_sel = jnp.where(swap, vf, pltpu.roll(vf, DH, 1))
    wkv[...] = jnp.where(lane < DH, k_sel, v_sel).astype(BF16)
    for i in (0, 4, 5):
        loads[i].wait()
    dy_mine = pltpu.make_async_copy(stage, dy_all.at[mine], local_sem.at[6])
    dy_mine.start()
    def project(e, _):
        @pl.when(e == 1)
        def _():
            gt.await_sibling(3)
            gx.await_sibling(3)

        @pl.when(e == 2)
        def _():
            gt.relay_near()
            gx.relay_near()
            gdy.start_own()

        @pl.when(e == 3)
        def _():
            gt.await_sibling(4)
            gx.await_sibling(4)

        @pl.when(e == 5)
        def _():
            gt.await_sibling(5)
            gx.await_sibling(5)

        @pl.when(e == 6)
        def _():
            gt.relay_diagonal()
            gx.relay_diagonal()

        @pl.when(e == 7)
        def _():
            gt.await_sibling(6)
            gx.await_sibling(6)

        m, b = e // 2, e % 2
        px = (hp % 2 + m % 2) % 2
        py = (hp // 2 + m // 2) % 2
        d = tok_slot(py * 2 + px, (cp + b) % 2)
        project_block(d, xg[d], gain_ref[...], wq, wkv, tabs[d], ht, q_ref, k_ref, v_ref)
        return 0

    lax.fori_loop(0, NB, project, 0)
    ht_copy = pltpu.make_async_copy(ht, ht_out, local_sem.at[7])
    ht_copy.start()
    vt_ref[...] = v_ref[...].T

    def attend(j, _):
        for c in range(CHUNKS):
            @pl.when(j == (1, 3, 4, 5)[c])
            def _():
                gdy.relay_near((c,))

        attend_block(j, q_ref, k_ref, vt_ref, e_ref, m_ref, ot_ref, lse_ref)
        return 0

    lax.fori_loop(0, NB, attend, 0)
    gdy.relay_diagonal()
    for number in (3, 4, 5, 6):
        gdy.await_sibling(number)
    gt.finish_sends()
    gx.finish_sends()
    gdy.finish_sends()
    dy_mine.wait()
    ht_copy.wait()


def backward_kernel(dy_all, wo_hbm, q_ref, k_ref, v_ref, ot_ref, lse_ref, tabs,
                    gq_ref, gkv_ref, ot_all,
                    dyv, wo, do_ref, kt_ref, dk_ref, dv_ref, give, take,
                    local_sem, o_send, o_recv, pair_send, pair_recv):
    hp, cp, xn, yn, dn = neighbours()
    mine = head_slot(hp, cp)
    hw = HEADS * DH
    wo_load = pltpu.make_async_copy(wo_hbm.at[pl.ds(pl.multiple_of(mine * hw, hw), hw)], wo, local_sem.at[NB])
    wo_load.start()
    for d in range(NB):
        pltpu.make_async_copy(dy_all.at[d], dyv.at[d], local_sem.at[d]).start()
    ot_mine = pltpu.make_async_copy(ot_ref, ot_all.at[mine], local_sem.at[NB + 1])
    ot_mine.start()
    enter_barrier()
    go = Gather(ot_ref, ot_all, head_slot, o_send, o_recv, hw)
    go.start_own()
    kt_ref[...] = k_ref[...].T
    dk_ref[...] = jnp.zeros_like(dk_ref)
    dv_ref[...] = jnp.zeros_like(dv_ref)
    wo_load.wait()

    def project(d, _):
        pltpu.make_async_copy(dy_all.at[d], dyv.at[d], local_sem.at[d]).wait()
        do = nt_dot(dyv[d], wo[...]).astype(BF16)
        dst = rows_of(seq_block(d))
        for h in range(HEADS):
            do_ref[h, dst, :] = do[:, DH * h:DH * (h + 1)]
        return 0

    lax.fori_loop(0, NB, project, 0)

    def attend(j, _):
        @pl.when(j == 5)
        def _():
            go.relay_near(range(0, CHUNKS // 2))

        @pl.when(j == 6)
        def _():
            go.relay_near(range(CHUNKS // 2, CHUNKS))

        slot = stored_block(j)
        src = rows_of(slot)
        q4 = q_ref[:, rows_of(j), :].reshape(CW, DH)
        do4 = do_ref[:, rows_of(j), :].reshape(CW, DH)
        o4t = jnp.concatenate([ot_ref[DH * h:DH * (h + 1), src] for h in range(HEADS)], axis=1)
        lse = jnp.concatenate([lse_ref[h:h + 1, rows_of(j)] for h in range(HEADS)], axis=1)
        delta = jnp.sum(do4.astype(F32).T * o4t.astype(F32), axis=0, keepdims=True)

        def tile(kb, dqt, masked):
            keys = rows_of(kb)
            p = jnp.exp2(nt_dot(k_ref[keys, :], q4) * EXP2_SCALE - lse)
            if masked:
                p = jnp.where(causal_tile(), p, 0.0)
            dp = nt_dot(v_ref[keys, :], do4)
            dv_ref[keys, :] += dot(p.astype(BF16), do4)
            ds = (p * (dp - delta)).astype(BF16)
            dk_ref[keys, :] += dot(ds, q4)
            return dqt + dot(kt_ref[:, keys], ds)

        dqt = tile(j, jnp.zeros((DH, CW), F32), True)
        dqt = lax.fori_loop(0, j, functools.partial(tile, masked=False), dqt) * (DH ** -0.5)
        cos_t, sin_t = unpack_table(tabs[slot])
        for p in range(HEADS // 2):
            pair = jnp.concatenate([dqt[:, BLK * (2 * p):BLK * (2 * p + 1)], dqt[:, BLK * (2 * p + 1):BLK * (2 * p + 2)]], axis=0)
            dq = pair.T.astype(BF16).astype(F32)
            gq_ref[src, 128 * p:128 * (p + 1)] = rope_pairs(dq, cos_t, -sin_t).astype(BF16)
        return 0

    lax.fori_loop(0, NB, attend, 0)
    give[:, :DH] = (dk_ref[...] * (DH ** -0.5)).astype(BF16)
    give[:, DH:] = dv_ref[...].astype(BF16)
    swap = pltpu.make_async_remote_copy(
        src_ref=give, dst_ref=take, send_sem=pair_send, recv_sem=pair_recv, device_id=(hp, 1 - cp), device_id_type=MESH)
    swap.start()
    go.relay_diagonal()
    swap.wait_recv()
    lane = lax.broadcasted_iota(jnp.int32, (BLK, 2 * DH), 1)
    for i in range(NB // 2):
        slot = cp * 4 + i
        src = rows_of(seq_block(slot))
        total = (give[src, :].astype(F32) + take[src, :].astype(F32)).astype(BF16).astype(F32)
        cos_t, sin_t = unpack_table(tabs[slot])
        turned = rope_pairs(total, cos_t, -sin_t)
        gkv_ref[(i % 2) * BLK:(i % 2 + 1) * BLK, 128 * (i // 2):128 * (i // 2 + 1)] = jnp.where(lane < DH, turned, total).astype(BF16)
    for number in (3, 4, 5, 6):
        go.await_sibling(number)
    swap.wait_send()
    go.finish_sends()
    ot_mine.wait()


def nth_peer(e):
    hp, cp = lax.axis_index('hp'), lax.axis_index('cp')
    m, b = e // 2, e % 2
    px = (hp % 2 + m % 2) % 2
    py = (hp // 2 + m // 2) % 2
    return py * 2 + px, (cp + b) % 2


def weight_grad(a_ref, b, stage):
    stage[...] = dot(a_ref[...].reshape(NB * BLK, NB * BLK), b)


def grads_kernel(gq_own, gkv_own, ot_hbm, dy_hbm, ht_hbm, wo_hbm, wq_hbm, wk_hbm, wv_hbm, x_ref, dy_ref, gain_ref,
                 out_ref, gh_ref, gq_all, gwo_hbm, gwk_ref, gwv_ref, gg_ref,
                 gkvg, ot, dya, wbuf, wk, wv, stage, acc, o_mine, gq_mine, bk, bv, pass_gq, gains,
                 local_sem, stage_sem, mine_sem, q_send, q_recv, kv_send, kv_recv, gain_send, gain_recv):
    hp, cp, xn, yn, dn = neighbours()
    me_tok, me_head = tok_slot(hp, cp), head_slot(hp, cp)
    my_rows = rows_of(me_tok)
    copy = pltpu.make_async_copy
    loads = dict(
        ot=copy(ot_hbm, ot, local_sem.at[0]), wo=copy(wo_hbm, wbuf, local_sem.at[1]),
        dy=copy(dy_hbm, dya, local_sem.at[2]), gq=copy(gq_own, pass_gq, local_sem.at[3]),
        gkv=copy(gkv_own, gkvg.at[me_head], local_sem.at[4]),
        wk=copy(wk_hbm, wk, local_sem.at[5]), wv=copy(wv_hbm, wv, local_sem.at[6]))
    for name in ('gkv', 'ot', 'wo', 'gq', 'dy', 'wk', 'wv'):
        loads[name].start()
    enter_barrier()
    gkv = Gather(gkv_own, gkvg, head_slot, kv_send, kv_recv, 2 * BLK)
    ggq = Gather(gq_own, gq_all, head_slot, q_send, q_recv, NB * BLK)
    gkv.start_own()
    ggq.start_own()
    loads['gq'].wait()
    keep_gq = copy(pass_gq, gq_all.at[me_head], local_sem.at[7])
    keep_gq.start()

    loads['ot'].wait()

    def turn(d, _):
        o_mine[:, rows_of(d)] = ot[d, :, my_rows].T
        return 0

    lax.fori_loop(0, NB, turn, 0)
    loads['wo'].wait()

    def out_cols(n, _):
        cols = rows_of(n)
        out_ref[:, cols] = (x_ref[:, cols].astype(F32) + dot(o_mine[...], wbuf[:, cols])).astype(BF16)
        return 0

    lax.fori_loop(0, NB, out_cols, 0)
    wq_load = copy(wq_hbm, wbuf, local_sem.at[8])
    wq_load.start()
    gkv.relay_near()
    loads['dy'].wait()

    def stage_out(n, slot):
        return copy(stage.at[slot], gwo_hbm.at[:, rows_of(n)], stage_sem.at[slot])

    def wo_cols(n, _):
        @pl.when(n == 1)
        def _():
            gkv.relay_diagonal()

        @pl.when(n == 3)
        def _():
            ggq.relay_near(range(0, CHUNKS // 2))

        slot = n % 2

        @pl.when(n >= 2)
        def _():
            stage_out(n - 2, slot).wait()

        weight_grad(ot, dya[:, :, rows_of(n)].reshape(NB * BLK, BLK), stage.at[slot])
        stage_out(n, slot).start()
        return 0

    lax.fori_loop(0, NB, wo_cols, 0)
    ht_load = copy(ht_hbm, dya, local_sem.at[9])
    ht_load.start()
    ggq.relay_near(range(CHUNKS // 2, CHUNKS))

    for number in (3, 4, 5, 6):
        gkv.await_sibling(number)
    loads['gkv'].wait()
    for c in range(2):
        for r in range(2):
            dst = pl.ds((c * 2 + r) * 2 * BLK, 2 * BLK)
            for p in range(2):
                even = gkvg[4 * p + c, :, 128 * r:128 * (r + 1)]
                odd = gkvg[4 * p + 2 + c, :, 128 * r:128 * (r + 1)]
                bk[dst, 128 * p:128 * (p + 1)] = jnp.concatenate([even[:, :DH], odd[:, :DH]], axis=1)
                bv[dst, 128 * p:128 * (p + 1)] = jnp.concatenate([even[:, DH:], odd[:, DH:]], axis=1)
    ht_load.wait()
    weight_grad(dya, bk[...], gwk_ref)
    weight_grad(dya, bv[...], gwv_ref)

    loads['wk'].wait()
    loads['wv'].wait()
    acc[...] = nt_dot(bk[my_rows, :], wk[...]) + nt_dot(bv[my_rows, :], wv[...])
    wq_load.wait()
    keep_gq.wait()
    for number in (3, 4, 5):
        ggq.await_sibling(number)

    def fetch(e):
        return copy(gq_all.at[head_slot(*nth_peer(e)), my_rows], gq_mine.at[e], mine_sem.at[e])

    def add_head(e, _):
        fetch(e).wait()
        cols = rows_of(head_slot(*nth_peer(e)))
        acc[...] += nt_dot(gq_mine[e], wbuf[:, cols])
        return 0

    for e in range(6):
        fetch(e).start()
    lax.fori_loop(0, 6, add_head, 0)
    ggq.relay_diagonal()
    fetch(6).start()
    ggq.await_sibling(6)
    fetch(7).start()
    lax.fori_loop(6, NB, add_head, 0)

    x = x_ref[...].astype(F32)
    inv = lax.rsqrt(jnp.mean(x * x, axis=-1, keepdims=True) + NORM_EPS)
    x_hat = x * inv
    d_norm = acc[...]
    gains[me_tok] = jnp.sum(d_norm * x_hat, axis=0, keepdims=True)

    def gain_copy(m):
        return pltpu.make_async_remote_copy(
            src_ref=gains.at[me_tok], dst_ref=gains.at[me_tok], send_sem=gain_send.at[m - 1], recv_sem=gain_recv.at[m - 1],
            device_id=((hp + m // 2) % 4, (cp + m % 2) % 2), device_id_type=MESH)

    d_hat = d_norm * gain_ref[...]
    row_mean = jnp.mean(d_hat * x_hat, axis=-1, keepdims=True)
    for m in range(1, NB):
        gain_copy(m).start()
    gh_ref[...] = (dy_ref[...].astype(F32) + inv * (d_hat - x_hat * row_mean)).astype(BF16)
    for m in range(1, NB):
        ref = gains.at[tok_slot((hp + 4 - m // 2) % 4, (cp + m % 2) % 2)]
        pltpu.make_async_remote_copy(
            src_ref=ref, dst_ref=ref, send_sem=gain_send.at[m - 1], recv_sem=gain_recv.at[m - 1],
            device_id=(hp, 1 - cp), device_id_type=MESH).wait_recv()
    total = gains[0]
    for d in range(1, NB):
        total = total + gains[d]
    gg_ref[...] = total
    for m in range(1, NB):
        gain_copy(m).wait_send()
    for n in (NB - 2, NB - 1):
        stage_out(n, n % 2).wait()
    gkv.finish_sends()
    ggq.finish_sends()


def wq_kernel(ht_ref, gq_ref, *refs):
    ins, outs = refs[:len(refs) // 2], refs[len(refs) // 2 + 1:]
    for src, dst in zip(ins, outs):
        dst[...] = src[...]
    refs[len(refs) // 2][...] = dot(ht_ref[...], gq_ref[0])


VMEM_SPEC = pl.BlockSpec(memory_space=pltpu.VMEM)
ANY_SPEC = pl.BlockSpec(memory_space=pl.ANY)


def run_forward(x_own, dy_own, gain, w_q, w_k, w_v, tab):
    rows, width = x_own.shape
    toks = rows * NB
    hw = HEADS * DH
    return pl.pallas_call(
        forward_kernel,
        out_shape=(
            jax.ShapeDtypeStruct((NB, rows, width), BF16),
            jax.ShapeDtypeStruct((width, toks), BF16),
            jax.ShapeDtypeStruct((HEADS, toks, DH), BF16),
            jax.ShapeDtypeStruct((toks, DH), BF16),
            jax.ShapeDtypeStruct((toks, DH), BF16),
            jax.ShapeDtypeStruct((hw, toks), BF16),
            jax.ShapeDtypeStruct((HEADS, toks), F32),
            jax.ShapeDtypeStruct((NB, 128, 128), F32),
        ),
        in_specs=[ANY_SPEC, ANY_SPEC, VMEM_SPEC, ANY_SPEC, ANY_SPEC, ANY_SPEC, ANY_SPEC],
        out_specs=(ANY_SPEC, ANY_SPEC) + (VMEM_SPEC,) * 6,
        scratch_shapes=[
            pltpu.VMEM((NB, rows, width), BF16), pltpu.VMEM((width, toks), BF16),
            pltpu.VMEM((toks, CW), F32), pltpu.VMEM((NB, CW), F32), pltpu.VMEM((DH, toks), BF16),
            pltpu.VMEM((width, hw), BF16), pltpu.VMEM((width, 128), BF16), pltpu.VMEM((width, 128), BF16),
            pltpu.VMEM((width, 128), BF16), pltpu.VMEM((rows, width), BF16),
            pltpu.SemaphoreType.DMA((8,)),
        ] + gather_sems() + gather_sems() + gather_sems(),
        compiler_params=pltpu.CompilerParams(vmem_limit_bytes=60 * 1024 * 1024, collective_id=0, has_side_effects=True),
        cost_estimate=pl.CostEstimate(flops=30_000_000_000, bytes_accessed=20_000_000, transcendentals=0),
        name="attn_forward",
    )(x_own, dy_own, gain, w_q, w_k, w_v, tab)


def run_backward(dy_all, w_o, q, k, v, o_t, lse, tabs):
    _, rows, width = dy_all.shape
    toks = rows * NB
    hw = HEADS * DH
    return pl.pallas_call(
        backward_kernel,
        out_shape=(
            jax.ShapeDtypeStruct((toks, hw), BF16),
            jax.ShapeDtypeStruct((2 * BLK, hw), BF16),
            jax.ShapeDtypeStruct((NB, hw, toks), BF16),
        ),
        in_specs=[ANY_SPEC, ANY_SPEC] + [VMEM_SPEC] * 6,
        out_specs=(VMEM_SPEC, VMEM_SPEC, ANY_SPEC),
        scratch_shapes=[
            pltpu.VMEM((NB, rows, width), BF16), pltpu.VMEM((hw, width), BF16),
            pltpu.VMEM((HEADS, toks, DH), BF16), pltpu.VMEM((DH, toks), BF16),
            pltpu.VMEM((toks, DH), F32), pltpu.VMEM((toks, DH), F32),
            pltpu.VMEM((toks, 2 * DH), BF16), pltpu.VMEM((toks, 2 * DH), BF16),
            pltpu.SemaphoreType.DMA((NB + 2,)),
        ] + gather_sems() + [pltpu.SemaphoreType.DMA, pltpu.SemaphoreType.DMA],
        compiler_params=pltpu.CompilerParams(vmem_limit_bytes=60 * 1024 * 1024, collective_id=1, has_side_effects=True),
        cost_estimate=pl.CostEstimate(flops=40_000_000_000, bytes_accessed=20_000_000, transcendentals=0),
        name="attn_backward",
    )(dy_all, w_o, q, k, v, o_t, lse, tabs)


def run_grads(gq, gkv, ot_all, dy_all, h_t, w_o, w_q, w_k, w_v, x_own, dy_own, gain):
    rows, width = x_own.shape
    toks = rows * NB
    hw = HEADS * DH
    kv = w_k.shape[1]
    dma = pltpu.SemaphoreType.DMA
    return pl.pallas_call(
        grads_kernel,
        out_shape=(
            jax.ShapeDtypeStruct((rows, width), BF16), jax.ShapeDtypeStruct((rows, width), BF16),
            jax.ShapeDtypeStruct((NB, toks, hw), BF16), jax.ShapeDtypeStruct((NB * hw, width), F32),
            jax.ShapeDtypeStruct((width, kv), F32), jax.ShapeDtypeStruct((width, kv), F32),
            jax.ShapeDtypeStruct((1, width), F32),
        ),
        in_specs=[ANY_SPEC] * 9 + [VMEM_SPEC] * 3,
        out_specs=(VMEM_SPEC, VMEM_SPEC, ANY_SPEC, ANY_SPEC, VMEM_SPEC, VMEM_SPEC, VMEM_SPEC),
        scratch_shapes=[
            pltpu.VMEM((NB, 2 * BLK, hw), BF16), pltpu.VMEM((NB, hw, toks), BF16), pltpu.VMEM((NB, rows, width), BF16),
            pltpu.VMEM((NB * hw, width), BF16), pltpu.VMEM((width, kv), BF16), pltpu.VMEM((width, kv), BF16),
            pltpu.VMEM((2, NB * hw, BLK), F32), pltpu.VMEM((rows, width), F32), pltpu.VMEM((rows, NB * hw), BF16),
            pltpu.VMEM((NB, rows, hw), BF16), pltpu.VMEM((toks, kv), BF16), pltpu.VMEM((toks, kv), BF16),
            pltpu.VMEM((toks, hw), BF16), pltpu.VMEM((NB, 1, width), F32),
            dma((10,)), dma((2,)), dma((NB,)),
        ] + gather_sems() + gather_sems() + [dma((7,)), dma((7,))],
        compiler_params=pltpu.CompilerParams(vmem_limit_bytes=60 * 1024 * 1024, collective_id=2, has_side_effects=True),
        cost_estimate=pl.CostEstimate(flops=40_000_000_000, bytes_accessed=60_000_000, transcendentals=0),
        name="grads",
    )(gq, gkv, ot_all, dy_all, h_t.reshape(NB, BLK, toks), w_o, w_q, w_k, w_v, x_own, dy_own, gain)


def run_wq(h_t, gq_all, passed):
    width, toks = h_t.shape
    hw = HEADS * DH
    cols = pl.BlockSpec((width, hw), lambda n: (0, n))
    specs = [cols] + [pl.BlockSpec((a.shape[0] // NB,) + a.shape[1:], lambda n: (n, 0)) for a in passed[1:]]
    return pl.pallas_call(
        wq_kernel,
        grid=(NB,),
        out_shape=(jax.ShapeDtypeStruct((width, NB * hw), F32),) + tuple(jax.ShapeDtypeStruct(a.shape, a.dtype) for a in passed),
        in_specs=[VMEM_SPEC, pl.BlockSpec((1, toks, hw), lambda n: (n, 0, 0))] + specs,
        out_specs=(cols,) + tuple(specs),
        compiler_params=pltpu.CompilerParams(vmem_limit_bytes=60 * 1024 * 1024),
        cost_estimate=pl.CostEstimate(flops=17_000_000_000, bytes_accessed=67_000_000, transcendentals=0),
        name="wq_grad",
    )(h_t, gq_all, *passed)


def solution(mesh):
    def device_step(hidden, grad_out, positions, norm_gain, w_q, w_k, w_v, w_o, inv_freq):
        angles = positions.astype(F32)[:, None] * inv_freq[None, :]
        cos_h, sin_h = jnp.cos(angles), jnp.sin(angles)
        tab = jnp.concatenate([cos_h[:128], sin_h[:128], cos_h[128:], sin_h[128:]], axis=1)
        gain = norm_gain.astype(F32)[None, :]
        dy_all, h_t, q, k, v, o_t, lse, tabs = run_forward(hidden, grad_out, gain, w_q, w_k, w_v, tab)
        g_q, g_kv, ot_all = run_backward(dy_all, w_o, q, k, v, o_t, lse, tabs)
        output, grad_hidden, gq_all, gwo, grad_wk, grad_wv, grad_gain = run_grads(
            g_q, g_kv, ot_all, dy_all, h_t, w_o, w_q, w_k, w_v, hidden, grad_out, gain)
        grad_wq, grad_wo, output, grad_hidden, grad_wk, grad_wv = run_wq(
            h_t, gq_all, (gwo, output, grad_hidden, grad_wk, grad_wv))
        return output, grad_hidden, grad_wq, grad_wk, grad_wv, grad_wo, grad_gain[0]

    seq_spec = P(('cp', 'hp'), None)
    whole = P()
    return jax.shard_map(device_step, mesh=mesh, in_specs=(seq_spec, seq_spec, P(('cp', 'hp')), whole, whole, whole, whole, whole, whole), out_specs=(seq_spec, seq_spec, whole, whole, whole, whole, whole), check_vma=False)
```

```python
import functools
import math

import jax
import jax.numpy as jnp
from jax import lax
from jax.experimental import pallas as pl
from jax.experimental.pallas import tpu as pltpu
from jax.sharding import PartitionSpec as P

NORM_EPS = 1e-5
BLK = 256
HEADS = 4
DH = 64
NB = 8
CW = HEADS * BLK
EXP2_SCALE = (DH ** -0.5) * math.log2(math.e)
F32 = jnp.float32
BF16 = jnp.bfloat16


def seq_block(d):
    cp, half, sub = d // 4, (d // 2) % 2, d % 2
    return 2 * ((1 - half) * cp + half * (3 - cp)) + sub


def stored_block(j):
    b, sub = j // 2, j % 2
    half = b // 2
    cp = (1 - half) * b + half * (3 - b)
    return cp * 4 + half * 2 + sub


def nt_dot(a, b):
    return lax.dot_general(a, b, (((1,), (1,)), ((), ())), preferred_element_type=F32)


def dot(a, b):
    return jnp.dot(a, b, preferred_element_type=F32)


def rope_pairs(t, cos_t, sin_t):
    lane = lax.broadcasted_iota(jnp.int32, t.shape, 1)
    partner = jnp.where(lane % DH < DH // 2, pltpu.roll(t, 128 - DH // 2, 1), pltpu.roll(t, DH // 2, 1))
    return t * cos_t + partner * sin_t


def rows_of(b):
    return pl.ds(pl.multiple_of(b * BLK, BLK), BLK)


def causal_tile():
    row = lax.broadcasted_iota(jnp.int32, (BLK, CW), 0)
    col = lax.broadcasted_iota(jnp.int32, (BLK, CW), 1)
    return row <= col % BLK


MESH = pl.DeviceIdType.MESH
CHUNKS = 4


def neighbours():
    hp, cp = lax.axis_index('hp'), lax.axis_index('cp')
    flip = 1 - 2 * (hp % 2)
    y_hp = (hp + 2) % 4
    return hp, cp, hp + flip, y_hp, y_hp + flip


def tok_slot(hp, cp):
    return cp * 4 + hp


def head_slot(hp, cp):
    return hp * 2 + cp


def enter_barrier():
    hp, cp = lax.axis_index('hp'), lax.axis_index('cp')
    barrier = pltpu.get_barrier_semaphore()
    for m in range(1, 8):
        pl.semaphore_signal(barrier, inc=1, device_id=((hp + m // 2) % 4, (cp + m % 2) % 2), device_id_type=MESH)
    pl.semaphore_wait(barrier, 7)


class Gather:
    def __init__(self, src, dst, slot, send, recv, rows):
        self.src, self.dst, self.slot, self.send, self.recv = src, dst, slot, send, recv
        self.step = rows // CHUNKS
        self.hp, self.cp, self.xn, self.yn, self.dn = neighbours()

    def part(self, ref, c):
        return ref.at[pl.ds(c * self.step, self.step)]

    def place(self, hp, cp, c):
        return self.part(self.dst.at[self.slot(hp, cp)], c)

    def copy(self, kind, c):
        hp, cp, xn, yn, dn = self.hp, self.cp, self.xn, self.yn, self.dn
        origin, lands, to = {
            'own_x': (hp, 0, (xn, cp)), 'own_y': (hp, 1, (yn, cp)), 'own_s': (hp, 3, (hp, 1 - cp)),
            'x_s': (xn, 4, (hp, 1 - cp)), 'y_s': (yn, 5, (hp, 1 - cp)), 'd_s': (dn, 6, (hp, 1 - cp)),
            'x_y': (xn, 2, (yn, cp)), 'y_x': (yn, 2, (xn, cp)),
        }[kind]
        number = ('own_x', 'own_y', 'own_s', 'x_s', 'y_s', 'd_s', 'x_y', 'y_x').index(kind)
        src = self.part(self.src, c) if kind.startswith('own') else self.place(origin, cp, c)
        return pltpu.make_async_remote_copy(
            src_ref=src, dst_ref=self.place(origin, cp, c), send_sem=self.send.at[number, c],
            recv_sem=self.recv.at[lands, c], device_id=to, device_id_type=MESH)

    def await_from(self, number, c):
        hp, cp = ((self.xn, self.cp), (self.yn, self.cp), (self.dn, self.cp), (self.hp, 1 - self.cp),
                  (self.xn, 1 - self.cp), (self.yn, 1 - self.cp), (self.dn, 1 - self.cp))[number]
        ref = self.place(hp, cp, c)
        pltpu.make_async_remote_copy(
            src_ref=ref, dst_ref=ref, send_sem=self.send.at[0, c], recv_sem=self.recv.at[number, c],
            device_id=(self.hp, 1 - self.cp), device_id_type=MESH).wait_recv()

    def start_own(self):
        for c in range(CHUNKS):
            for kind in ('own_x', 'own_y', 'own_s'):
                self.copy(kind, c).start()

    def relay_near(self, chunks=range(CHUNKS)):
        for c in chunks:
            self.await_from(0, c)
            self.copy('x_s', c).start()
            if c < CHUNKS // 2:
                self.copy('x_y', c).start()
            self.await_from(1, c)
            self.copy('y_s', c).start()
            if c >= CHUNKS // 2:
                self.copy('y_x', c).start()

    def relay_diagonal(self):
        for c in range(CHUNKS):
            self.await_from(2, c)
            self.copy('d_s', c).start()

    def await_sibling(self, number):
        for c in range(CHUNKS):
            self.await_from(number, c)

    def finish_sends(self):
        for c in range(CHUNKS):
            for kind in ('own_x', 'own_y', 'own_s', 'x_s', 'y_s', 'd_s'):
                self.copy(kind, c).wait_send()
            self.copy('x_y' if c < CHUNKS // 2 else 'y_x', c).wait_send()


def gather_sems():
    return [pltpu.SemaphoreType.DMA((8, CHUNKS)), pltpu.SemaphoreType.DMA((7, CHUNKS))]


def unpack_table(tab):
    group = lax.broadcasted_iota(jnp.int32, tab.shape, 1) // (DH // 2)
    turned = [tab] + [pltpu.roll(tab, 32 * i, 1) for i in (1, 2, 3)]

    def pick(order):
        out = turned[order[3]]
        for g in range(3):
            out = jnp.where(group == g, turned[order[g]], out)
        return out

    sign = jnp.where(group % 2 == 0, -1.0, 1.0)
    cos_t = jnp.concatenate([pick((0, 1, 2, 3)), pick((2, 3, 0, 1))], axis=0)
    sin_t = jnp.concatenate([pick((3, 0, 1, 2)) * sign, pick((1, 2, 3, 0)) * sign], axis=0)
    return cos_t, sin_t


def project_block(d, x, gain, wq_ref, wkv_ref, tab, ht_ref, q_ref, k_ref, v_ref):
    xf = x.astype(F32)
    inv = lax.rsqrt(jnp.mean(xf * xf, axis=-1, keepdims=True) + NORM_EPS)
    h = (xf * inv * gain).astype(BF16)
    ht_ref[:, rows_of(d)] = h.T
    dst = rows_of(seq_block(d))
    cos_t, sin_t = unpack_table(tab)
    y = dot(h, wq_ref[...])
    for p in range(HEADS // 2):
        qr = rope_pairs(y[:, 128 * p:128 * (p + 1)], cos_t, sin_t).astype(BF16)
        q_ref[2 * p, dst, :] = qr[:, :DH]
        q_ref[2 * p + 1, dst, :] = qr[:, DH:]
    kv = dot(h, wkv_ref[...])
    k_ref[dst, :] = rope_pairs(kv, cos_t, sin_t).astype(BF16)[:, :DH]
    v_ref[dst, :] = kv.astype(BF16)[:, DH:]


def attend_block(j, q_ref, k_ref, vt_ref, e_ref, m_ref, ot_ref, lse_ref):
    q4 = q_ref[:, rows_of(j), :].reshape(CW, DH)

    def score_tile(kb, carry, masked):
        m_old, l_old = carry
        s = nt_dot(k_ref[rows_of(kb), :], q4) * EXP2_SCALE
        if masked:
            s = jnp.where(causal_tile(), s, -1e30)
        m_new = jnp.maximum(m_old, jnp.max(s, axis=0, keepdims=True))
        e = jnp.exp2(s - m_new)
        e_ref[rows_of(kb), :] = e
        m_ref[pl.ds(kb, 1), :] = m_new
        return m_new, l_old * jnp.exp2(m_old - m_new) + jnp.sum(e, axis=0, keepdims=True)

    carry = (jnp.full((1, CW), -1e30, F32), jnp.zeros((1, CW), F32))
    carry = score_tile(j, carry, True)
    m_fin, l_fin = lax.fori_loop(0, j, functools.partial(score_tile, masked=False), carry)
    inv_l = 1.0 / l_fin
    lse = m_fin + jnp.log2(l_fin)

    def out_tile(kb, acc):
        f = jnp.exp2(m_ref[pl.ds(kb, 1), :] - m_fin) * inv_l
        p = (e_ref[rows_of(kb), :] * f).astype(BF16)
        return acc + dot(vt_ref[:, rows_of(kb)], p)

    acc = lax.fori_loop(0, j + 1, out_tile, jnp.zeros((DH, CW), F32)).astype(BF16)
    dst = rows_of(stored_block(j))
    for h in range(HEADS):
        ot_ref[DH * h:DH * (h + 1), dst] = acc[:, BLK * h:BLK * (h + 1)]
        lse_ref[h:h + 1, rows_of(j)] = lse[:, BLK * h:BLK * (h + 1)]


def forward_kernel(x_own, dy_own, gain_ref, wq_hbm, wk_hbm, wv_hbm, tab_own,
                   dy_all, ht_out, q_ref, k_ref, v_ref, ot_ref, lse_ref, tabs,
                   xg, ht, e_ref, m_ref, vt_ref, wq, wk, wv, wkv, stage,
                   local_sem, t_send, t_recv, x_send, x_recv, dy_send, dy_recv):
    hp, cp, xn, yn, dn = neighbours()
    mine = tok_slot(hp, cp)
    hw = HEADS * DH
    loads = [
        pltpu.make_async_copy(x_own, xg.at[mine], local_sem.at[0]),
        pltpu.make_async_copy(wq_hbm.at[:, pl.ds(pl.multiple_of(head_slot(hp, cp) * hw, hw), hw)], wq, local_sem.at[1]),
        pltpu.make_async_copy(wk_hbm.at[:, pl.ds(pl.multiple_of((hp // 2) * 128, 128), 128)], wk, local_sem.at[2]),
        pltpu.make_async_copy(wv_hbm.at[:, pl.ds(pl.multiple_of((hp // 2) * 128, 128), 128)], wv, local_sem.at[3]),
        pltpu.make_async_copy(dy_own, stage, local_sem.at[4]),
        pltpu.make_async_copy(tab_own, tabs.at[mine], local_sem.at[5]),
    ]
    for load in loads:
        load.start()
    enter_barrier()
    gx = Gather(x_own, xg, tok_slot, x_send, x_recv, BLK)
    gdy = Gather(dy_own, dy_all, tok_slot, dy_send, dy_recv, BLK)

    gt = Gather(tab_own, tabs, tok_slot, t_send, t_recv, 128)
    gt.start_own()
    gx.start_own()
    for load in loads[1:4]:
        load.wait()
    lane = lax.broadcasted_iota(jnp.int32, wk.shape, 1)
    swap = hp % 2 == 1
    kf, vf = wk[...].astype(F32), wv[...].astype(F32)
    k_sel = jnp.where(swap, pltpu.roll(kf, DH, 1), kf)
    v_sel = jnp.where(swap, vf, pltpu.roll(vf, DH, 1))
    wkv[...] = jnp.where(lane < DH, k_sel, v_sel).astype(BF16)
    for i in (0, 4, 5):
        loads[i].wait()
    dy_mine = pltpu.make_async_copy(stage, dy_all.at[mine], local_sem.at[6])
    dy_mine.start()
    def project(e, _):
        @pl.when(e == 1)
        def _():
            gt.await_sibling(3)
            gx.await_sibling(3)

        @pl.when(e == 2)
        def _():
            gt.relay_near()
            gx.relay_near()
            gdy.start_own()

        @pl.when(e == 3)
        def _():
            gt.await_sibling(4)
            gx.await_sibling(4)

        @pl.when(e == 5)
        def _():
            gt.await_sibling(5)
            gx.await_sibling(5)

        @pl.when(e == 6)
        def _():
            gt.relay_diagonal()
            gx.relay_diagonal()

        @pl.when(e == 7)
        def _():
            gt.await_sibling(6)
            gx.await_sibling(6)

        m, b = e // 2, e % 2
        px = (hp % 2 + m % 2) % 2
        py = (hp // 2 + m // 2) % 2
        d = tok_slot(py * 2 + px, (cp + b) % 2)
        project_block(d, xg[d], gain_ref[...], wq, wkv, tabs[d], ht, q_ref, k_ref, v_ref)
        return 0

    lax.fori_loop(0, NB, project, 0)
    ht_copy = pltpu.make_async_copy(ht, ht_out, local_sem.at[7])
    ht_copy.start()
    vt_ref[...] = v_ref[...].T

    def attend(j, _):
        for c in range(CHUNKS):
            @pl.when(j == (1, 3, 4, 5)[c])
            def _():
                gdy.relay_near((c,))

        attend_block(j, q_ref, k_ref, vt_ref, e_ref, m_ref, ot_ref, lse_ref)
        return 0

    lax.fori_loop(0, NB, attend, 0)
    gdy.relay_diagonal()
    for number in (3, 4, 5, 6):
        gdy.await_sibling(number)
    gt.finish_sends()
    gx.finish_sends()
    gdy.finish_sends()
    dy_mine.wait()
    ht_copy.wait()


def backward_kernel(dy_all, wo_hbm, q_ref, k_ref, v_ref, ot_ref, lse_ref, tabs,
                    gq_ref, ot_all,
                    dyv, wo, do_ref, kt_ref, dk_ref, dv_ref, give, take,
                    local_sem, o_send, o_recv, pair_send, pair_recv):
    hp, cp, xn, yn, dn = neighbours()
    mine = head_slot(hp, cp)
    hw = HEADS * DH
    wo_load = pltpu.make_async_copy(wo_hbm.at[pl.ds(pl.multiple_of(mine * hw, hw), hw)], wo, local_sem.at[NB])
    wo_load.start()
    for d in range(NB):
        pltpu.make_async_copy(dy_all.at[d], dyv.at[d], local_sem.at[d]).start()
    ot_mine = pltpu.make_async_copy(ot_ref, ot_all.at[mine], local_sem.at[NB + 1])
    ot_mine.start()
    enter_barrier()
    go = Gather(ot_ref, ot_all, head_slot, o_send, o_recv, hw)
    go.start_own()
    kt_ref[...] = k_ref[...].T
    dk_ref[...] = jnp.zeros_like(dk_ref)
    dv_ref[...] = jnp.zeros_like(dv_ref)
    wo_load.wait()

    def project(d, _):
        pltpu.make_async_copy(dy_all.at[d], dyv.at[d], local_sem.at[d]).wait()
        do = nt_dot(dyv[d], wo[...]).astype(BF16)
        dst = rows_of(seq_block(d))
        for h in range(HEADS):
            do_ref[h, dst, :] = do[:, DH * h:DH * (h + 1)]
        return 0

    lax.fori_loop(0, NB, project, 0)

    def attend(j, _):
        @pl.when(j == 5)
        def _():
            go.relay_near(range(0, CHUNKS // 2))

        @pl.when(j == 6)
        def _():
            go.relay_near(range(CHUNKS // 2, CHUNKS))

        slot = stored_block(j)
        src = rows_of(slot)
        q4 = q_ref[:, rows_of(j), :].reshape(CW, DH)
        do4 = do_ref[:, rows_of(j), :].reshape(CW, DH)
        o4t = jnp.concatenate([ot_ref[DH * h:DH * (h + 1), src] for h in range(HEADS)], axis=1)
        lse = jnp.concatenate([lse_ref[h:h + 1, rows_of(j)] for h in range(HEADS)], axis=1)
        delta = jnp.sum(do4.astype(F32).T * o4t.astype(F32), axis=0, keepdims=True)

        def tile(kb, dqt, masked):
            keys = rows_of(kb)
            p = jnp.exp2(nt_dot(k_ref[keys, :], q4) * EXP2_SCALE - lse)
            if masked:
                p = jnp.where(causal_tile(), p, 0.0)
            dp = nt_dot(v_ref[keys, :], do4)
            dv_ref[keys, :] += dot(p.astype(BF16), do4)
            ds = (p * (dp - delta)).astype(BF16)
            dk_ref[keys, :] += dot(ds, q4)
            return dqt + dot(kt_ref[:, keys], ds)

        dqt = tile(j, jnp.zeros((DH, CW), F32), True)
        dqt = lax.fori_loop(0, j, functools.partial(tile, masked=False), dqt) * (DH ** -0.5)
        cos_t, sin_t = unpack_table(tabs[slot])
        for p in range(HEADS // 2):
            pair = jnp.concatenate([dqt[:, BLK * (2 * p):BLK * (2 * p + 1)], dqt[:, BLK * (2 * p + 1):BLK * (2 * p + 2)]], axis=0)
            dq = pair.T.astype(BF16).astype(F32)
            gq_ref[src, 128 * p:128 * (p + 1)] = rope_pairs(dq, cos_t, -sin_t).astype(BF16)
        return 0

    lax.fori_loop(0, NB, attend, 0)
    give[:, :DH] = (dk_ref[...] * (DH ** -0.5)).astype(BF16)
    give[:, DH:] = dv_ref[...].astype(BF16)
    swap = pltpu.make_async_remote_copy(
        src_ref=give, dst_ref=take, send_sem=pair_send, recv_sem=pair_recv, device_id=(hp, 1 - cp), device_id_type=MESH)
    swap.start()
    go.relay_diagonal()
    swap.wait_recv()
    lane = lax.broadcasted_iota(jnp.int32, (BLK, 2 * DH), 1)
    for i in range(NB // 2):
        slot = cp * 4 + i
        src = rows_of(seq_block(slot))
        total = (give[src, :].astype(F32) + take[src, :].astype(F32)).astype(BF16).astype(F32)
        cos_t, sin_t = unpack_table(tabs[slot])
        turned = rope_pairs(total, cos_t, -sin_t)
        gq_ref[NB * BLK + (i % 2) * BLK:NB * BLK + (i % 2 + 1) * BLK, 128 * (i // 2):128 * (i // 2 + 1)] = jnp.where(lane < DH, turned, total).astype(BF16)
    for number in (3, 4, 5, 6):
        go.await_sibling(number)
    swap.wait_send()
    go.finish_sends()
    ot_mine.wait()


def wo_kernel(info, ot_ref, dy_ref, wo_ref, x_ref, gwo_ref, out_ref, o_mine):
    @pl.when(pl.program_id(0) == 0)
    def _():
        for d in range(NB):
            o_mine[:, BLK * d:BLK * (d + 1)] = ot_ref[d, :, rows_of(info[0])].T

    gwo_ref[...] = dot(ot_ref[...].reshape(NB * BLK, NB * BLK), dy_ref[...].reshape(NB * BLK, BLK))
    out_ref[...] = (x_ref[...].astype(F32) + dot(o_mine[...], wo_ref[...])).astype(BF16)


def near_kernel(info, ht_ref, own_ref, sib_ref, x_ref, y_ref, wq_ref, gwq_ref, acc_ref):
    e = pl.program_id(0)
    for i, g_ref in enumerate((own_ref, sib_ref, x_ref, y_ref)):
        @pl.when(e == i)
        def _():
            gwq_ref[...] = dot(ht_ref[...], g_ref[:NB * BLK, :])
            part = nt_dot(g_ref[rows_of(info[0]), :], wq_ref[...])
            acc_ref[...] = part if i == 0 else acc_ref[...] + part


def far_kernel(info, ht_ref, own_kv, sib_kv, x_kv, y_kv, sx_ref, sy_ref, da_ref, db_ref, sda_ref, sdb_ref,
               wq_ref, wk_ref, wv_ref, x_own, dy_own, gain_ref, acc_in, gwq_in,
               gwq_ref, gwk_ref, gwv_ref, gh_ref, gg_ref, acc, g_s, gkvg, bk, bv):
    e = pl.program_id(0)
    toks = NB * BLK

    @pl.when(e == 0)
    def _():
        acc[...] = acc_in[...]
        for i, ref in enumerate((own_kv, sib_kv, x_kv, y_kv)):
            gkvg[info[1 + i]] = ref[...]

    halves = ((sx_ref, None), (sy_ref, None), (da_ref, db_ref), (sda_ref, sdb_ref))
    for i, (first, second) in enumerate(halves):
        @pl.when(e == i)
        def _():
            if second is None:
                g_s[...] = first[...]
            else:
                half = first.shape[0]
                g_s[:half, :] = first[...]
                g_s[half:, :] = second[...]

    gkvg[info[5 + e]] = g_s[toks:, :]
    acc[...] += nt_dot(g_s[rows_of(info[0]), :], wq_ref[...])
    gwq_ref[...] = dot(ht_ref[...], g_s[:toks, :])

    @pl.when(e == 3)
    def _():
        for c in range(2):
            for r in range(2):
                dst = pl.ds((c * 2 + r) * 2 * BLK, 2 * BLK)
                for p in range(2):
                    even = gkvg[4 * p + c, :, 128 * r:128 * (r + 1)]
                    odd = gkvg[4 * p + 2 + c, :, 128 * r:128 * (r + 1)]
                    bk[dst, 128 * p:128 * (p + 1)] = jnp.concatenate([even[:, :DH], odd[:, :DH]], axis=1)
                    bv[dst, 128 * p:128 * (p + 1)] = jnp.concatenate([even[:, DH:], odd[:, DH:]], axis=1)
        gwk_ref[...] = dot(ht_ref[...], bk[...])
        gwv_ref[...] = dot(ht_ref[...], bv[...])
        mine = rows_of(info[0])
        d_norm = acc[...] + nt_dot(bk[mine, :], wk_ref[...]) + nt_dot(bv[mine, :], wv_ref[...])
        x = x_own[...].astype(F32)
        inv = lax.rsqrt(jnp.mean(x * x, axis=-1, keepdims=True) + NORM_EPS)
        x_hat = x * inv
        gg_ref[...] = jnp.sum(d_norm * x_hat, axis=0, keepdims=True)
        d_hat = d_norm * gain_ref[...]
        row_mean = jnp.mean(d_hat * x_hat, axis=-1, keepdims=True)
        gh_ref[...] = (dy_own[...].astype(F32) + inv * (d_hat - x_hat * row_mean)).astype(BF16)


def gain_kernel(part_ref, gg_ref, gains, send, recv):
    hp, cp = lax.axis_index('hp'), lax.axis_index('cp')
    mine = tok_slot(hp, cp)
    enter_barrier()

    def gain_copy(m):
        return pltpu.make_async_remote_copy(
            src_ref=part_ref, dst_ref=gains.at[mine], send_sem=send.at[m - 1], recv_sem=recv.at[m - 1],
            device_id=((hp + m // 2) % 4, (cp + m % 2) % 2), device_id_type=MESH)

    for m in range(1, NB):
        gain_copy(m).start()
    gains[mine] = part_ref[...]
    for m in range(1, NB):
        ref = gains.at[tok_slot((hp + 4 - m // 2) % 4, (cp + m % 2) % 2)]
        pltpu.make_async_remote_copy(
            src_ref=ref, dst_ref=ref, send_sem=send.at[m - 1], recv_sem=recv.at[m - 1],
            device_id=(hp, 1 - cp), device_id_type=MESH).wait_recv()
    total = gains[0]
    for d in range(1, NB):
        total = total + gains[d]
    gg_ref[...] = total
    for m in range(1, NB):
        gain_copy(m).wait_send()


VMEM_SPEC = pl.BlockSpec(memory_space=pltpu.VMEM)
ANY_SPEC = pl.BlockSpec(memory_space=pl.ANY)


def run_forward(x_own, dy_own, gain, w_q, w_k, w_v, tab):
    rows, width = x_own.shape
    toks = rows * NB
    hw = HEADS * DH
    return pl.pallas_call(
        forward_kernel,
        out_shape=(
            jax.ShapeDtypeStruct((NB, rows, width), BF16),
            jax.ShapeDtypeStruct((width, toks), BF16),
            jax.ShapeDtypeStruct((HEADS, toks, DH), BF16),
            jax.ShapeDtypeStruct((toks, DH), BF16),
            jax.ShapeDtypeStruct((toks, DH), BF16),
            jax.ShapeDtypeStruct((hw, toks), BF16),
            jax.ShapeDtypeStruct((HEADS, toks), F32),
            jax.ShapeDtypeStruct((NB, 128, 128), F32),
        ),
        in_specs=[ANY_SPEC, ANY_SPEC, VMEM_SPEC, ANY_SPEC, ANY_SPEC, ANY_SPEC, ANY_SPEC],
        out_specs=(ANY_SPEC, ANY_SPEC) + (VMEM_SPEC,) * 6,
        scratch_shapes=[
            pltpu.VMEM((NB, rows, width), BF16), pltpu.VMEM((width, toks), BF16),
            pltpu.VMEM((toks, CW), F32), pltpu.VMEM((NB, CW), F32), pltpu.VMEM((DH, toks), BF16),
            pltpu.VMEM((width, hw), BF16), pltpu.VMEM((width, 128), BF16), pltpu.VMEM((width, 128), BF16),
            pltpu.VMEM((width, 128), BF16), pltpu.VMEM((rows, width), BF16),
            pltpu.SemaphoreType.DMA((8,)),
        ] + gather_sems() + gather_sems() + gather_sems(),
        compiler_params=pltpu.CompilerParams(vmem_limit_bytes=60 * 1024 * 1024, collective_id=0, has_side_effects=True),
        cost_estimate=pl.CostEstimate(flops=30_000_000_000, bytes_accessed=20_000_000, transcendentals=0),
        name="attn_forward",
    )(x_own, dy_own, gain, w_q, w_k, w_v, tab)


def run_backward(dy_all, w_o, q, k, v, o_t, lse, tabs):
    _, rows, width = dy_all.shape
    toks = rows * NB
    hw = HEADS * DH
    return pl.pallas_call(
        backward_kernel,
        out_shape=(
            jax.ShapeDtypeStruct((toks + 2 * BLK, hw), BF16),
            jax.ShapeDtypeStruct((NB, hw, toks), BF16),
        ),
        in_specs=[ANY_SPEC, ANY_SPEC] + [VMEM_SPEC] * 6,
        out_specs=(VMEM_SPEC, ANY_SPEC),
        scratch_shapes=[
            pltpu.VMEM((NB, rows, width), BF16), pltpu.VMEM((hw, width), BF16),
            pltpu.VMEM((HEADS, toks, DH), BF16), pltpu.VMEM((DH, toks), BF16),
            pltpu.VMEM((toks, DH), F32), pltpu.VMEM((toks, DH), F32),
            pltpu.VMEM((toks, 2 * DH), BF16), pltpu.VMEM((toks, 2 * DH), BF16),
            pltpu.SemaphoreType.DMA((NB + 2,)),
        ] + gather_sems() + [pltpu.SemaphoreType.DMA, pltpu.SemaphoreType.DMA],
        compiler_params=pltpu.CompilerParams(vmem_limit_bytes=60 * 1024 * 1024, collective_id=1, has_side_effects=True),
        cost_estimate=pl.CostEstimate(flops=40_000_000_000, bytes_accessed=20_000_000, transcendentals=0),
        name="attn_backward",
    )(dy_all, w_o, q, k, v, o_t, lse, tabs)


def grid_call(kernel, steps, info, args, in_specs, out_shape, out_specs, scratch, flops, name, aliases=None):
    return pl.pallas_call(
        kernel,
        out_shape=out_shape,
        grid_spec=pltpu.PrefetchScalarGridSpec(
            num_scalar_prefetch=1, grid=(steps,), in_specs=in_specs, out_specs=out_specs, scratch_shapes=scratch),
        input_output_aliases=aliases or {},
        compiler_params=pltpu.CompilerParams(vmem_limit_bytes=60 * 1024 * 1024),
        cost_estimate=pl.CostEstimate(flops=flops, bytes_accessed=40_000_000, transcendentals=0),
        name=name,
    )(info, *args)


def whole_block(a):
    return pl.BlockSpec(a.shape, lambda n, info: (0,) * len(a.shape))


def run_wo(info, ot_all, dy_all, w_o, x_own):
    rows, width = x_own.shape
    hw = HEADS * DH
    cols = lambda r: pl.BlockSpec((r, BLK), lambda n, info: (0, n))
    return grid_call(
        wo_kernel, NB, info, (ot_all, dy_all, w_o, x_own),
        [VMEM_SPEC, pl.BlockSpec((NB, rows, BLK), lambda n, info: (0, 0, n)), cols(NB * hw), cols(rows)],
        (jax.ShapeDtypeStruct((NB * hw, width), F32), jax.ShapeDtypeStruct((rows, width), BF16)),
        (cols(NB * hw), cols(rows)), [pltpu.VMEM((rows, NB * hw), BF16)], 20_000_000_000, "wo_grad")


def run_near(info, h_t, own, sib, x, y, w_q):
    width, toks = h_t.shape
    cols = pl.BlockSpec((width, BLK), lambda n, info: (0, info[1 + n]))
    acc = jax.ShapeDtypeStruct((BLK, width), F32)
    return grid_call(
        near_kernel, 4, info, (h_t, own, sib, x, y, w_q), [VMEM_SPEC] * 5 + [cols],
        (jax.ShapeDtypeStruct((width, NB * BLK), F32), acc), (cols, whole_block(acc)), [], 10_000_000_000, "wq_near")


def run_far(info, h_t, near, sx, sy, d_a, d_b, sd_a, sd_b, w_q, w_k, w_v, x_own, dy_own, gain, acc, gwq):
    width, toks = h_t.shape
    rows, kv = x_own.shape[0], w_k.shape[1]
    cols = pl.BlockSpec((width, BLK), lambda n, info: (0, info[5 + n]))
    kv_rows = pl.BlockSpec((2 * BLK, BLK), lambda n, info: (NB // 2, 0))
    outs = (jax.ShapeDtypeStruct((width, NB * BLK), F32), jax.ShapeDtypeStruct((width, kv), F32), jax.ShapeDtypeStruct((width, kv), F32),
            jax.ShapeDtypeStruct((rows, width), BF16), jax.ShapeDtypeStruct((1, width), F32))
    return grid_call(
        far_kernel, 4, info,
        (h_t, *near, sx, sy, d_a, d_b, sd_a, sd_b, w_q, w_k, w_v, x_own, dy_own, gain, acc, gwq),
        [VMEM_SPEC] + [kv_rows] * 4 + [VMEM_SPEC] * 6 + [cols] + [VMEM_SPEC] * 6 + [ANY_SPEC],
        outs, (cols,) + tuple(whole_block(o) for o in outs[1:]),
        [pltpu.VMEM((rows, width), F32), pltpu.VMEM((toks + 2 * BLK, BLK), BF16), pltpu.VMEM((NB, 2 * BLK, BLK), BF16),
         pltpu.VMEM((toks, kv), BF16), pltpu.VMEM((toks, kv), BF16)],
        15_000_000_000, "wq_far", aliases={19: 0})


def run_gain(part):
    dma = pltpu.SemaphoreType.DMA
    return pl.pallas_call(
        gain_kernel, out_shape=jax.ShapeDtypeStruct(part.shape, F32), in_specs=[VMEM_SPEC], out_specs=VMEM_SPEC,
        scratch_shapes=[pltpu.VMEM((NB,) + part.shape, F32), dma((7,)), dma((7,))],
        compiler_params=pltpu.CompilerParams(collective_id=2, has_side_effects=True), name="gain_sum")(part)


def solution(mesh):
    def device_step(hidden, grad_out, positions, norm_gain, w_q, w_k, w_v, w_o, inv_freq):
        angles = positions.astype(F32)[:, None] * inv_freq[None, :]
        cos_h, sin_h = jnp.cos(angles), jnp.sin(angles)
        tab = jnp.concatenate([cos_h[:128], sin_h[:128], cos_h[128:], sin_h[128:]], axis=1)
        gain = norm_gain.astype(F32)[None, :]
        dy_all, h_t, q, k, v, o_t, lse, tabs = run_forward(hidden, grad_out, gain, w_q, w_k, w_v, tab)
        g, ot_all = run_backward(dy_all, w_o, q, k, v, o_t, lse, tabs)
        hp, cp, xn, yn, dn = neighbours()
        slots = [head_slot(a, b) for a, b in ((hp, cp), (hp, 1 - cp), (xn, cp), (yn, cp), (xn, 1 - cp), (yn, 1 - cp), (dn, cp), (dn, 1 - cp))]
        info = jnp.stack([tok_slot(hp, cp)] + slots).astype(jnp.int32)
        along_x = lambda a: lax.ppermute(a, 'hp', [(i, i ^ 1) for i in range(4)])
        along_y = lambda a: lax.ppermute(a, 'hp', [(i, i ^ 2) for i in range(4)])
        to_sib = lambda a: lax.ppermute(a, 'cp', [(0, 1), (1, 0)])
        half = g.shape[0] // 2
        x, y, sib = along_x(g), along_y(g), to_sib(g)
        grad_wo, output = run_wo(info, ot_all, dy_all, w_o, hidden)
        x, y, sib, output = lax.optimization_barrier((x, y, sib, output))
        d_a, d_b = along_y(x[:half]), along_x(y[half:])
        sx, sy = to_sib(x), to_sib(y)
        gwq, acc = run_near(info, h_t, g, sib, x, y, w_q)
        d_a, d_b, acc = lax.optimization_barrier((d_a, d_b, acc))
        sd_a, sd_b = to_sib(d_a), to_sib(d_b)
        grad_wq, grad_wk, grad_wv, grad_hidden, part = run_far(
            info, h_t, (g, sib, x, y), sx, sy, d_a, d_b, sd_a, sd_b, w_q, w_k, w_v, hidden, grad_out, gain, acc, gwq)
        grad_gain = run_gain(part)
        return output, grad_hidden, grad_wq, grad_wk, grad_wv, grad_wo, grad_gain[0]

    seq_spec = P(('cp', 'hp'), None)
    whole = P()
    return jax.shard_map(device_step, mesh=mesh, in_specs=(seq_spec, seq_spec, P(('cp', 'hp')), whole, whole, whole, whole, whole, whole), out_specs=(seq_spec, seq_spec, whole, whole, whole, whole, whole), check_vma=False)
```

```python
import functools
import math

import jax
import jax.numpy as jnp
from jax import lax
from jax.experimental import pallas as pl
from jax.experimental.pallas import tpu as pltpu
from jax.sharding import PartitionSpec as P

NORM_EPS = 1e-5
BLK = 256
HEADS = 4
DH = 64
NB = 8
CW = HEADS * BLK
EXP2_SCALE = (DH ** -0.5) * math.log2(math.e)
F32 = jnp.float32
BF16 = jnp.bfloat16


def seq_block(d):
    cp, half, sub = d // 4, (d // 2) % 2, d % 2
    return 2 * ((1 - half) * cp + half * (3 - cp)) + sub


def stored_block(j):
    b, sub = j // 2, j % 2
    half = b // 2
    cp = (1 - half) * b + half * (3 - b)
    return cp * 4 + half * 2 + sub


def nt_dot(a, b):
    return lax.dot_general(a, b, (((1,), (1,)), ((), ())), preferred_element_type=F32)


def dot(a, b):
    return jnp.dot(a, b, preferred_element_type=F32)


def rope_pairs(t, cos_t, sin_t):
    lane = lax.broadcasted_iota(jnp.int32, t.shape, 1)
    partner = jnp.where(lane % DH < DH // 2, pltpu.roll(t, 128 - DH // 2, 1), pltpu.roll(t, DH // 2, 1))
    return t * cos_t + partner * sin_t


def rows_of(b):
    return pl.ds(pl.multiple_of(b * BLK, BLK), BLK)


def causal_tile():
    row = lax.broadcasted_iota(jnp.int32, (BLK, CW), 0)
    col = lax.broadcasted_iota(jnp.int32, (BLK, CW), 1)
    return row <= col % BLK


MESH = pl.DeviceIdType.MESH
CHUNKS = 4


def neighbours():
    hp, cp = lax.axis_index('hp'), lax.axis_index('cp')
    flip = 1 - 2 * (hp % 2)
    y_hp = (hp + 2) % 4
    return hp, cp, hp + flip, y_hp, y_hp + flip


def tok_slot(hp, cp):
    return cp * 4 + hp


def head_slot(hp, cp):
    return hp * 2 + cp


def enter_barrier():
    hp, cp = lax.axis_index('hp'), lax.axis_index('cp')
    barrier = pltpu.get_barrier_semaphore()
    for m in range(1, 8):
        pl.semaphore_signal(barrier, inc=1, device_id=((hp + m // 2) % 4, (cp + m % 2) % 2), device_id_type=MESH)
    pl.semaphore_wait(barrier, 7)


class Gather:
    def __init__(self, src, dst, slot, send, recv, rows):
        self.src, self.dst, self.slot, self.send, self.recv = src, dst, slot, send, recv
        self.step = rows // CHUNKS
        self.hp, self.cp, self.xn, self.yn, self.dn = neighbours()

    def part(self, ref, c):
        return ref.at[pl.ds(c * self.step, self.step)]

    def place(self, hp, cp, c):
        return self.part(self.dst.at[self.slot(hp, cp)], c)

    def copy(self, kind, c):
        hp, cp, xn, yn, dn = self.hp, self.cp, self.xn, self.yn, self.dn
        origin, lands, to = {
            'own_x': (hp, 0, (xn, cp)), 'own_y': (hp, 1, (yn, cp)), 'own_s': (hp, 3, (hp, 1 - cp)),
            'x_s': (xn, 4, (hp, 1 - cp)), 'y_s': (yn, 5, (hp, 1 - cp)), 'd_s': (dn, 6, (hp, 1 - cp)),
            'x_y': (xn, 2, (yn, cp)), 'y_x': (yn, 2, (xn, cp)),
        }[kind]
        number = ('own_x', 'own_y', 'own_s', 'x_s', 'y_s', 'd_s', 'x_y', 'y_x').index(kind)
        src = self.part(self.src, c) if kind.startswith('own') else self.place(origin, cp, c)
        return pltpu.make_async_remote_copy(
            src_ref=src, dst_ref=self.place(origin, cp, c), send_sem=self.send.at[number, c],
            recv_sem=self.recv.at[lands, c], device_id=to, device_id_type=MESH)

    def await_from(self, number, c):
        hp, cp = ((self.xn, self.cp), (self.yn, self.cp), (self.dn, self.cp), (self.hp, 1 - self.cp),
                  (self.xn, 1 - self.cp), (self.yn, 1 - self.cp), (self.dn, 1 - self.cp))[number]
        ref = self.place(hp, cp, c)
        pltpu.make_async_remote_copy(
            src_ref=ref, dst_ref=ref, send_sem=self.send.at[0, c], recv_sem=self.recv.at[number, c],
            device_id=(self.hp, 1 - self.cp), device_id_type=MESH).wait_recv()

    def start_own(self):
        for c in range(CHUNKS):
            for kind in ('own_x', 'own_y', 'own_s'):
                self.copy(kind, c).start()

    def relay_near(self, chunks=range(CHUNKS)):
        for c in chunks:
            self.await_from(0, c)
            self.copy('x_s', c).start()
            if c < CHUNKS // 2:
                self.copy('x_y', c).start()
            self.await_from(1, c)
            self.copy('y_s', c).start()
            if c >= CHUNKS // 2:
                self.copy('y_x', c).start()

    def relay_diagonal(self):
        for c in range(CHUNKS):
            self.await_from(2, c)
            self.copy('d_s', c).start()

    def await_sibling(self, number):
        for c in range(CHUNKS):
            self.await_from(number, c)

    def finish_sends(self):
        for c in range(CHUNKS):
            for kind in ('own_x', 'own_y', 'own_s', 'x_s', 'y_s', 'd_s'):
                self.copy(kind, c).wait_send()
            self.copy('x_y' if c < CHUNKS // 2 else 'y_x', c).wait_send()


def gather_sems():
    return [pltpu.SemaphoreType.DMA((8, CHUNKS)), pltpu.SemaphoreType.DMA((7, CHUNKS))]


def unpack_table(tab):
    group = lax.broadcasted_iota(jnp.int32, tab.shape, 1) // (DH // 2)
    turned = [tab] + [pltpu.roll(tab, 32 * i, 1) for i in (1, 2, 3)]

    def pick(order):
        out = turned[order[3]]
        for g in range(3):
            out = jnp.where(group == g, turned[order[g]], out)
        return out

    sign = jnp.where(group % 2 == 0, -1.0, 1.0)
    cos_t = jnp.concatenate([pick((0, 1, 2, 3)), pick((2, 3, 0, 1))], axis=0)
    sin_t = jnp.concatenate([pick((3, 0, 1, 2)) * sign, pick((1, 2, 3, 0)) * sign], axis=0)
    return cos_t, sin_t


def project_block(d, x, gain, wq_ref, wkv_ref, tab, ht_ref, q_ref, k_ref, v_ref):
    xf = x.astype(F32)
    inv = lax.rsqrt(jnp.mean(xf * xf, axis=-1, keepdims=True) + NORM_EPS)
    h = (xf * inv * gain).astype(BF16)
    ht_ref[:, rows_of(d)] = h.T
    dst = rows_of(seq_block(d))
    cos_t, sin_t = unpack_table(tab)
    y = dot(h, wq_ref[...])
    for p in range(HEADS // 2):
        qr = rope_pairs(y[:, 128 * p:128 * (p + 1)], cos_t, sin_t).astype(BF16)
        q_ref[2 * p, dst, :] = qr[:, :DH]
        q_ref[2 * p + 1, dst, :] = qr[:, DH:]
    kv = dot(h, wkv_ref[...])
    k_ref[dst, :] = rope_pairs(kv, cos_t, sin_t).astype(BF16)[:, :DH]
    v_ref[dst, :] = kv.astype(BF16)[:, DH:]


def attend_block(j, q_ref, k_ref, vt_ref, e_ref, m_ref, ot_ref, lse_ref):
    q4 = q_ref[:, rows_of(j), :].reshape(CW, DH)

    def score_tile(kb, carry, masked):
        m_old, l_old = carry
        s = nt_dot(k_ref[rows_of(kb), :], q4) * EXP2_SCALE
        if masked:
            s = jnp.where(causal_tile(), s, -1e30)
        m_new = jnp.maximum(m_old, jnp.max(s, axis=0, keepdims=True))
        e = jnp.exp2(s - m_new)
        e_ref[rows_of(kb), :] = e
        m_ref[pl.ds(kb, 1), :] = m_new
        return m_new, l_old * jnp.exp2(m_old - m_new) + jnp.sum(e, axis=0, keepdims=True)

    carry = (jnp.full((1, CW), -1e30, F32), jnp.zeros((1, CW), F32))
    carry = score_tile(j, carry, True)
    m_fin, l_fin = lax.fori_loop(0, j, functools.partial(score_tile, masked=False), carry)
    inv_l = 1.0 / l_fin
    lse = m_fin + jnp.log2(l_fin)

    def out_tile(kb, acc):
        f = jnp.exp2(m_ref[pl.ds(kb, 1), :] - m_fin) * inv_l
        p = (e_ref[rows_of(kb), :] * f).astype(BF16)
        return acc + dot(vt_ref[:, rows_of(kb)], p)

    acc = lax.fori_loop(0, j + 1, out_tile, jnp.zeros((DH, CW), F32)).astype(BF16)
    dst = rows_of(stored_block(j))
    for h in range(HEADS):
        ot_ref[DH * h:DH * (h + 1), dst] = acc[:, BLK * h:BLK * (h + 1)]
        lse_ref[h:h + 1, rows_of(j)] = lse[:, BLK * h:BLK * (h + 1)]


def nth_peer(e):
    hp, cp = lax.axis_index('hp'), lax.axis_index('cp')
    m, b = e // 2, e % 2
    px = (hp % 2 + m % 2) % 2
    py = (hp // 2 + m // 2) % 2
    return py * 2 + px, (cp + b) % 2


def attention_kernel(x_own, dy_own, gain_ref, wq_hbm, wk_hbm, wv_hbm, wo_hbm, tab_own,
                     dy_all, ht_out, gq_ref, ot_all,
                     xg, ht, e_ref, m_ref, vt_ref, wq, wk, wv, wkv, stage, q_ref, k_ref, v_ref, ot_ref, lse_ref, tabs,
                     wo, do_ref, kt_ref, dk_ref, dv_ref, give, take,
                     local_sem, dy_sem, t_send, t_recv, x_send, x_recv, dy_send, dy_recv, o_send, o_recv, pair_send, pair_recv):
    hp, cp, xn, yn, dn = neighbours()
    mine = tok_slot(hp, cp)
    hw = HEADS * DH
    loads = [
        pltpu.make_async_copy(x_own, xg.at[mine], local_sem.at[0]),
        pltpu.make_async_copy(wq_hbm.at[:, pl.ds(pl.multiple_of(head_slot(hp, cp) * hw, hw), hw)], wq, local_sem.at[1]),
        pltpu.make_async_copy(wk_hbm.at[:, pl.ds(pl.multiple_of((hp // 2) * 128, 128), 128)], wk, local_sem.at[2]),
        pltpu.make_async_copy(wv_hbm.at[:, pl.ds(pl.multiple_of((hp // 2) * 128, 128), 128)], wv, local_sem.at[3]),
        pltpu.make_async_copy(dy_own, stage, local_sem.at[4]),
        pltpu.make_async_copy(tab_own, tabs.at[mine], local_sem.at[5]),
    ]
    for load in loads:
        load.start()
    wo_load = pltpu.make_async_copy(wo_hbm.at[pl.ds(pl.multiple_of(head_slot(hp, cp) * hw, hw), hw)], wo, local_sem.at[8])
    wo_load.start()
    enter_barrier()
    gx = Gather(x_own, xg, tok_slot, x_send, x_recv, BLK)
    gdy = Gather(dy_own, dy_all, tok_slot, dy_send, dy_recv, BLK)

    gt = Gather(tab_own, tabs, tok_slot, t_send, t_recv, 128)
    gt.start_own()
    gx.start_own()
    for load in loads[1:4]:
        load.wait()
    lane = lax.broadcasted_iota(jnp.int32, wk.shape, 1)
    swap = hp % 2 == 1
    kf, vf = wk[...].astype(F32), wv[...].astype(F32)
    k_sel = jnp.where(swap, pltpu.roll(kf, DH, 1), kf)
    v_sel = jnp.where(swap, vf, pltpu.roll(vf, DH, 1))
    wkv[...] = jnp.where(lane < DH, k_sel, v_sel).astype(BF16)
    for i in (0, 4, 5):
        loads[i].wait()
    dy_mine = pltpu.make_async_copy(stage, dy_all.at[mine], local_sem.at[6])
    dy_mine.start()
    def project(e, _):
        @pl.when(e == 1)
        def _():
            gt.await_sibling(3)
            gx.await_sibling(3)

        @pl.when(e == 2)
        def _():
            gt.relay_near()
            gx.relay_near()
            gdy.start_own()

        @pl.when(e == 3)
        def _():
            gt.await_sibling(4)
            gx.await_sibling(4)

        @pl.when(e == 5)
        def _():
            gt.await_sibling(5)
            gx.await_sibling(5)

        @pl.when(e == 6)
        def _():
            gt.relay_diagonal()
            gx.relay_diagonal()

        @pl.when(e == 7)
        def _():
            gt.await_sibling(6)
            gx.await_sibling(6)

        d = tok_slot(*nth_peer(e))
        project_block(d, xg[d], gain_ref[...], wq, wkv, tabs[d], ht, q_ref, k_ref, v_ref)
        return 0

    lax.fori_loop(0, NB, project, 0)
    ht_copy = pltpu.make_async_copy(ht, ht_out, local_sem.at[7])
    ht_copy.start()
    vt_ref[...] = v_ref[...].T

    def attend(j, _):
        for c in range(CHUNKS):
            @pl.when(j == (1, 3, 5, 6)[c])
            def _():
                gdy.relay_near((c,))

        attend_block(j, q_ref, k_ref, vt_ref, e_ref, m_ref, ot_ref, lse_ref)
        return 0

    lax.fori_loop(0, NB, attend, 0)
    go = Gather(ot_ref, ot_all, head_slot, o_send, o_recv, hw)
    kt_ref[...] = k_ref[...].T
    dk_ref[...] = jnp.zeros_like(dk_ref)
    dv_ref[...] = jnp.zeros_like(dv_ref)
    go.start_own()
    ot_mine = pltpu.make_async_copy(ot_ref, ot_all.at[head_slot(hp, cp)], local_sem.at[9])
    ot_mine.start()
    wo_load.wait()
    gx.finish_sends()
    dy_mine.wait()

    def dy_load(e):
        d = tok_slot(*nth_peer(e))
        return pltpu.make_async_copy(dy_all.at[d], xg.at[d], dy_sem.at[e])

    def project_dy(e, _):
        dy_load(e).wait()
        d = tok_slot(*nth_peer(e))
        do = nt_dot(xg[d], wo[...]).astype(BF16)
        dst = rows_of(seq_block(d))
        for h in range(HEADS):
            do_ref[h, dst, :] = do[:, DH * h:DH * (h + 1)]
        return 0

    for number in (3, 4, 5):
        gdy.await_sibling(number)
    for e in range(6):
        dy_load(e).start()
    lax.fori_loop(0, 6, project_dy, 0)
    gdy.relay_diagonal()
    dy_load(6).start()
    gdy.await_sibling(6)
    dy_load(7).start()
    lax.fori_loop(6, NB, project_dy, 0)

    def attend_back(j, _):
        for c in range(CHUNKS):
            @pl.when(j == (2, 4, 5, 6)[c])
            def _():
                go.relay_near((c,))

        slot = stored_block(j)
        src = rows_of(slot)
        q4 = q_ref[:, rows_of(j), :].reshape(CW, DH)
        do4 = do_ref[:, rows_of(j), :].reshape(CW, DH)
        o4t = jnp.concatenate([ot_ref[DH * h:DH * (h + 1), src] for h in range(HEADS)], axis=1)
        lse = jnp.concatenate([lse_ref[h:h + 1, rows_of(j)] for h in range(HEADS)], axis=1)
        delta = jnp.sum(do4.astype(F32).T * o4t.astype(F32), axis=0, keepdims=True)

        def tile(kb, dqt, masked):
            keys = rows_of(kb)
            p = jnp.exp2(nt_dot(k_ref[keys, :], q4) * EXP2_SCALE - lse)
            if masked:
                p = jnp.where(causal_tile(), p, 0.0)
            dp = nt_dot(v_ref[keys, :], do4)
            dv_ref[keys, :] += dot(p.astype(BF16), do4)
            ds = (p * (dp - delta)).astype(BF16)
            dk_ref[keys, :] += dot(ds, q4)
            return dqt + dot(kt_ref[:, keys], ds)

        dqt = tile(j, jnp.zeros((DH, CW), F32), True)
        dqt = lax.fori_loop(0, j, functools.partial(tile, masked=False), dqt) * (DH ** -0.5)
        cos_t, sin_t = unpack_table(tabs[slot])
        for p in range(HEADS // 2):
            pair = jnp.concatenate([dqt[:, BLK * (2 * p):BLK * (2 * p + 1)], dqt[:, BLK * (2 * p + 1):BLK * (2 * p + 2)]], axis=0)
            dq = pair.T.astype(BF16).astype(F32)
            gq_ref[src, 128 * p:128 * (p + 1)] = rope_pairs(dq, cos_t, -sin_t).astype(BF16)
        return 0

    lax.fori_loop(0, NB, attend_back, 0)
    give[:, :DH] = (dk_ref[...] * (DH ** -0.5)).astype(BF16)
    give[:, DH:] = dv_ref[...].astype(BF16)
    swap = pltpu.make_async_remote_copy(
        src_ref=give, dst_ref=take, send_sem=pair_send, recv_sem=pair_recv, device_id=(hp, 1 - cp), device_id_type=MESH)
    go.relay_diagonal()
    swap.start()
    for number in (3, 4, 5):
        go.await_sibling(number)
    swap.wait_recv()
    lane = lax.broadcasted_iota(jnp.int32, (BLK, 2 * DH), 1)
    for i in range(NB // 2):
        slot = cp * 4 + i
        src = rows_of(seq_block(slot))
        total = (give[src, :].astype(F32) + take[src, :].astype(F32)).astype(BF16).astype(F32)
        cos_t, sin_t = unpack_table(tabs[slot])
        turned = rope_pairs(total, cos_t, -sin_t)
        gq_ref[NB * BLK + (i % 2) * BLK:NB * BLK + (i % 2 + 1) * BLK, 128 * (i // 2):128 * (i // 2 + 1)] = jnp.where(lane < DH, turned, total).astype(BF16)
    go.await_sibling(6)
    swap.wait_send()
    go.finish_sends()
    ot_mine.wait()
    gt.finish_sends()
    gdy.finish_sends()
    ht_copy.wait()


def wo_kernel(info, ot_ref, dy_ref, wo_ref, x_ref, gwo_ref, out_ref, o_mine):
    @pl.when(pl.program_id(0) == 0)
    def _():
        for d in range(NB):
            o_mine[:, BLK * d:BLK * (d + 1)] = ot_ref[d, :, rows_of(info[0])].T

    gwo_ref[...] = dot(ot_ref[...].reshape(NB * BLK, NB * BLK), dy_ref[...].reshape(NB * BLK, BLK))
    out_ref[...] = (x_ref[...].astype(F32) + dot(o_mine[...], wo_ref[...])).astype(BF16)


def near_kernel(info, ht_ref, own_ref, sib_ref, x_ref, y_ref, wq_ref, gwq_ref, acc_ref):
    e = pl.program_id(0)
    for i, g_ref in enumerate((own_ref, sib_ref, x_ref, y_ref)):
        @pl.when(e == i)
        def _():
            gwq_ref[...] = dot(ht_ref[...], g_ref[:NB * BLK, :])
            part = nt_dot(g_ref[rows_of(info[0]), :], wq_ref[...])
            acc_ref[...] = part if i == 0 else acc_ref[...] + part


def far_kernel(info, ht_ref, own_kv, sib_kv, x_kv, y_kv, sx_ref, sy_ref, da_ref, db_ref, sda_ref, sdb_ref,
               wq_ref, wk_ref, wv_ref, x_own, dy_own, gain_ref, acc_in, gwq_in,
               gwq_ref, gwk_ref, gwv_ref, gh_ref, gg_ref, acc, g_s, gkvg, bk, bv):
    e = pl.program_id(0)
    toks = NB * BLK

    @pl.when(e == 0)
    def _():
        acc[...] = acc_in[...]
        for i, ref in enumerate((own_kv, sib_kv, x_kv, y_kv)):
            gkvg[info[1 + i]] = ref[...]

    halves = ((sx_ref, None), (sy_ref, None), (da_ref, db_ref), (sda_ref, sdb_ref))
    for i, (first, second) in enumerate(halves):
        @pl.when(e == i)
        def _():
            if second is None:
                g_s[...] = first[...]
            else:
                half = first.shape[0]
                g_s[:half, :] = first[...]
                g_s[half:, :] = second[...]

    gkvg[info[5 + e]] = g_s[toks:, :]
    acc[...] += nt_dot(g_s[rows_of(info[0]), :], wq_ref[...])
    gwq_ref[...] = dot(ht_ref[...], g_s[:toks, :])

    @pl.when(e == 3)
    def _():
        for c in range(2):
            for r in range(2):
                dst = pl.ds((c * 2 + r) * 2 * BLK, 2 * BLK)
                for p in range(2):
                    even = gkvg[4 * p + c, :, 128 * r:128 * (r + 1)]
                    odd = gkvg[4 * p + 2 + c, :, 128 * r:128 * (r + 1)]
                    bk[dst, 128 * p:128 * (p + 1)] = jnp.concatenate([even[:, :DH], odd[:, :DH]], axis=1)
                    bv[dst, 128 * p:128 * (p + 1)] = jnp.concatenate([even[:, DH:], odd[:, DH:]], axis=1)
        gwk_ref[...] = dot(ht_ref[...], bk[...])
        gwv_ref[...] = dot(ht_ref[...], bv[...])
        mine = rows_of(info[0])
        d_norm = acc[...] + nt_dot(bk[mine, :], wk_ref[...]) + nt_dot(bv[mine, :], wv_ref[...])
        x = x_own[...].astype(F32)
        inv = lax.rsqrt(jnp.mean(x * x, axis=-1, keepdims=True) + NORM_EPS)
        x_hat = x * inv
        gg_ref[...] = jnp.sum(d_norm * x_hat, axis=0, keepdims=True)
        d_hat = d_norm * gain_ref[...]
        row_mean = jnp.mean(d_hat * x_hat, axis=-1, keepdims=True)
        gh_ref[...] = (dy_own[...].astype(F32) + inv * (d_hat - x_hat * row_mean)).astype(BF16)


def gain_kernel(part_ref, gg_ref, gains, send, recv):
    hp, cp = lax.axis_index('hp'), lax.axis_index('cp')
    mine = tok_slot(hp, cp)
    enter_barrier()

    def gain_copy(m):
        return pltpu.make_async_remote_copy(
            src_ref=part_ref, dst_ref=gains.at[mine], send_sem=send.at[m - 1], recv_sem=recv.at[m - 1],
            device_id=((hp + m // 2) % 4, (cp + m % 2) % 2), device_id_type=MESH)

    for m in range(1, NB):
        gain_copy(m).start()
    gains[mine] = part_ref[...]
    for m in range(1, NB):
        ref = gains.at[tok_slot((hp + 4 - m // 2) % 4, (cp + m % 2) % 2)]
        pltpu.make_async_remote_copy(
            src_ref=ref, dst_ref=ref, send_sem=send.at[m - 1], recv_sem=recv.at[m - 1],
            device_id=(hp, 1 - cp), device_id_type=MESH).wait_recv()
    total = gains[0]
    for d in range(1, NB):
        total = total + gains[d]
    gg_ref[...] = total
    for m in range(1, NB):
        gain_copy(m).wait_send()


VMEM_SPEC = pl.BlockSpec(memory_space=pltpu.VMEM)
ANY_SPEC = pl.BlockSpec(memory_space=pl.ANY)


def run_attention(x_own, dy_own, gain, w_q, w_k, w_v, w_o, tab):
    rows, width = x_own.shape
    toks = rows * NB
    hw = HEADS * DH
    dma = pltpu.SemaphoreType.DMA
    b16 = lambda *shape: pltpu.VMEM(shape, BF16)
    f32 = lambda *shape: pltpu.VMEM(shape, F32)
    return pl.pallas_call(
        attention_kernel,
        out_shape=(
            jax.ShapeDtypeStruct((NB, rows, width), BF16),
            jax.ShapeDtypeStruct((width, toks), BF16),
            jax.ShapeDtypeStruct((toks + 2 * BLK, hw), BF16),
            jax.ShapeDtypeStruct((NB, hw, toks), BF16),
        ),
        in_specs=[ANY_SPEC, ANY_SPEC, VMEM_SPEC] + [ANY_SPEC] * 5,
        out_specs=(ANY_SPEC, ANY_SPEC, VMEM_SPEC, ANY_SPEC),
        scratch_shapes=[
            b16(NB, rows, width), b16(width, toks), f32(toks, CW), f32(NB, CW), b16(DH, toks),
            b16(width, hw), b16(width, 128), b16(width, 128), b16(width, 128), b16(rows, width),
            b16(HEADS, toks, DH), b16(toks, DH), b16(toks, DH), b16(hw, toks), f32(HEADS, toks), f32(NB, 128, 128),
            b16(hw, width), b16(HEADS, toks, DH), b16(DH, toks), f32(toks, DH), f32(toks, DH), b16(toks, 2 * DH), b16(toks, 2 * DH),
            dma((10,)), dma((NB,)),
        ] + gather_sems() * 4 + [dma, dma],
        compiler_params=pltpu.CompilerParams(vmem_limit_bytes=60 * 1024 * 1024, collective_id=0, has_side_effects=True),
        cost_estimate=pl.CostEstimate(flops=70_000_000_000, bytes_accessed=40_000_000, transcendentals=0),
        name="attention",
    )(x_own, dy_own, gain, w_q, w_k, w_v, w_o, tab)


def grid_call(kernel, steps, info, args, in_specs, out_shape, out_specs, scratch, flops, name, aliases=None):
    return pl.pallas_call(
        kernel,
        out_shape=out_shape,
        grid_spec=pltpu.PrefetchScalarGridSpec(
            num_scalar_prefetch=1, grid=(steps,), in_specs=in_specs, out_specs=out_specs, scratch_shapes=scratch),
        input_output_aliases=aliases or {},
        compiler_params=pltpu.CompilerParams(vmem_limit_bytes=60 * 1024 * 1024),
        cost_estimate=pl.CostEstimate(flops=flops, bytes_accessed=40_000_000, transcendentals=0),
        name=name,
    )(info, *args)


def whole_block(a):
    return pl.BlockSpec(a.shape, lambda n, info: (0,) * len(a.shape))


def run_wo(info, ot_all, dy_all, w_o, x_own):
    rows, width = x_own.shape
    hw = HEADS * DH
    cols = lambda r: pl.BlockSpec((r, BLK), lambda n, info: (0, n))
    return grid_call(
        wo_kernel, NB, info, (ot_all, dy_all, w_o, x_own),
        [VMEM_SPEC, pl.BlockSpec((NB, rows, BLK), lambda n, info: (0, 0, n)), cols(NB * hw), cols(rows)],
        (jax.ShapeDtypeStruct((NB * hw, width), F32), jax.ShapeDtypeStruct((rows, width), BF16)),
        (cols(NB * hw), cols(rows)), [pltpu.VMEM((rows, NB * hw), BF16)], 20_000_000_000, "wo_grad")


def run_near(info, h_t, own, sib, x, y, w_q):
    width, toks = h_t.shape
    cols = pl.BlockSpec((width, BLK), lambda n, info: (0, info[1 + n]))
    acc = jax.ShapeDtypeStruct((BLK, width), F32)
    return grid_call(
        near_kernel, 4, info, (h_t, own, sib, x, y, w_q), [VMEM_SPEC] * 5 + [cols],
        (jax.ShapeDtypeStruct((width, NB * BLK), F32), acc), (cols, whole_block(acc)), [], 10_000_000_000, "wq_near")


def run_far(info, h_t, near, sx, sy, d_a, d_b, sd_a, sd_b, w_q, w_k, w_v, x_own, dy_own, gain, acc, gwq):
    width, toks = h_t.shape
    rows, kv = x_own.shape[0], w_k.shape[1]
    cols = pl.BlockSpec((width, BLK), lambda n, info: (0, info[5 + n]))
    kv_rows = pl.BlockSpec((2 * BLK, BLK), lambda n, info: (NB // 2, 0))
    outs = (jax.ShapeDtypeStruct((width, NB * BLK), F32), jax.ShapeDtypeStruct((width, kv), F32), jax.ShapeDtypeStruct((width, kv), F32),
            jax.ShapeDtypeStruct((rows, width), BF16), jax.ShapeDtypeStruct((1, width), F32))
    return grid_call(
        far_kernel, 4, info,
        (h_t, *near, sx, sy, d_a, d_b, sd_a, sd_b, w_q, w_k, w_v, x_own, dy_own, gain, acc, gwq),
        [VMEM_SPEC] + [kv_rows] * 4 + [VMEM_SPEC] * 6 + [cols] + [VMEM_SPEC] * 6 + [ANY_SPEC],
        outs, (cols,) + tuple(whole_block(o) for o in outs[1:]),
        [pltpu.VMEM((rows, width), F32), pltpu.VMEM((toks + 2 * BLK, BLK), BF16), pltpu.VMEM((NB, 2 * BLK, BLK), BF16),
         pltpu.VMEM((toks, kv), BF16), pltpu.VMEM((toks, kv), BF16)],
        15_000_000_000, "wq_far", aliases={19: 0})


def run_gain(part):
    dma = pltpu.SemaphoreType.DMA
    return pl.pallas_call(
        gain_kernel, out_shape=jax.ShapeDtypeStruct(part.shape, F32), in_specs=[VMEM_SPEC], out_specs=VMEM_SPEC,
        scratch_shapes=[pltpu.VMEM((NB,) + part.shape, F32), dma((7,)), dma((7,))],
        compiler_params=pltpu.CompilerParams(collective_id=2, has_side_effects=True), name="gain_sum")(part)


def solution(mesh):
    def device_step(hidden, grad_out, positions, norm_gain, w_q, w_k, w_v, w_o, inv_freq):
        lane = jnp.arange(128)[None, :]
        pos = positions.reshape(2, 128)
        token = jnp.where(lane < 64, pos[0][:, None], pos[1][:, None]).astype(F32)
        angles = token * jnp.tile(inv_freq, 4)[None, :]
        tab = jnp.where(lane % 64 < 32, jnp.cos(angles), jnp.sin(angles))
        gain = norm_gain.astype(F32)[None, :]
        dy_all, h_t, g, ot_all = run_attention(hidden, grad_out, gain, w_q, w_k, w_v, w_o, tab)
        hp, cp, xn, yn, dn = neighbours()
        slots = [head_slot(a, b) for a, b in ((hp, cp), (hp, 1 - cp), (xn, cp), (yn, cp), (xn, 1 - cp), (yn, 1 - cp), (dn, cp), (dn, 1 - cp))]
        info = jnp.stack([tok_slot(hp, cp)] + slots).astype(jnp.int32)
        along_x = lambda a: lax.ppermute(a, 'hp', [(i, i ^ 1) for i in range(4)])
        along_y = lambda a: lax.ppermute(a, 'hp', [(i, i ^ 2) for i in range(4)])
        to_sib = lambda a: lax.ppermute(a, 'cp', [(0, 1), (1, 0)])
        half = g.shape[0] // 2
        x, y, sib = along_x(g), along_y(g), to_sib(g)
        grad_wo, output = run_wo(info, ot_all, dy_all, w_o, hidden)
        x, y, sib, output = lax.optimization_barrier((x, y, sib, output))
        d_a, d_b = along_y(x[:half]), along_x(y[half:])
        sx, sy = to_sib(x), to_sib(y)
        gwq, acc = run_near(info, h_t, g, sib, x, y, w_q)
        d_a, d_b, acc = lax.optimization_barrier((d_a, d_b, acc))
        sd_a, sd_b = to_sib(d_a), to_sib(d_b)
        grad_wq, grad_wk, grad_wv, grad_hidden, part = run_far(
            info, h_t, (g, sib, x, y), sx, sy, d_a, d_b, sd_a, sd_b, w_q, w_k, w_v, hidden, grad_out, gain, acc, gwq)
        grad_gain = run_gain(part)
        return output, grad_hidden, grad_wq, grad_wk, grad_wv, grad_wo, grad_gain[0]

    seq_spec = P(('cp', 'hp'), None)
    whole = P()
    return jax.shard_map(device_step, mesh=mesh, in_specs=(seq_spec, seq_spec, P(('cp', 'hp')), whole, whole, whole, whole, whole, whole), out_specs=(seq_spec, seq_spec, whole, whole, whole, whole, whole), check_vma=False)
```

```python
import functools
import math

import jax
import jax.numpy as jnp
from jax import lax
from jax.experimental import pallas as pl
from jax.experimental.pallas import tpu as pltpu
from jax.sharding import PartitionSpec as P

NORM_EPS = 1e-5
BLK = 256
HEADS = 4
DH = 64
NB = 8
CW = HEADS * BLK
EXP2_SCALE = (DH ** -0.5) * math.log2(math.e)
F32 = jnp.float32
BF16 = jnp.bfloat16


def seq_block(d):
    cp, half, sub = d // 4, (d // 2) % 2, d % 2
    return 2 * ((1 - half) * cp + half * (3 - cp)) + sub


def stored_block(j):
    b, sub = j // 2, j % 2
    half = b // 2
    cp = (1 - half) * b + half * (3 - b)
    return cp * 4 + half * 2 + sub


def nt_dot(a, b):
    return lax.dot_general(a, b, (((1,), (1,)), ((), ())), preferred_element_type=F32)


def dot(a, b):
    return jnp.dot(a, b, preferred_element_type=F32)


def rope_pairs(t, cos_t, sin_t):
    lane = lax.broadcasted_iota(jnp.int32, t.shape, 1)
    partner = jnp.where(lane % DH < DH // 2, pltpu.roll(t, 128 - DH // 2, 1), pltpu.roll(t, DH // 2, 1))
    return t * cos_t + partner * sin_t


def rows_of(b):
    return pl.ds(pl.multiple_of(b * BLK, BLK), BLK)


def key_rows(kb, tiles):
    return pl.ds(pl.multiple_of(kb * tiles * BLK, tiles * BLK), tiles * BLK)


def by_pairs(count, tile, carry):
    carry = lax.fori_loop(0, count // 2, functools.partial(tile, tiles=2), carry)
    return lax.fori_loop(count - count % 2, count, tile, carry)


def causal_tile():
    row = lax.broadcasted_iota(jnp.int32, (BLK, CW), 0)
    col = lax.broadcasted_iota(jnp.int32, (BLK, CW), 1)
    return row <= col % BLK


MESH = pl.DeviceIdType.MESH
CHUNKS = 4


def neighbours():
    hp, cp = lax.axis_index('hp'), lax.axis_index('cp')
    flip = 1 - 2 * (hp % 2)
    y_hp = (hp + 2) % 4
    return hp, cp, hp + flip, y_hp, y_hp + flip


def tok_slot(hp, cp):
    return cp * 4 + hp


def head_slot(hp, cp):
    return hp * 2 + cp


def enter_barrier():
    hp, cp = lax.axis_index('hp'), lax.axis_index('cp')
    barrier = pltpu.get_barrier_semaphore()
    for m in range(1, 8):
        pl.semaphore_signal(barrier, inc=1, device_id=((hp + m // 2) % 4, (cp + m % 2) % 2), device_id_type=MESH)
    pl.semaphore_wait(barrier, 7)


class Gather:
    def __init__(self, src, dst, slot, send, recv, rows):
        self.src, self.dst, self.slot, self.send, self.recv = src, dst, slot, send, recv
        self.step = rows // CHUNKS
        self.hp, self.cp, self.xn, self.yn, self.dn = neighbours()

    def part(self, ref, c):
        return ref.at[pl.ds(c * self.step, self.step)]

    def place(self, hp, cp, c):
        return self.part(self.dst.at[self.slot(hp, cp)], c)

    def copy(self, kind, c):
        hp, cp, xn, yn, dn = self.hp, self.cp, self.xn, self.yn, self.dn
        origin, lands, to = {
            'own_x': (hp, 0, (xn, cp)), 'own_y': (hp, 1, (yn, cp)), 'own_s': (hp, 3, (hp, 1 - cp)),
            'x_s': (xn, 4, (hp, 1 - cp)), 'y_s': (yn, 5, (hp, 1 - cp)), 'd_s': (dn, 6, (hp, 1 - cp)),
            'x_y': (xn, 2, (yn, cp)), 'y_x': (yn, 2, (xn, cp)),
        }[kind]
        number = ('own_x', 'own_y', 'own_s', 'x_s', 'y_s', 'd_s', 'x_y', 'y_x').index(kind)
        src = self.part(self.src, c) if kind.startswith('own') else self.place(origin, cp, c)
        return pltpu.make_async_remote_copy(
            src_ref=src, dst_ref=self.place(origin, cp, c), send_sem=self.send.at[number, c],
            recv_sem=self.recv.at[lands, c], device_id=to, device_id_type=MESH)

    def await_from(self, number, c):
        hp, cp = ((self.xn, self.cp), (self.yn, self.cp), (self.dn, self.cp), (self.hp, 1 - self.cp),
                  (self.xn, 1 - self.cp), (self.yn, 1 - self.cp), (self.dn, 1 - self.cp))[number]
        ref = self.place(hp, cp, c)
        pltpu.make_async_remote_copy(
            src_ref=ref, dst_ref=ref, send_sem=self.send.at[0, c], recv_sem=self.recv.at[number, c],
            device_id=(self.hp, 1 - self.cp), device_id_type=MESH).wait_recv()

    def start_own(self):
        for c in range(CHUNKS):
            for kind in ('own_x', 'own_y', 'own_s'):
                self.copy(kind, c).start()

    def relay_near(self, chunks=range(CHUNKS)):
        for c in chunks:
            self.await_from(0, c)
            self.copy('x_s', c).start()
            if c < CHUNKS // 2:
                self.copy('x_y', c).start()
            self.await_from(1, c)
            self.copy('y_s', c).start()
            if c >= CHUNKS // 2:
                self.copy('y_x', c).start()

    def relay_diagonal(self):
        for c in range(CHUNKS):
            self.await_from(2, c)
            self.copy('d_s', c).start()

    def await_sibling(self, number):
        for c in range(CHUNKS):
            self.await_from(number, c)

    def finish_sends(self):
        for c in range(CHUNKS):
            for kind in ('own_x', 'own_y', 'own_s', 'x_s', 'y_s', 'd_s'):
                self.copy(kind, c).wait_send()
            self.copy('x_y' if c < CHUNKS // 2 else 'y_x', c).wait_send()


def gather_sems():
    return [pltpu.SemaphoreType.DMA((8, CHUNKS)), pltpu.SemaphoreType.DMA((7, CHUNKS))]


def unpack_table(tab):
    group = lax.broadcasted_iota(jnp.int32, tab.shape, 1) // (DH // 2)
    turned = [tab] + [pltpu.roll(tab, 32 * i, 1) for i in (1, 2, 3)]

    def pick(order):
        out = turned[order[3]]
        for g in range(3):
            out = jnp.where(group == g, turned[order[g]], out)
        return out

    sign = jnp.where(group % 2 == 0, -1.0, 1.0)
    cos_t = jnp.concatenate([pick((0, 1, 2, 3)), pick((2, 3, 0, 1))], axis=0)
    sin_t = jnp.concatenate([pick((3, 0, 1, 2)) * sign, pick((1, 2, 3, 0)) * sign], axis=0)
    return cos_t, sin_t


def project_block(d, x, gain, wq_ref, wkv_ref, tab, ht_ref, q_ref, k_ref, v_ref):
    xf = x.astype(F32)
    inv = lax.rsqrt(jnp.mean(xf * xf, axis=-1, keepdims=True) + NORM_EPS)
    h = (xf * inv * gain).astype(BF16)
    ht_ref[:, rows_of(d)] = h.T
    dst = rows_of(seq_block(d))
    cos_t, sin_t = unpack_table(tab)
    y = dot(h, wq_ref[...])
    for p in range(HEADS // 2):
        qr = rope_pairs(y[:, 128 * p:128 * (p + 1)], cos_t, sin_t).astype(BF16)
        q_ref[2 * p, dst, :] = qr[:, :DH]
        q_ref[2 * p + 1, dst, :] = qr[:, DH:]
    kv = dot(h, wkv_ref[...])
    k_ref[dst, :] = rope_pairs(kv, cos_t, sin_t).astype(BF16)[:, :DH]
    v_ref[dst, :] = kv.astype(BF16)[:, DH:]


def attend_block(j, q_ref, k_ref, vt_ref, e_ref, m_ref, ot_ref, lse_ref):
    q4 = q_ref[:, rows_of(j), :].reshape(CW, DH)

    def score_tile(kb, carry, masked, tiles=1):
        m_old, l_old = carry
        keys = key_rows(kb, tiles)
        s = nt_dot(k_ref[keys, :], q4) * EXP2_SCALE
        if masked:
            s = jnp.where(causal_tile(), s, -1e30)
        m_new = jnp.maximum(m_old, jnp.max(s, axis=0, keepdims=True))
        e = jnp.exp2(s - m_new)
        e_ref[keys, :] = e
        for i in range(tiles):
            m_ref[pl.ds(kb * tiles + i, 1), :] = m_new
        return m_new, l_old * jnp.exp2(m_old - m_new) + jnp.sum(e, axis=0, keepdims=True)

    carry = (jnp.full((1, CW), -1e30, F32), jnp.zeros((1, CW), F32))
    carry = score_tile(j, carry, True)
    m_fin, l_fin = by_pairs(j, functools.partial(score_tile, masked=False), carry)
    inv_l = 1.0 / l_fin
    lse = m_fin + jnp.log2(l_fin)

    def out_tile(kb, acc, tiles=1):
        parts = []
        for i in range(tiles):
            f = jnp.exp2(m_ref[pl.ds(kb * tiles + i, 1), :] - m_fin) * inv_l
            parts.append((e_ref[rows_of(kb * tiles + i), :] * f).astype(BF16))
        return acc + dot(vt_ref[:, key_rows(kb, tiles)], jnp.concatenate(parts, axis=0))

    acc = by_pairs(j + 1, out_tile, jnp.zeros((DH, CW), F32)).astype(BF16)
    dst = rows_of(stored_block(j))
    for h in range(HEADS):
        ot_ref[DH * h:DH * (h + 1), dst] = acc[:, BLK * h:BLK * (h + 1)]
        lse_ref[h:h + 1, rows_of(j)] = lse[:, BLK * h:BLK * (h + 1)]


def nth_peer(e):
    hp, cp = lax.axis_index('hp'), lax.axis_index('cp')
    m, b = e // 2, e % 2
    px = (hp % 2 + m % 2) % 2
    py = (hp // 2 + m // 2) % 2
    return py * 2 + px, (cp + b) % 2


def attention_kernel(x_own, dy_own, gain_ref, wq_hbm, wk_hbm, wv_hbm, wo_hbm, tab_own,
                     dy_all, ht_out, gq_ref, ot_all,
                     xg, ht, e_ref, m_ref, vt_ref, wq, wk, wv, wkv, stage, q_ref, k_ref, v_ref, ot_ref, lse_ref, tabs,
                     wo, wot, do_ref, kt_ref, dk_ref, dv_ref, give, take,
                     local_sem, dy_sem, t_send, t_recv, x_send, x_recv, dy_send, dy_recv, o_send, o_recv, pair_send, pair_recv):
    hp, cp, xn, yn, dn = neighbours()
    mine = tok_slot(hp, cp)
    hw = HEADS * DH
    loads = [
        pltpu.make_async_copy(x_own, xg.at[mine], local_sem.at[0]),
        pltpu.make_async_copy(wq_hbm.at[:, pl.ds(pl.multiple_of(head_slot(hp, cp) * hw, hw), hw)], wq, local_sem.at[1]),
        pltpu.make_async_copy(wk_hbm.at[:, pl.ds(pl.multiple_of((hp // 2) * 128, 128), 128)], wk, local_sem.at[2]),
        pltpu.make_async_copy(wv_hbm.at[:, pl.ds(pl.multiple_of((hp // 2) * 128, 128), 128)], wv, local_sem.at[3]),
        pltpu.make_async_copy(dy_own, stage, local_sem.at[4]),
        pltpu.make_async_copy(tab_own, tabs.at[mine], local_sem.at[5]),
    ]
    for load in loads:
        load.start()
    wo_load = pltpu.make_async_copy(wo_hbm.at[pl.ds(pl.multiple_of(head_slot(hp, cp) * hw, hw), hw)], wo, local_sem.at[8])
    wo_load.start()
    enter_barrier()
    gx = Gather(x_own, xg, tok_slot, x_send, x_recv, BLK)
    gdy = Gather(dy_own, dy_all, tok_slot, dy_send, dy_recv, BLK)

    gt = Gather(tab_own, tabs, tok_slot, t_send, t_recv, 128)
    gt.start_own()
    gx.start_own()
    for load in loads[1:4]:
        load.wait()
    lane = lax.broadcasted_iota(jnp.int32, wk.shape, 1)
    swap = hp % 2 == 1
    kf, vf = wk[...].astype(F32), wv[...].astype(F32)
    k_sel = jnp.where(swap, pltpu.roll(kf, DH, 1), kf)
    v_sel = jnp.where(swap, vf, pltpu.roll(vf, DH, 1))
    wkv[...] = jnp.where(lane < DH, k_sel, v_sel).astype(BF16)
    wo_load.wait()
    wot[...] = wo[...].T
    for i in (0, 4, 5):
        loads[i].wait()
    dy_mine = pltpu.make_async_copy(stage, dy_all.at[mine], local_sem.at[6])
    dy_mine.start()
    def project(e, _):
        @pl.when(e == 1)
        def _():
            gt.await_sibling(3)
            gx.await_sibling(3)

        @pl.when(e == 2)
        def _():
            gt.relay_near()
            gx.relay_near()
            gdy.start_own()

        @pl.when(e == 3)
        def _():
            gt.await_sibling(4)
            gx.await_sibling(4)

        @pl.when(e == 5)
        def _():
            gt.await_sibling(5)
            gx.await_sibling(5)

        @pl.when(e == 6)
        def _():
            gt.relay_diagonal()
            gx.relay_diagonal()

        @pl.when(e == 7)
        def _():
            gt.await_sibling(6)
            gx.await_sibling(6)

        d = tok_slot(*nth_peer(e))
        project_block(d, xg[d], gain_ref[...], wq, wkv, tabs[d], ht, q_ref, k_ref, v_ref)
        return 0

    lax.fori_loop(0, NB, project, 0)
    ht_copy = pltpu.make_async_copy(ht, ht_out, local_sem.at[7])
    ht_copy.start()
    vt_ref[...] = v_ref[...].T

    def attend(j, _):
        for c in range(CHUNKS):
            @pl.when(j == (1, 3, 5, 6)[c])
            def _():
                gdy.relay_near((c,))

        attend_block(j, q_ref, k_ref, vt_ref, e_ref, m_ref, ot_ref, lse_ref)
        return 0

    lax.fori_loop(0, NB, attend, 0)
    go = Gather(ot_ref, ot_all, head_slot, o_send, o_recv, hw)
    kt_ref[...] = k_ref[...].T
    dk_ref[...] = jnp.zeros_like(dk_ref)
    dv_ref[...] = jnp.zeros_like(dv_ref)
    go.start_own()
    ot_mine = pltpu.make_async_copy(ot_ref, ot_all.at[head_slot(hp, cp)], local_sem.at[9])
    ot_mine.start()
    gx.finish_sends()
    dy_mine.wait()

    def dy_load(e):
        d = tok_slot(*nth_peer(e))
        return pltpu.make_async_copy(dy_all.at[d], xg.at[d], dy_sem.at[e])

    def project_dy(e, _):
        dy_load(e).wait()
        d = tok_slot(*nth_peer(e))
        do = dot(xg[d], wot[...]).astype(BF16)
        dst = rows_of(seq_block(d))
        for h in range(HEADS):
            do_ref[h, dst, :] = do[:, DH * h:DH * (h + 1)]
        return 0

    for number in (3, 4, 5):
        gdy.await_sibling(number)
    for e in range(6):
        dy_load(e).start()
    lax.fori_loop(0, 6, project_dy, 0)
    gdy.relay_diagonal()
    dy_load(6).start()
    gdy.await_sibling(6)
    dy_load(7).start()
    lax.fori_loop(6, NB, project_dy, 0)

    def attend_back(j, _):
        for c in range(CHUNKS):
            @pl.when(j == (2, 4, 5, 6)[c])
            def _():
                go.relay_near((c,))

        slot = stored_block(j)
        src = rows_of(slot)
        q4 = q_ref[:, rows_of(j), :].reshape(CW, DH)
        do4 = do_ref[:, rows_of(j), :].reshape(CW, DH)
        o4t = jnp.concatenate([ot_ref[DH * h:DH * (h + 1), src] for h in range(HEADS)], axis=1)
        lse = jnp.concatenate([lse_ref[h:h + 1, rows_of(j)] for h in range(HEADS)], axis=1)
        delta = jnp.sum(do4.astype(F32).T * o4t.astype(F32), axis=0, keepdims=True)

        def tile(kb, dqt, masked, tiles=1):
            keys = key_rows(kb, tiles)
            p = jnp.exp2(nt_dot(k_ref[keys, :], q4) * EXP2_SCALE - lse)
            if masked:
                p = jnp.where(causal_tile(), p, 0.0)
            dp = nt_dot(v_ref[keys, :], do4)
            dv_ref[keys, :] += dot(p.astype(BF16), do4)
            ds = (p * (dp - delta)).astype(BF16)
            dk_ref[keys, :] += dot(ds, q4)
            return dqt + dot(kt_ref[:, keys], ds)

        dqt = tile(j, jnp.zeros((DH, CW), F32), True)
        dqt = by_pairs(j, functools.partial(tile, masked=False), dqt) * (DH ** -0.5)
        cos_t, sin_t = unpack_table(tabs[slot])
        for p in range(HEADS // 2):
            pair = jnp.concatenate([dqt[:, BLK * (2 * p):BLK * (2 * p + 1)], dqt[:, BLK * (2 * p + 1):BLK * (2 * p + 2)]], axis=0)
            dq = pair.T.astype(BF16).astype(F32)
            gq_ref[src, 128 * p:128 * (p + 1)] = rope_pairs(dq, cos_t, -sin_t).astype(BF16)
        return 0

    lax.fori_loop(0, NB, attend_back, 0)
    give[:, :DH] = (dk_ref[...] * (DH ** -0.5)).astype(BF16)
    give[:, DH:] = dv_ref[...].astype(BF16)
    swap = pltpu.make_async_remote_copy(
        src_ref=give, dst_ref=take, send_sem=pair_send, recv_sem=pair_recv, device_id=(hp, 1 - cp), device_id_type=MESH)
    go.relay_diagonal()
    swap.start()
    for number in (3, 4, 5):
        go.await_sibling(number)
    swap.wait_recv()
    lane = lax.broadcasted_iota(jnp.int32, (BLK, 2 * DH), 1)
    for i in range(NB // 2):
        slot = cp * 4 + i
        src = rows_of(seq_block(slot))
        total = (give[src, :].astype(F32) + take[src, :].astype(F32)).astype(BF16).astype(F32)
        cos_t, sin_t = unpack_table(tabs[slot])
        turned = rope_pairs(total, cos_t, -sin_t)
        gq_ref[NB * BLK + (i % 2) * BLK:NB * BLK + (i % 2 + 1) * BLK, 128 * (i // 2):128 * (i // 2 + 1)] = jnp.where(lane < DH, turned, total).astype(BF16)
    go.await_sibling(6)
    swap.wait_send()
    go.finish_sends()
    ot_mine.wait()
    gt.finish_sends()
    gdy.finish_sends()
    ht_copy.wait()


def start_rows(a_hbm, a_ref, sem):
    for i in range(NB):
        pltpu.make_async_copy(a_hbm.at[i], a_ref.at[i], sem.at[i]).start()


def product(a_hbm, a_ref, sem, b, out_ref):
    first = pl.program_id(0) == 0

    @pl.when(first)
    def _():
        def block(i, _):
            pltpu.make_async_copy(a_hbm.at[i], a_ref.at[i], sem.at[i]).wait()
            out_ref[rows_of(i), :] = dot(a_ref[i], b[...])
            return 0

        lax.fori_loop(0, NB, block, 0)

    @pl.when(jnp.logical_not(first))
    def _():
        out_ref[...] = dot(a_ref[...].reshape(NB * BLK, NB * BLK), b[...])


def wo_kernel(info, ot_hbm, dy_ref, wo_ref, x_ref, gwo_ref, out_ref, ot_ref, o_mine, b_ref, sem):
    first = pl.program_id(0) == 0

    @pl.when(first)
    def _():
        start_rows(ot_hbm, ot_ref, sem)

    b_ref[...] = dy_ref[...].reshape(NB * BLK, BLK)
    product(ot_hbm, ot_ref, sem, b_ref, gwo_ref)

    @pl.when(first)
    def _():
        for d in range(NB):
            o_mine[:, BLK * d:BLK * (d + 1)] = ot_ref[d, :, rows_of(info[0])].T

    out_ref[...] = (x_ref[...].astype(F32) + dot(o_mine[...], wo_ref[...])).astype(BF16)


def near_kernel(info, ht_hbm, own_hbm, sib_hbm, x_hbm, y_hbm, wq_ref, gwq_ref, acc_ref, ht_ref, g_ref, sem, g_sem):
    e = pl.program_id(0)
    toks = NB * BLK
    fetch = [pltpu.make_async_copy(src.at[pl.ds(0, toks)], g_ref.at[i], g_sem.at[i]) for i, src in enumerate((own_hbm, sib_hbm, x_hbm, y_hbm))]

    @pl.when(e == 0)
    def _():
        fetch[0].start()
        start_rows(ht_hbm, ht_ref, sem)
        for i in (1, 2, 3):
            fetch[i].start()

    for i in range(4):
        @pl.when(e == i)
        def _():
            fetch[i].wait()

    g = g_ref.at[e]
    product(ht_hbm, ht_ref, sem, g, gwq_ref)
    part = nt_dot(g[rows_of(info[0]), :], wq_ref[...])

    @pl.when(e == 0)
    def _():
        acc_ref[...] = part

    @pl.when(e > 0)
    def _():
        acc_ref[...] += part


def far_kernel(info, ht_hbm, own_hbm, sib_hbm, x_hbm, y_hbm, sx_hbm, sy_hbm, da_hbm, db_hbm, sda_hbm, sdb_hbm,
               wq_ref, wk_hbm, wv_hbm, x_hbm_own, dy_hbm_own, gain_ref, acc_hbm, gwq_in,
               gwq_ref, gwk_hbm, gwv_hbm, gh_ref, gg_ref,
               ht_ref, g_ref, kv4, gkvg, bk, bv, gwk, gwv, acc, acc_in, wk, wv, x_own, dy_own, sem, g_sem, kv_sem, late_sem):
    e = pl.program_id(0)
    toks = NB * BLK
    half = da_hbm.shape[0]
    copy = pltpu.make_async_copy
    lo, hi = pl.ds(0, half), pl.ds(half, half)
    fetch = ((copy(sx_hbm, g_ref.at[0], g_sem.at[0]),), (copy(sy_hbm, g_ref.at[1], g_sem.at[1]),),
             (copy(da_hbm, g_ref.at[2, lo], g_sem.at[2]), copy(db_hbm, g_ref.at[2, hi], g_sem.at[3])),
             (copy(sda_hbm, g_ref.at[3, lo], g_sem.at[4]), copy(sdb_hbm, g_ref.at[3, hi], g_sem.at[5])))
    near_kv = [copy(src.at[pl.ds(toks, 2 * BLK)], kv4.at[i], kv_sem.at[i]) for i, src in enumerate((own_hbm, sib_hbm, x_hbm, y_hbm))]
    late = [copy(src, dst, late_sem.at[i]) for i, (src, dst) in enumerate(
        ((acc_hbm, acc_in), (wk_hbm, wk), (wv_hbm, wv), (x_hbm_own, x_own), (dy_hbm_own, dy_own)))]
    give = [copy(gwk, gwk_hbm, late_sem.at[5]), copy(gwv, gwv_hbm, late_sem.at[6])]

    @pl.when(e == 0)
    def _():
        fetch[0][0].start()
        start_rows(ht_hbm, ht_ref, sem)
        for load in [c for group in fetch[1:] for c in group] + near_kv + late:
            load.start()
        fetch[0][0].wait()

    @pl.when(e == 1)
    def _():
        for load in [c for group in fetch[1:] for c in group] + near_kv:
            load.wait()
        for i in range(4):
            gkvg[info[1 + i]] = kv4[i]
            gkvg[info[5 + i]] = g_ref[i, toks:, :]
        for c in range(2):
            for r in range(2):
                dst = pl.ds((c * 2 + r) * 2 * BLK, 2 * BLK)
                for p in range(2):
                    even = gkvg[4 * p + c, :, 128 * r:128 * (r + 1)]
                    odd = gkvg[4 * p + 2 + c, :, 128 * r:128 * (r + 1)]
                    bk[dst, 128 * p:128 * (p + 1)] = jnp.concatenate([even[:, :DH], odd[:, :DH]], axis=1)
                    bv[dst, 128 * p:128 * (p + 1)] = jnp.concatenate([even[:, DH:], odd[:, DH:]], axis=1)
        a = ht_ref[...].reshape(toks, toks)
        gwk[...] = dot(a, bk[...])
        gwv[...] = dot(a, bv[...])
        for out in give:
            out.start()

    g = g_ref.at[e]
    part = nt_dot(g[rows_of(info[0]), :], wq_ref[...])

    @pl.when(e == 0)
    def _():
        acc[...] = part

    @pl.when(e > 0)
    def _():
        acc[...] += part

    product(ht_hbm, ht_ref, sem, g.at[pl.ds(0, toks)], gwq_ref)

    @pl.when(e == 3)
    def _():
        for load in late:
            load.wait()
        mine = rows_of(info[0])
        d_norm = acc[...] + acc_in[...] + nt_dot(bk[mine, :], wk[...]) + nt_dot(bv[mine, :], wv[...])
        x = x_own[...].astype(F32)
        inv = lax.rsqrt(jnp.mean(x * x, axis=-1, keepdims=True) + NORM_EPS)
        x_hat = x * inv
        gg_ref[...] = jnp.sum(d_norm * x_hat, axis=0, keepdims=True)
        d_hat = d_norm * gain_ref[...]
        row_mean = jnp.mean(d_hat * x_hat, axis=-1, keepdims=True)
        gh_ref[...] = (dy_own[...].astype(F32) + inv * (d_hat - x_hat * row_mean)).astype(BF16)
        for out in give:
            out.wait()


def gain_kernel(part_ref, gg_ref, gains, send, recv):
    hp, cp = lax.axis_index('hp'), lax.axis_index('cp')
    mine = tok_slot(hp, cp)
    enter_barrier()

    def gain_copy(m):
        return pltpu.make_async_remote_copy(
            src_ref=part_ref, dst_ref=gains.at[mine], send_sem=send.at[m - 1], recv_sem=recv.at[m - 1],
            device_id=((hp + m // 2) % 4, (cp + m % 2) % 2), device_id_type=MESH)

    for m in range(1, NB):
        gain_copy(m).start()
    gains[mine] = part_ref[...]
    for m in range(1, NB):
        ref = gains.at[tok_slot((hp + 4 - m // 2) % 4, (cp + m % 2) % 2)]
        pltpu.make_async_remote_copy(
            src_ref=ref, dst_ref=ref, send_sem=send.at[m - 1], recv_sem=recv.at[m - 1],
            device_id=(hp, 1 - cp), device_id_type=MESH).wait_recv()
    total = gains[0]
    for d in range(1, NB):
        total = total + gains[d]
    gg_ref[...] = total
    for m in range(1, NB):
        gain_copy(m).wait_send()


VMEM_SPEC = pl.BlockSpec(memory_space=pltpu.VMEM)
ANY_SPEC = pl.BlockSpec(memory_space=pl.ANY)


def run_attention(x_own, dy_own, gain, w_q, w_k, w_v, w_o, tab):
    rows, width = x_own.shape
    toks = rows * NB
    hw = HEADS * DH
    dma = pltpu.SemaphoreType.DMA
    b16 = lambda *shape: pltpu.VMEM(shape, BF16)
    f32 = lambda *shape: pltpu.VMEM(shape, F32)
    return pl.pallas_call(
        attention_kernel,
        out_shape=(
            jax.ShapeDtypeStruct((NB, rows, width), BF16),
            jax.ShapeDtypeStruct((width, toks), BF16),
            jax.ShapeDtypeStruct((toks + 2 * BLK, hw), BF16),
            jax.ShapeDtypeStruct((NB, hw, toks), BF16),
        ),
        in_specs=[ANY_SPEC, ANY_SPEC, VMEM_SPEC] + [ANY_SPEC] * 5,
        out_specs=(ANY_SPEC, ANY_SPEC, VMEM_SPEC, ANY_SPEC),
        scratch_shapes=[
            b16(NB, rows, width), b16(width, toks), f32(toks, CW), f32(NB, CW), b16(DH, toks),
            b16(width, hw), b16(width, 128), b16(width, 128), b16(width, 128), b16(rows, width),
            b16(HEADS, toks, DH), b16(toks, DH), b16(toks, DH), b16(hw, toks), f32(HEADS, toks), f32(NB, 128, 128),
            b16(hw, width), b16(width, hw), b16(HEADS, toks, DH), b16(DH, toks), f32(toks, DH), f32(toks, DH), b16(toks, 2 * DH), b16(toks, 2 * DH),
            dma((10,)), dma((NB,)),
        ] + gather_sems() * 4 + [dma, dma],
        compiler_params=pltpu.CompilerParams(vmem_limit_bytes=60 * 1024 * 1024, collective_id=0, has_side_effects=True),
        cost_estimate=pl.CostEstimate(flops=70_000_000_000, bytes_accessed=40_000_000, transcendentals=0),
        name="attention",
    )(x_own, dy_own, gain, w_q, w_k, w_v, w_o, tab)


def grid_call(kernel, steps, info, args, in_specs, out_shape, out_specs, scratch, flops, name, aliases=None):
    return pl.pallas_call(
        kernel,
        out_shape=out_shape,
        grid_spec=pltpu.PrefetchScalarGridSpec(
            num_scalar_prefetch=1, grid=(steps,), in_specs=in_specs, out_specs=out_specs, scratch_shapes=scratch),
        input_output_aliases=aliases or {},
        compiler_params=pltpu.CompilerParams(vmem_limit_bytes=60 * 1024 * 1024),
        cost_estimate=pl.CostEstimate(flops=flops, bytes_accessed=40_000_000, transcendentals=0),
        name=name,
    )(info, *args)


def whole_block(a):
    return pl.BlockSpec(a.shape, lambda n, info: (0,) * len(a.shape))


def run_wo(info, ot_all, dy_all, w_o, x_own):
    rows, width = x_own.shape
    hw = HEADS * DH
    cols = lambda r: pl.BlockSpec((r, BLK), lambda n, info: (0, n))
    return grid_call(
        wo_kernel, NB, info, (ot_all, dy_all, w_o, x_own),
        [ANY_SPEC, pl.BlockSpec((NB, rows, BLK), lambda n, info: (0, 0, n)), cols(NB * hw), cols(rows)],
        (jax.ShapeDtypeStruct((NB * hw, width), F32), jax.ShapeDtypeStruct((rows, width), BF16)),
        (cols(NB * hw), cols(rows)),
        [pltpu.VMEM(ot_all.shape, BF16), pltpu.VMEM((rows, NB * hw), BF16), pltpu.VMEM((NB * rows, BLK), BF16), pltpu.SemaphoreType.DMA((NB,))],
        20_000_000_000, "wo_grad")


def run_near(info, h_t, own, sib, x, y, w_q):
    width, toks = w_q.shape[0], NB * BLK
    cols = pl.BlockSpec((width, BLK), lambda n, info: (0, info[1 + n]))
    acc = jax.ShapeDtypeStruct((BLK, width), F32)
    dma = pltpu.SemaphoreType.DMA
    return grid_call(
        near_kernel, 4, info, (h_t, own, sib, x, y, w_q), [ANY_SPEC] * 5 + [cols],
        (jax.ShapeDtypeStruct((width, NB * BLK), F32), acc), (cols, whole_block(acc)),
        [pltpu.VMEM(h_t.shape, BF16), pltpu.VMEM((4, toks, BLK), BF16), dma((NB,)), dma((4,))], 10_000_000_000, "wq_near")


def run_far(info, h_t, near, sx, sy, d_a, d_b, sd_a, sd_b, w_q, w_k, w_v, x_own, dy_own, gain, acc, gwq):
    width, toks = w_q.shape[0], NB * BLK
    rows, kv = x_own.shape[0], w_k.shape[1]
    cols = pl.BlockSpec((width, BLK), lambda n, info: (0, info[5 + n]))
    outs = (jax.ShapeDtypeStruct((width, NB * BLK), F32), jax.ShapeDtypeStruct((width, kv), F32), jax.ShapeDtypeStruct((width, kv), F32),
            jax.ShapeDtypeStruct((rows, width), BF16), jax.ShapeDtypeStruct((1, width), F32))
    dma = pltpu.SemaphoreType.DMA
    b16 = lambda *shape: pltpu.VMEM(shape, BF16)
    f32 = lambda *shape: pltpu.VMEM(shape, F32)
    return grid_call(
        far_kernel, 4, info,
        (h_t, *near, sx, sy, d_a, d_b, sd_a, sd_b, w_q, w_k, w_v, x_own, dy_own, gain, acc, gwq),
        [ANY_SPEC] * 11 + [cols] + [ANY_SPEC] * 4 + [VMEM_SPEC] + [ANY_SPEC] * 2,
        outs, (cols, ANY_SPEC, ANY_SPEC, whole_block(outs[3]), whole_block(outs[4])),
        [b16(*h_t.shape), b16(4, toks + 2 * BLK, BLK), b16(4, 2 * BLK, BLK), b16(NB, 2 * BLK, BLK), b16(toks, kv), b16(toks, kv),
         f32(width, kv), f32(width, kv), f32(rows, width), f32(rows, width), b16(width, kv), b16(width, kv), b16(rows, width), b16(rows, width),
         dma((NB,)), dma((6,)), dma((4,)), dma((7,))],
        15_000_000_000, "wq_far", aliases={19: 0})


def run_gain(part):
    dma = pltpu.SemaphoreType.DMA
    return pl.pallas_call(
        gain_kernel, out_shape=jax.ShapeDtypeStruct(part.shape, F32), in_specs=[VMEM_SPEC], out_specs=VMEM_SPEC,
        scratch_shapes=[pltpu.VMEM((NB,) + part.shape, F32), dma((7,)), dma((7,))],
        compiler_params=pltpu.CompilerParams(collective_id=2, has_side_effects=True), name="gain_sum")(part)


def solution(mesh):
    def device_step(hidden, grad_out, positions, norm_gain, w_q, w_k, w_v, w_o, inv_freq):
        lane = jnp.arange(128)[None, :]
        pos = positions.reshape(2, 128)
        token = jnp.where(lane < 64, pos[0][:, None], pos[1][:, None]).astype(F32)
        angles = token * jnp.tile(inv_freq, 4)[None, :]
        tab = jnp.where(lane % 64 < 32, jnp.cos(angles), jnp.sin(angles))
        gain = norm_gain.astype(F32)[None, :]
        dy_all, h_t, g, ot_all = run_attention(hidden, grad_out, gain, w_q, w_k, w_v, w_o, tab)
        h_t = h_t.reshape(NB, BLK, -1)
        hp, cp, xn, yn, dn = neighbours()
        slots = [head_slot(a, b) for a, b in ((hp, cp), (hp, 1 - cp), (xn, cp), (yn, cp), (xn, 1 - cp), (yn, 1 - cp), (dn, cp), (dn, 1 - cp))]
        info = jnp.stack([tok_slot(hp, cp)] + slots).astype(jnp.int32)
        along_x = lambda a: lax.ppermute(a, 'hp', [(i, i ^ 1) for i in range(4)])
        along_y = lambda a: lax.ppermute(a, 'hp', [(i, i ^ 2) for i in range(4)])
        to_sib = lambda a: lax.ppermute(a, 'cp', [(0, 1), (1, 0)])
        half = g.shape[0] // 2
        x, y, sib = along_x(g), along_y(g), to_sib(g)
        grad_wo, output = run_wo(info, ot_all, dy_all, w_o, hidden)
        x, y, sib, output = lax.optimization_barrier((x, y, sib, output))
        d_a, d_b = along_y(x[:half]), along_x(y[half:])
        sx, sy = to_sib(x), to_sib(y)
        gwq, acc = run_near(info, h_t, g, sib, x, y, w_q)
        d_a, d_b, acc = lax.optimization_barrier((d_a, d_b, acc))
        sd_a, sd_b = to_sib(d_a), to_sib(d_b)
        grad_wq, grad_wk, grad_wv, grad_hidden, part = run_far(
            info, h_t, (g, sib, x, y), sx, sy, d_a, d_b, sd_a, sd_b, w_q, w_k, w_v, hidden, grad_out, gain, acc, gwq)
        grad_gain = run_gain(part)
        return output, grad_hidden, grad_wq, grad_wk, grad_wv, grad_wo, grad_gain[0]

    seq_spec = P(('cp', 'hp'), None)
    whole = P()
    return jax.shard_map(device_step, mesh=mesh, in_specs=(seq_spec, seq_spec, P(('cp', 'hp')), whole, whole, whole, whole, whole, whole), out_specs=(seq_spec, seq_spec, whole, whole, whole, whole, whole), check_vma=False)
```

```python
import functools
import math

import jax
import jax.numpy as jnp
from jax import lax
from jax.experimental import pallas as pl
from jax.experimental.pallas import tpu as pltpu
from jax.sharding import PartitionSpec as P

NORM_EPS = 1e-5
BLK = 256
HEADS = 4
DH = 64
NB = 8
CW = HEADS * BLK
EXP2_SCALE = (DH ** -0.5) * math.log2(math.e)
F32 = jnp.float32
BF16 = jnp.bfloat16


def seq_block(d):
    cp, half, sub = d // 4, (d // 2) % 2, d % 2
    return 2 * ((1 - half) * cp + half * (3 - cp)) + sub


def stored_block(j):
    b, sub = j // 2, j % 2
    half = b // 2
    cp = (1 - half) * b + half * (3 - b)
    return cp * 4 + half * 2 + sub


def nt_dot(a, b):
    return lax.dot_general(a, b, (((1,), (1,)), ((), ())), preferred_element_type=F32)


def dot(a, b):
    return jnp.dot(a, b, preferred_element_type=F32)


def rope_pairs(t, cos_t, sin_t):
    lane = lax.broadcasted_iota(jnp.int32, t.shape, 1)
    partner = jnp.where(lane % DH < DH // 2, pltpu.roll(t, 128 - DH // 2, 1), pltpu.roll(t, DH // 2, 1))
    return t * cos_t + partner * sin_t


def rows_of(b):
    return pl.ds(pl.multiple_of(b * BLK, BLK), BLK)


def key_rows(kb, tiles):
    return pl.ds(pl.multiple_of(kb * tiles * BLK, tiles * BLK), tiles * BLK)


def by_pairs(count, tile, carry):
    carry = lax.fori_loop(0, count // 2, functools.partial(tile, tiles=2), carry)
    return lax.fori_loop(count - count % 2, count, tile, carry)


def causal_tile():
    row = lax.broadcasted_iota(jnp.int32, (BLK, CW), 0)
    col = lax.broadcasted_iota(jnp.int32, (BLK, CW), 1)
    return row <= col % BLK


MESH = pl.DeviceIdType.MESH
CHUNKS = 4


def neighbours():
    hp, cp = lax.axis_index('hp'), lax.axis_index('cp')
    flip = 1 - 2 * (hp % 2)
    y_hp = (hp + 2) % 4
    return hp, cp, hp + flip, y_hp, y_hp + flip


def tok_slot(hp, cp):
    return cp * 4 + hp


def head_slot(hp, cp):
    return hp * 2 + cp


def enter_barrier():
    hp, cp = lax.axis_index('hp'), lax.axis_index('cp')
    barrier = pltpu.get_barrier_semaphore()
    for m in range(1, 8):
        pl.semaphore_signal(barrier, inc=1, device_id=((hp + m // 2) % 4, (cp + m % 2) % 2), device_id_type=MESH)
    pl.semaphore_wait(barrier, 7)


class Gather:
    def __init__(self, src, dst, slot, send, recv, rows):
        self.src, self.dst, self.slot, self.send, self.recv = src, dst, slot, send, recv
        self.step = rows // CHUNKS
        self.hp, self.cp, self.xn, self.yn, self.dn = neighbours()

    def part(self, ref, c):
        return ref.at[pl.ds(c * self.step, self.step)]

    def place(self, hp, cp, c):
        return self.part(self.dst.at[self.slot(hp, cp)], c)

    def copy(self, kind, c):
        hp, cp, xn, yn, dn = self.hp, self.cp, self.xn, self.yn, self.dn
        origin, lands, to = {
            'own_x': (hp, 0, (xn, cp)), 'own_y': (hp, 1, (yn, cp)), 'own_s': (hp, 3, (hp, 1 - cp)),
            'x_s': (xn, 4, (hp, 1 - cp)), 'y_s': (yn, 5, (hp, 1 - cp)), 'd_s': (dn, 6, (hp, 1 - cp)),
            'x_y': (xn, 2, (yn, cp)), 'y_x': (yn, 2, (xn, cp)),
        }[kind]
        number = ('own_x', 'own_y', 'own_s', 'x_s', 'y_s', 'd_s', 'x_y', 'y_x').index(kind)
        src = self.part(self.src, c) if kind.startswith('own') else self.place(origin, cp, c)
        return pltpu.make_async_remote_copy(
            src_ref=src, dst_ref=self.place(origin, cp, c), send_sem=self.send.at[number, c],
            recv_sem=self.recv.at[lands, c], device_id=to, device_id_type=MESH)

    def await_from(self, number, c):
        hp, cp = ((self.xn, self.cp), (self.yn, self.cp), (self.dn, self.cp), (self.hp, 1 - self.cp),
                  (self.xn, 1 - self.cp), (self.yn, 1 - self.cp), (self.dn, 1 - self.cp))[number]
        ref = self.place(hp, cp, c)
        pltpu.make_async_remote_copy(
            src_ref=ref, dst_ref=ref, send_sem=self.send.at[0, c], recv_sem=self.recv.at[number, c],
            device_id=(self.hp, 1 - self.cp), device_id_type=MESH).wait_recv()

    def start_own(self):
        for c in range(CHUNKS):
            for kind in ('own_x', 'own_y', 'own_s'):
                self.copy(kind, c).start()

    def relay_near(self, chunks=range(CHUNKS)):
        for c in chunks:
            self.await_from(0, c)
            self.copy('x_s', c).start()
            if c < CHUNKS // 2:
                self.copy('x_y', c).start()
            self.await_from(1, c)
            self.copy('y_s', c).start()
            if c >= CHUNKS // 2:
                self.copy('y_x', c).start()

    def relay_diagonal(self):
        for c in range(CHUNKS):
            self.await_from(2, c)
            self.copy('d_s', c).start()

    def await_sibling(self, number):
        for c in range(CHUNKS):
            self.await_from(number, c)

    def finish_sends(self):
        for c in range(CHUNKS):
            for kind in ('own_x', 'own_y', 'own_s', 'x_s', 'y_s', 'd_s'):
                self.copy(kind, c).wait_send()
            self.copy('x_y' if c < CHUNKS // 2 else 'y_x', c).wait_send()


def gather_sems():
    return [pltpu.SemaphoreType.DMA((8, CHUNKS)), pltpu.SemaphoreType.DMA((7, CHUNKS))]


def unpack_table(tab):
    group = lax.broadcasted_iota(jnp.int32, tab.shape, 1) // (DH // 2)
    turned = [tab] + [pltpu.roll(tab, 32 * i, 1) for i in (1, 2, 3)]

    def pick(order):
        out = turned[order[3]]
        for g in range(3):
            out = jnp.where(group == g, turned[order[g]], out)
        return out

    sign = jnp.where(group % 2 == 0, -1.0, 1.0)
    cos_t = jnp.concatenate([pick((0, 1, 2, 3)), pick((2, 3, 0, 1))], axis=0)
    sin_t = jnp.concatenate([pick((3, 0, 1, 2)) * sign, pick((1, 2, 3, 0)) * sign], axis=0)
    return cos_t, sin_t


def project_block(d, x, gain, wq_ref, wkv_ref, tab, ht_ref, q_ref, k_ref, v_ref):
    xf = x.astype(F32)
    inv = lax.rsqrt(jnp.mean(xf * xf, axis=-1, keepdims=True) + NORM_EPS)
    h = (xf * inv * gain).astype(BF16)
    ht_ref[:, rows_of(d)] = h.T
    dst = rows_of(seq_block(d))
    cos_t, sin_t = unpack_table(tab)
    y = dot(h, wq_ref[...])
    for p in range(HEADS // 2):
        qr = rope_pairs(y[:, 128 * p:128 * (p + 1)], cos_t, sin_t).astype(BF16)
        q_ref[2 * p, dst, :] = qr[:, :DH]
        q_ref[2 * p + 1, dst, :] = qr[:, DH:]
    kv = dot(h, wkv_ref[...])
    k_ref[dst, :] = rope_pairs(kv, cos_t, sin_t).astype(BF16)[:, :DH]
    v_ref[dst, :] = kv.astype(BF16)[:, DH:]


def attend_block(j, q_ref, k_ref, vt_ref, e_ref, m_ref, ot_ref, lse_ref):
    q4 = q_ref[:, rows_of(j), :].reshape(CW, DH)

    def score_tile(kb, carry, masked, tiles=1):
        m_old, l_old = carry
        keys = key_rows(kb, tiles)
        s = nt_dot(k_ref[keys, :], q4) * EXP2_SCALE
        if masked:
            s = jnp.where(causal_tile(), s, -1e30)
        m_new = jnp.maximum(m_old, jnp.max(s, axis=0, keepdims=True))
        e = jnp.exp2(s - m_new)
        e_ref[keys, :] = e
        for i in range(tiles):
            m_ref[pl.ds(kb * tiles + i, 1), :] = m_new
        return m_new, l_old * jnp.exp2(m_old - m_new) + jnp.sum(e, axis=0, keepdims=True)

    carry = (jnp.full((1, CW), -1e30, F32), jnp.zeros((1, CW), F32))
    carry = score_tile(j, carry, True)
    m_fin, l_fin = by_pairs(j, functools.partial(score_tile, masked=False), carry)
    inv_l = 1.0 / l_fin
    lse = m_fin + jnp.log2(l_fin)

    def out_tile(kb, acc, tiles=1):
        parts = []
        for i in range(tiles):
            f = jnp.exp2(m_ref[pl.ds(kb * tiles + i, 1), :] - m_fin) * inv_l
            parts.append((e_ref[rows_of(kb * tiles + i), :] * f).astype(BF16))
        return acc + dot(vt_ref[:, key_rows(kb, tiles)], jnp.concatenate(parts, axis=0))

    acc = by_pairs(j + 1, out_tile, jnp.zeros((DH, CW), F32)).astype(BF16)
    dst = rows_of(stored_block(j))
    for h in range(HEADS):
        ot_ref[DH * h:DH * (h + 1), dst] = acc[:, BLK * h:BLK * (h + 1)]
        lse_ref[h:h + 1, rows_of(j)] = lse[:, BLK * h:BLK * (h + 1)]


def nth_peer(e):
    hp, cp = lax.axis_index('hp'), lax.axis_index('cp')
    m, b = e // 2, e % 2
    px = (hp % 2 + m % 2) % 2
    py = (hp // 2 + m // 2) % 2
    return py * 2 + px, (cp + b) % 2


def attention_kernel(x_own, dy_own, gain_ref, wq_hbm, wk_hbm, wv_hbm, wo_hbm, tab_own,
                     dy_all, ht_out, gq_ref, ot_all,
                     xg, ht, e_ref, m_ref, vt_ref, wq, wk, wv, wkv, stage, q_ref, k_ref, v_ref, ot_ref, lse_ref, tabs,
                     wo, wot, do_ref, kt_ref, dk_ref, dv_ref, give, take,
                     local_sem, dy_sem, t_send, t_recv, x_send, x_recv, dy_send, dy_recv, o_send, o_recv, pair_send, pair_recv):
    hp, cp, xn, yn, dn = neighbours()
    mine = tok_slot(hp, cp)
    hw = HEADS * DH
    loads = [
        pltpu.make_async_copy(x_own, xg.at[mine], local_sem.at[0]),
        pltpu.make_async_copy(wq_hbm.at[:, pl.ds(pl.multiple_of(head_slot(hp, cp) * hw, hw), hw)], wq, local_sem.at[1]),
        pltpu.make_async_copy(wk_hbm.at[:, pl.ds(pl.multiple_of((hp // 2) * 128, 128), 128)], wk, local_sem.at[2]),
        pltpu.make_async_copy(wv_hbm.at[:, pl.ds(pl.multiple_of((hp // 2) * 128, 128), 128)], wv, local_sem.at[3]),
        pltpu.make_async_copy(dy_own, stage, local_sem.at[4]),
        pltpu.make_async_copy(tab_own, tabs.at[mine], local_sem.at[5]),
    ]
    for load in loads:
        load.start()
    wo_load = pltpu.make_async_copy(wo_hbm.at[pl.ds(pl.multiple_of(head_slot(hp, cp) * hw, hw), hw)], wo, local_sem.at[8])
    wo_load.start()
    enter_barrier()
    gx = Gather(x_own, xg, tok_slot, x_send, x_recv, BLK)
    gdy = Gather(dy_own, dy_all, tok_slot, dy_send, dy_recv, BLK)

    gt = Gather(tab_own, tabs, tok_slot, t_send, t_recv, 128)
    gt.start_own()
    gx.start_own()
    for load in loads[1:4]:
        load.wait()
    lane = lax.broadcasted_iota(jnp.int32, wk.shape, 1)
    swap = hp % 2 == 1
    kf, vf = wk[...].astype(F32), wv[...].astype(F32)
    k_sel = jnp.where(swap, pltpu.roll(kf, DH, 1), kf)
    v_sel = jnp.where(swap, vf, pltpu.roll(vf, DH, 1))
    wkv[...] = jnp.where(lane < DH, k_sel, v_sel).astype(BF16)
    wo_load.wait()
    wot[...] = wo[...].T
    for i in (0, 4, 5):
        loads[i].wait()
    dy_mine = pltpu.make_async_copy(stage, dy_all.at[mine], local_sem.at[6])
    dy_mine.start()
    def project(e, _):
        @pl.when(e == 1)
        def _():
            gt.await_sibling(3)
            gx.await_sibling(3)

        @pl.when(e == 2)
        def _():
            gt.relay_near()
            gx.relay_near()
            gdy.start_own()

        @pl.when(e == 3)
        def _():
            gt.await_sibling(4)
            gx.await_sibling(4)

        @pl.when(e == 5)
        def _():
            gt.await_sibling(5)
            gx.await_sibling(5)

        @pl.when(e == 6)
        def _():
            gt.relay_diagonal()
            gx.relay_diagonal()

        @pl.when(e == 7)
        def _():
            gt.await_sibling(6)
            gx.await_sibling(6)

        d = tok_slot(*nth_peer(e))
        project_block(d, xg[d], gain_ref[...], wq, wkv, tabs[d], ht, q_ref, k_ref, v_ref)
        return 0

    lax.fori_loop(0, NB, project, 0)
    ht_copy = pltpu.make_async_copy(ht, ht_out, local_sem.at[7])
    ht_copy.start()
    vt_ref[...] = v_ref[...].T

    def attend(j, _):
        for c in range(CHUNKS):
            @pl.when(j == (1, 3, 5, 6)[c])
            def _():
                gdy.relay_near((c,))

        attend_block(j, q_ref, k_ref, vt_ref, e_ref, m_ref, ot_ref, lse_ref)
        return 0

    lax.fori_loop(0, NB, attend, 0)
    go = Gather(ot_ref, ot_all, head_slot, o_send, o_recv, hw)
    kt_ref[...] = k_ref[...].T
    dk_ref[...] = jnp.zeros_like(dk_ref)
    dv_ref[...] = jnp.zeros_like(dv_ref)
    go.start_own()
    ot_mine = pltpu.make_async_copy(ot_ref, ot_all.at[head_slot(hp, cp)], local_sem.at[9])
    ot_mine.start()
    gx.finish_sends()
    dy_mine.wait()

    def dy_load(e):
        d = tok_slot(*nth_peer(e))
        return pltpu.make_async_copy(dy_all.at[d], xg.at[d], dy_sem.at[e])

    def project_dy(e, _):
        dy_load(e).wait()
        d = tok_slot(*nth_peer(e))
        do = dot(xg[d], wot[...]).astype(BF16)
        dst = rows_of(seq_block(d))
        for h in range(HEADS):
            do_ref[h, dst, :] = do[:, DH * h:DH * (h + 1)]
        return 0

    for number in (3, 4, 5):
        gdy.await_sibling(number)
    for e in range(6):
        dy_load(e).start()
    lax.fori_loop(0, 6, project_dy, 0)
    gdy.relay_diagonal()
    dy_load(6).start()
    gdy.await_sibling(6)
    dy_load(7).start()
    lax.fori_loop(6, NB, project_dy, 0)

    def attend_back(j, _):
        for c in range(CHUNKS):
            @pl.when(j == (2, 4, 5, 6)[c])
            def _():
                go.relay_near((c,))

        slot = stored_block(j)
        src = rows_of(slot)
        q4 = q_ref[:, rows_of(j), :].reshape(CW, DH)
        do4 = do_ref[:, rows_of(j), :].reshape(CW, DH)
        o4t = jnp.concatenate([ot_ref[DH * h:DH * (h + 1), src] for h in range(HEADS)], axis=1)
        lse = jnp.concatenate([lse_ref[h:h + 1, rows_of(j)] for h in range(HEADS)], axis=1)
        delta = jnp.sum(do4.astype(F32).T * o4t.astype(F32), axis=0, keepdims=True)

        def tile(kb, dqt, masked, tiles=1):
            keys = key_rows(kb, tiles)
            p = jnp.exp2(nt_dot(k_ref[keys, :], q4) * EXP2_SCALE - lse)
            if masked:
                p = jnp.where(causal_tile(), p, 0.0)
            dp = nt_dot(v_ref[keys, :], do4)
            dv_ref[keys, :] += dot(p.astype(BF16), do4)
            ds = (p * (dp - delta)).astype(BF16)
            dk_ref[keys, :] += dot(ds, q4)
            return dqt + dot(kt_ref[:, keys], ds)

        dqt = tile(j, jnp.zeros((DH, CW), F32), True)
        dqt = by_pairs(j, functools.partial(tile, masked=False), dqt) * (DH ** -0.5)
        cos_t, sin_t = unpack_table(tabs[slot])
        for p in range(HEADS // 2):
            pair = jnp.concatenate([dqt[:, BLK * (2 * p):BLK * (2 * p + 1)], dqt[:, BLK * (2 * p + 1):BLK * (2 * p + 2)]], axis=0)
            dq = pair.T.astype(BF16).astype(F32)
            gq_ref[src, 128 * p:128 * (p + 1)] = rope_pairs(dq, cos_t, -sin_t).astype(BF16)
        return 0

    lax.fori_loop(0, NB, attend_back, 0)
    give[:, :DH] = (dk_ref[...] * (DH ** -0.5)).astype(BF16)
    give[:, DH:] = dv_ref[...].astype(BF16)
    swap = pltpu.make_async_remote_copy(
        src_ref=give, dst_ref=take, send_sem=pair_send, recv_sem=pair_recv, device_id=(hp, 1 - cp), device_id_type=MESH)
    go.relay_diagonal()
    swap.start()
    for number in (3, 4, 5):
        go.await_sibling(number)
    swap.wait_recv()
    lane = lax.broadcasted_iota(jnp.int32, (BLK, 2 * DH), 1)
    for i in range(NB // 2):
        slot = cp * 4 + i
        src = rows_of(seq_block(slot))
        total = (give[src, :].astype(F32) + take[src, :].astype(F32)).astype(BF16).astype(F32)
        cos_t, sin_t = unpack_table(tabs[slot])
        turned = rope_pairs(total, cos_t, -sin_t)
        gq_ref[NB * BLK + (i % 2) * BLK:NB * BLK + (i % 2 + 1) * BLK, 128 * (i // 2):128 * (i // 2 + 1)] = jnp.where(lane < DH, turned, total).astype(BF16)
    go.await_sibling(6)
    swap.wait_send()
    go.finish_sends()
    ot_mine.wait()
    gt.finish_sends()
    gdy.finish_sends()
    ht_copy.wait()


def flat(a_ref):
    return a_ref[...].reshape(NB * BLK, NB * BLK)


def wo_kernel(info, ot_ref, dy_ref, wo_ref, x_ref, gwo_ref, out_ref, o_mine):
    @pl.when(pl.program_id(0) == 0)
    def _():
        for d in range(NB):
            o_mine[:, BLK * d:BLK * (d + 1)] = ot_ref[d, :, rows_of(info[0])].T

    gwo_ref[...] = dot(flat(ot_ref), dy_ref[...].reshape(NB * BLK, BLK))
    out_ref[...] = (x_ref[...].astype(F32) + dot(o_mine[...], wo_ref[...])).astype(BF16)


def near_kernel(info, ht_ref, own_hbm, sib_hbm, x_hbm, y_hbm, wq_ref, gwq_ref, acc_ref, g_ref, g_sem):
    e = pl.program_id(0)
    toks = NB * BLK
    fetch = [pltpu.make_async_copy(src.at[pl.ds(0, toks)], g_ref.at[i], g_sem.at[i]) for i, src in enumerate((own_hbm, sib_hbm, x_hbm, y_hbm))]

    @pl.when(e == 0)
    def _():
        for load in fetch:
            load.start()

    for i in range(4):
        @pl.when(e == i)
        def _():
            fetch[i].wait()

    g = g_ref.at[e]
    gwq_ref[...] = dot(flat(ht_ref), g[...])
    part = nt_dot(g[rows_of(info[0]), :], wq_ref[...])

    @pl.when(e == 0)
    def _():
        acc_ref[...] = part

    @pl.when(e > 0)
    def _():
        acc_ref[...] += part


def far_kernel(info, ht_ref, own_hbm, sib_hbm, x_hbm, y_hbm, sx_hbm, sy_hbm, da_hbm, db_hbm, sda_hbm, sdb_hbm,
               wq_ref, wk_hbm, wv_hbm, x_hbm_own, dy_hbm_own, gain_ref, acc_hbm, gwq_in,
               gwq_ref, gwk_hbm, gwv_hbm, gh_ref, gg_ref,
               g_ref, kv4, gkvg, bk, bv, gwk, gwv, acc, acc_in, wk, wv, x_own, dy_own, g_sem, kv_sem, late_sem):
    e = pl.program_id(0)
    toks = NB * BLK
    half = da_hbm.shape[0]
    copy = pltpu.make_async_copy
    lo, hi = pl.ds(0, half), pl.ds(half, half)
    fetch = ((copy(sx_hbm, g_ref.at[0], g_sem.at[0]),), (copy(sy_hbm, g_ref.at[1], g_sem.at[1]),),
             (copy(da_hbm, g_ref.at[2, lo], g_sem.at[2]), copy(db_hbm, g_ref.at[2, hi], g_sem.at[3])),
             (copy(sda_hbm, g_ref.at[3, lo], g_sem.at[4]), copy(sdb_hbm, g_ref.at[3, hi], g_sem.at[5])))
    near_kv = [copy(src.at[pl.ds(toks, 2 * BLK)], kv4.at[i], kv_sem.at[i]) for i, src in enumerate((own_hbm, sib_hbm, x_hbm, y_hbm))]
    late = [copy(src, dst, late_sem.at[i]) for i, (src, dst) in enumerate(
        ((acc_hbm, acc_in), (wk_hbm, wk), (wv_hbm, wv), (x_hbm_own, x_own), (dy_hbm_own, dy_own)))]
    give = [copy(gwk, gwk_hbm, late_sem.at[5]), copy(gwv, gwv_hbm, late_sem.at[6])]

    @pl.when(e == 0)
    def _():
        fetch[0][0].start()
        for load in [c for group in fetch[1:] for c in group] + near_kv + late:
            load.start()
        fetch[0][0].wait()

    @pl.when(e == 1)
    def _():
        for load in [c for group in fetch[1:] for c in group] + near_kv:
            load.wait()
        for i in range(4):
            gkvg[info[1 + i]] = kv4[i]
            gkvg[info[5 + i]] = g_ref[i, toks:, :]
        for c in range(2):
            for r in range(2):
                dst = pl.ds((c * 2 + r) * 2 * BLK, 2 * BLK)
                for p in range(2):
                    even = gkvg[4 * p + c, :, 128 * r:128 * (r + 1)]
                    odd = gkvg[4 * p + 2 + c, :, 128 * r:128 * (r + 1)]
                    bk[dst, 128 * p:128 * (p + 1)] = jnp.concatenate([even[:, :DH], odd[:, :DH]], axis=1)
                    bv[dst, 128 * p:128 * (p + 1)] = jnp.concatenate([even[:, DH:], odd[:, DH:]], axis=1)
        gwk[...] = dot(flat(ht_ref), bk[...])
        gwv[...] = dot(flat(ht_ref), bv[...])
        for out in give:
            out.start()

    g = g_ref.at[e]
    part = nt_dot(g[rows_of(info[0]), :], wq_ref[...])

    @pl.when(e == 0)
    def _():
        acc[...] = part

    @pl.when(e > 0)
    def _():
        acc[...] += part

    gwq_ref[...] = dot(flat(ht_ref), g[:toks, :])

    @pl.when(e == 3)
    def _():
        for load in late:
            load.wait()
        mine = rows_of(info[0])
        d_norm = acc[...] + acc_in[...] + nt_dot(bk[mine, :], wk[...]) + nt_dot(bv[mine, :], wv[...])
        x = x_own[...].astype(F32)
        inv = lax.rsqrt(jnp.mean(x * x, axis=-1, keepdims=True) + NORM_EPS)
        x_hat = x * inv
        gg_ref[...] = jnp.sum(d_norm * x_hat, axis=0, keepdims=True)
        d_hat = d_norm * gain_ref[...]
        row_mean = jnp.mean(d_hat * x_hat, axis=-1, keepdims=True)
        gh_ref[...] = (dy_own[...].astype(F32) + inv * (d_hat - x_hat * row_mean)).astype(BF16)
        for out in give:
            out.wait()


def gain_kernel(part_ref, gg_ref, gains, send, recv):
    hp, cp = lax.axis_index('hp'), lax.axis_index('cp')
    mine = tok_slot(hp, cp)
    enter_barrier()

    def gain_copy(m):
        return pltpu.make_async_remote_copy(
            src_ref=part_ref, dst_ref=gains.at[mine], send_sem=send.at[m - 1], recv_sem=recv.at[m - 1],
            device_id=((hp + m // 2) % 4, (cp + m % 2) % 2), device_id_type=MESH)

    for m in range(1, NB):
        gain_copy(m).start()
    gains[mine] = part_ref[...]
    for m in range(1, NB):
        ref = gains.at[tok_slot((hp + 4 - m // 2) % 4, (cp + m % 2) % 2)]
        pltpu.make_async_remote_copy(
            src_ref=ref, dst_ref=ref, send_sem=send.at[m - 1], recv_sem=recv.at[m - 1],
            device_id=(hp, 1 - cp), device_id_type=MESH).wait_recv()
    total = gains[0]
    for d in range(1, NB):
        total = total + gains[d]
    gg_ref[...] = total
    for m in range(1, NB):
        gain_copy(m).wait_send()


VMEM_SPEC = pl.BlockSpec(memory_space=pltpu.VMEM)
ANY_SPEC = pl.BlockSpec(memory_space=pl.ANY)


def run_attention(x_own, dy_own, gain, w_q, w_k, w_v, w_o, tab):
    rows, width = x_own.shape
    toks = rows * NB
    hw = HEADS * DH
    dma = pltpu.SemaphoreType.DMA
    b16 = lambda *shape: pltpu.VMEM(shape, BF16)
    f32 = lambda *shape: pltpu.VMEM(shape, F32)
    return pl.pallas_call(
        attention_kernel,
        out_shape=(
            jax.ShapeDtypeStruct((NB, rows, width), BF16),
            jax.ShapeDtypeStruct((width, toks), BF16),
            jax.ShapeDtypeStruct((toks + 2 * BLK, hw), BF16),
            jax.ShapeDtypeStruct((NB, hw, toks), BF16),
        ),
        in_specs=[ANY_SPEC, ANY_SPEC, VMEM_SPEC] + [ANY_SPEC] * 5,
        out_specs=(ANY_SPEC, ANY_SPEC, VMEM_SPEC, ANY_SPEC),
        scratch_shapes=[
            b16(NB, rows, width), b16(width, toks), f32(toks, CW), f32(NB, CW), b16(DH, toks),
            b16(width, hw), b16(width, 128), b16(width, 128), b16(width, 128), b16(rows, width),
            b16(HEADS, toks, DH), b16(toks, DH), b16(toks, DH), b16(hw, toks), f32(HEADS, toks), f32(NB, 128, 128),
            b16(hw, width), b16(width, hw), b16(HEADS, toks, DH), b16(DH, toks), f32(toks, DH), f32(toks, DH), b16(toks, 2 * DH), b16(toks, 2 * DH),
            dma((10,)), dma((NB,)),
        ] + gather_sems() * 4 + [dma, dma],
        compiler_params=pltpu.CompilerParams(vmem_limit_bytes=60 * 1024 * 1024, collective_id=0, has_side_effects=True),
        cost_estimate=pl.CostEstimate(flops=70_000_000_000, bytes_accessed=40_000_000, transcendentals=0),
        name="attention",
    )(x_own, dy_own, gain, w_q, w_k, w_v, w_o, tab)


def grid_call(kernel, steps, info, args, in_specs, out_shape, out_specs, scratch, flops, name, aliases=None):
    return pl.pallas_call(
        kernel,
        out_shape=out_shape,
        grid_spec=pltpu.PrefetchScalarGridSpec(
            num_scalar_prefetch=1, grid=(steps,), in_specs=in_specs, out_specs=out_specs, scratch_shapes=scratch),
        input_output_aliases=aliases or {},
        compiler_params=pltpu.CompilerParams(vmem_limit_bytes=60 * 1024 * 1024),
        cost_estimate=pl.CostEstimate(flops=flops, bytes_accessed=40_000_000, transcendentals=0),
        name=name,
    )(info, *args)


def whole_block(a):
    return pl.BlockSpec(a.shape, lambda n, info: (0,) * len(a.shape))


def run_wo(info, ot_all, dy_all, w_o, x_own):
    rows, width = x_own.shape
    hw = HEADS * DH
    cols = lambda r: pl.BlockSpec((r, BLK), lambda n, info: (0, n))
    return grid_call(
        wo_kernel, NB, info, (ot_all, dy_all, w_o, x_own),
        [VMEM_SPEC, pl.BlockSpec((NB, rows, BLK), lambda n, info: (0, 0, n)), cols(NB * hw), cols(rows)],
        (jax.ShapeDtypeStruct((NB * hw, width), F32), jax.ShapeDtypeStruct((rows, width), BF16)),
        (cols(NB * hw), cols(rows)),
        [pltpu.VMEM((rows, NB * hw), BF16)], 20_000_000_000, "wo_grad")


def run_near(info, h_t, own, sib, x, y, w_q):
    width, toks = w_q.shape[0], NB * BLK
    cols = pl.BlockSpec((width, BLK), lambda n, info: (0, info[1 + n]))
    acc = jax.ShapeDtypeStruct((BLK, width), F32)
    dma = pltpu.SemaphoreType.DMA
    return grid_call(
        near_kernel, 4, info, (h_t, own, sib, x, y, w_q), [VMEM_SPEC] + [ANY_SPEC] * 4 + [cols],
        (jax.ShapeDtypeStruct((width, NB * BLK), F32), acc), (cols, whole_block(acc)),
        [pltpu.VMEM((4, toks, BLK), BF16), dma((4,))], 10_000_000_000, "wq_near")


def run_far(info, h_t, near, sx, sy, d_a, d_b, sd_a, sd_b, w_q, w_k, w_v, x_own, dy_own, gain, acc, gwq):
    width, toks = w_q.shape[0], NB * BLK
    rows, kv = x_own.shape[0], w_k.shape[1]
    cols = pl.BlockSpec((width, BLK), lambda n, info: (0, info[5 + n]))
    outs = (jax.ShapeDtypeStruct((width, NB * BLK), F32), jax.ShapeDtypeStruct((width, kv), F32), jax.ShapeDtypeStruct((width, kv), F32),
            jax.ShapeDtypeStruct((rows, width), BF16), jax.ShapeDtypeStruct((1, width), F32))
    dma = pltpu.SemaphoreType.DMA
    b16 = lambda *shape: pltpu.VMEM(shape, BF16)
    f32 = lambda *shape: pltpu.VMEM(shape, F32)
    return grid_call(
        far_kernel, 4, info,
        (h_t, *near, sx, sy, d_a, d_b, sd_a, sd_b, w_q, w_k, w_v, x_own, dy_own, gain, acc, gwq),
        [VMEM_SPEC] + [ANY_SPEC] * 10 + [cols] + [ANY_SPEC] * 4 + [VMEM_SPEC] + [ANY_SPEC] * 2,
        outs, (cols, ANY_SPEC, ANY_SPEC, whole_block(outs[3]), whole_block(outs[4])),
        [b16(4, toks + 2 * BLK, BLK), b16(4, 2 * BLK, BLK), b16(NB, 2 * BLK, BLK), b16(toks, kv), b16(toks, kv),
         f32(width, kv), f32(width, kv), f32(rows, width), f32(rows, width), b16(width, kv), b16(width, kv), b16(rows, width), b16(rows, width),
         dma((6,)), dma((4,)), dma((7,))],
        15_000_000_000, "wq_far", aliases={19: 0})


def run_gain(part):
    dma = pltpu.SemaphoreType.DMA
    return pl.pallas_call(
        gain_kernel, out_shape=jax.ShapeDtypeStruct(part.shape, F32), in_specs=[VMEM_SPEC], out_specs=VMEM_SPEC,
        scratch_shapes=[pltpu.VMEM((NB,) + part.shape, F32), dma((7,)), dma((7,))],
        compiler_params=pltpu.CompilerParams(collective_id=2, has_side_effects=True), name="gain_sum")(part)


def solution(mesh):
    def device_step(hidden, grad_out, positions, norm_gain, w_q, w_k, w_v, w_o, inv_freq):
        lane = jnp.arange(128)[None, :]
        pos = positions.reshape(2, 128)
        token = jnp.where(lane < 64, pos[0][:, None], pos[1][:, None]).astype(F32)
        angles = token * jnp.tile(inv_freq, 4)[None, :]
        tab = jnp.where(lane % 64 < 32, jnp.cos(angles), jnp.sin(angles))
        gain = norm_gain.astype(F32)[None, :]
        dy_all, h_t, g, ot_all = run_attention(hidden, grad_out, gain, w_q, w_k, w_v, w_o, tab)
        h_t = h_t.reshape(NB, BLK, -1)
        hp, cp, xn, yn, dn = neighbours()
        slots = [head_slot(a, b) for a, b in ((hp, cp), (hp, 1 - cp), (xn, cp), (yn, cp), (xn, 1 - cp), (yn, 1 - cp), (dn, cp), (dn, 1 - cp))]
        info = jnp.stack([tok_slot(hp, cp)] + slots).astype(jnp.int32)
        along_x = lambda a: lax.ppermute(a, 'hp', [(i, i ^ 1) for i in range(4)])
        along_y = lambda a: lax.ppermute(a, 'hp', [(i, i ^ 2) for i in range(4)])
        to_sib = lambda a: lax.ppermute(a, 'cp', [(0, 1), (1, 0)])
        half = g.shape[0] // 2
        x, y, sib = along_x(g), along_y(g), to_sib(g)
        grad_wo, output = run_wo(info, ot_all, dy_all, w_o, hidden)
        x, y, sib, output = lax.optimization_barrier((x, y, sib, output))
        d_a, d_b = along_y(x[:half]), along_x(y[half:])
        sx, sy = to_sib(x), to_sib(y)
        gwq, acc = run_near(info, h_t, g, sib, x, y, w_q)
        d_a, d_b, acc = lax.optimization_barrier((d_a, d_b, acc))
        sd_a, sd_b = to_sib(d_a), to_sib(d_b)
        grad_wq, grad_wk, grad_wv, grad_hidden, part = run_far(
            info, h_t, (g, sib, x, y), sx, sy, d_a, d_b, sd_a, sd_b, w_q, w_k, w_v, hidden, grad_out, gain, acc, gwq)
        grad_gain = run_gain(part)
        return output, grad_hidden, grad_wq, grad_wk, grad_wv, grad_wo, grad_gain[0]

    seq_spec = P(('cp', 'hp'), None)
    whole = P()
    return jax.shard_map(device_step, mesh=mesh, in_specs=(seq_spec, seq_spec, P(('cp', 'hp')), whole, whole, whole, whole, whole, whole), out_specs=(seq_spec, seq_spec, whole, whole, whole, whole, whole), check_vma=False)
```

```python
import functools
import math

import jax
import jax.numpy as jnp
from jax import lax
from jax.experimental import pallas as pl
from jax.experimental.pallas import tpu as pltpu
from jax.sharding import PartitionSpec as P

NORM_EPS = 1e-5
BLK = 256
HEADS = 4
DH = 64
NB = 8
CW = HEADS * BLK
EXP2_SCALE = (DH ** -0.5) * math.log2(math.e)
F32 = jnp.float32
BF16 = jnp.bfloat16


def seq_block(d):
    cp, half, sub = d // 4, (d // 2) % 2, d % 2
    return 2 * ((1 - half) * cp + half * (3 - cp)) + sub


def stored_block(j):
    b, sub = j // 2, j % 2
    half = b // 2
    cp = (1 - half) * b + half * (3 - b)
    return cp * 4 + half * 2 + sub


def nt_dot(a, b):
    return lax.dot_general(a, b, (((1,), (1,)), ((), ())), preferred_element_type=F32)


def dot(a, b):
    return jnp.dot(a, b, preferred_element_type=F32)


def rope_pairs(t, cos_t, sin_t):
    lane = lax.broadcasted_iota(jnp.int32, t.shape, 1)
    partner = jnp.where(lane % DH < DH // 2, pltpu.roll(t, 128 - DH // 2, 1), pltpu.roll(t, DH // 2, 1))
    return t * cos_t + partner * sin_t


def rows_of(b):
    return pl.ds(pl.multiple_of(b * BLK, BLK), BLK)


def key_rows(kb, tiles):
    return pl.ds(pl.multiple_of(kb * tiles * BLK, tiles * BLK), tiles * BLK)


def by_pairs(count, tile, carry):
    carry = lax.fori_loop(0, count // 2, functools.partial(tile, tiles=2), carry)
    return lax.fori_loop(count - count % 2, count, tile, carry)


def causal_tile():
    row = lax.broadcasted_iota(jnp.int32, (BLK, CW), 0)
    col = lax.broadcasted_iota(jnp.int32, (BLK, CW), 1)
    return row <= col % BLK


MESH = pl.DeviceIdType.MESH
CHUNKS = 4


def neighbours():
    hp, cp = lax.axis_index('hp'), lax.axis_index('cp')
    flip = 1 - 2 * (hp % 2)
    y_hp = (hp + 2) % 4
    return hp, cp, hp + flip, y_hp, y_hp + flip


def tok_slot(hp, cp):
    return cp * 4 + hp


def head_slot(hp, cp):
    return hp * 2 + cp


def enter_barrier():
    hp, cp = lax.axis_index('hp'), lax.axis_index('cp')
    barrier = pltpu.get_barrier_semaphore()
    for m in range(1, 8):
        pl.semaphore_signal(barrier, inc=1, device_id=((hp + m // 2) % 4, (cp + m % 2) % 2), device_id_type=MESH)
    pl.semaphore_wait(barrier, 7)


class Gather:
    def __init__(self, src, dst, slot, send, recv, rows):
        self.src, self.dst, self.slot, self.send, self.recv = src, dst, slot, send, recv
        self.step = rows // CHUNKS
        self.hp, self.cp, self.xn, self.yn, self.dn = neighbours()

    def part(self, ref, c):
        return ref.at[pl.ds(c * self.step, self.step)]

    def place(self, hp, cp, c):
        return self.part(self.dst.at[self.slot(hp, cp)], c)

    def copy(self, kind, c):
        hp, cp, xn, yn, dn = self.hp, self.cp, self.xn, self.yn, self.dn
        origin, lands, to = {
            'own_x': (hp, 0, (xn, cp)), 'own_y': (hp, 1, (yn, cp)), 'own_s': (hp, 3, (hp, 1 - cp)),
            'x_s': (xn, 4, (hp, 1 - cp)), 'y_s': (yn, 5, (hp, 1 - cp)), 'd_s': (dn, 6, (hp, 1 - cp)),
            'x_y': (xn, 2, (yn, cp)), 'y_x': (yn, 2, (xn, cp)),
        }[kind]
        number = ('own_x', 'own_y', 'own_s', 'x_s', 'y_s', 'd_s', 'x_y', 'y_x').index(kind)
        src = self.part(self.src, c) if kind.startswith('own') else self.place(origin, cp, c)
        return pltpu.make_async_remote_copy(
            src_ref=src, dst_ref=self.place(origin, cp, c), send_sem=self.send.at[number, c],
            recv_sem=self.recv.at[lands, c], device_id=to, device_id_type=MESH)

    def await_from(self, number, c):
        hp, cp = ((self.xn, self.cp), (self.yn, self.cp), (self.dn, self.cp), (self.hp, 1 - self.cp),
                  (self.xn, 1 - self.cp), (self.yn, 1 - self.cp), (self.dn, 1 - self.cp))[number]
        ref = self.place(hp, cp, c)
        pltpu.make_async_remote_copy(
            src_ref=ref, dst_ref=ref, send_sem=self.send.at[0, c], recv_sem=self.recv.at[number, c],
            device_id=(self.hp, 1 - self.cp), device_id_type=MESH).wait_recv()

    def start_own(self):
        for c in range(CHUNKS):
            for kind in ('own_x', 'own_y', 'own_s'):
                self.copy(kind, c).start()

    def relay_near(self, chunks=range(CHUNKS)):
        for c in chunks:
            self.await_from(0, c)
            self.copy('x_s', c).start()
            if c < CHUNKS // 2:
                self.copy('x_y', c).start()
            self.await_from(1, c)
            self.copy('y_s', c).start()
            if c >= CHUNKS // 2:
                self.copy('y_x', c).start()

    def relay_diagonal(self):
        for c in range(CHUNKS):
            self.await_from(2, c)
            self.copy('d_s', c).start()

    def await_sibling(self, number):
        for c in range(CHUNKS):
            self.await_from(number, c)

    def finish_sends(self):
        for c in range(CHUNKS):
            for kind in ('own_x', 'own_y', 'own_s', 'x_s', 'y_s', 'd_s'):
                self.copy(kind, c).wait_send()
            self.copy('x_y' if c < CHUNKS // 2 else 'y_x', c).wait_send()


def gather_sems():
    return [pltpu.SemaphoreType.DMA((8, CHUNKS)), pltpu.SemaphoreType.DMA((7, CHUNKS))]


def unpack_table(tab):
    group = lax.broadcasted_iota(jnp.int32, tab.shape, 1) // (DH // 2)
    turned = [tab] + [pltpu.roll(tab, 32 * i, 1) for i in (1, 2, 3)]

    def pick(order):
        out = turned[order[3]]
        for g in range(3):
            out = jnp.where(group == g, turned[order[g]], out)
        return out

    sign = jnp.where(group % 2 == 0, -1.0, 1.0)
    cos_t = jnp.concatenate([pick((0, 1, 2, 3)), pick((2, 3, 0, 1))], axis=0)
    sin_t = jnp.concatenate([pick((3, 0, 1, 2)) * sign, pick((1, 2, 3, 0)) * sign], axis=0)
    return cos_t, sin_t


def project_block(d, x, gain, wq_ref, wkv_ref, tab, ht_ref, q_ref, k_ref, v_ref):
    xf = x.astype(F32)
    inv = lax.rsqrt(jnp.mean(xf * xf, axis=-1, keepdims=True) + NORM_EPS)
    h = (xf * inv * gain).astype(BF16)
    ht_ref[:, rows_of(d)] = h.T
    dst = rows_of(seq_block(d))
    cos_t, sin_t = unpack_table(tab)
    y = dot(h, wq_ref[...])
    for p in range(HEADS // 2):
        qr = rope_pairs(y[:, 128 * p:128 * (p + 1)], cos_t, sin_t).astype(BF16)
        q_ref[2 * p, dst, :] = qr[:, :DH]
        q_ref[2 * p + 1, dst, :] = qr[:, DH:]
    kv = dot(h, wkv_ref[...])
    k_ref[dst, :] = rope_pairs(kv, cos_t, sin_t).astype(BF16)[:, :DH]
    v_ref[dst, :] = kv.astype(BF16)[:, DH:]


def attend_block(j, q_ref, k_ref, vt_ref, e_ref, m_ref, ot_ref, lse_ref):
    q4 = q_ref[:, rows_of(j), :].reshape(CW, DH)

    def score_tile(kb, carry, masked, tiles=1):
        m_old, l_old = carry
        keys = key_rows(kb, tiles)
        s = nt_dot(k_ref[keys, :], q4) * EXP2_SCALE
        if masked:
            s = jnp.where(causal_tile(), s, -1e30)
        m_new = jnp.maximum(m_old, jnp.max(s, axis=0, keepdims=True))
        e = jnp.exp2(s - m_new)
        e_ref[keys, :] = e
        for i in range(tiles):
            m_ref[pl.ds(kb * tiles + i, 1), :] = m_new
        return m_new, l_old * jnp.exp2(m_old - m_new) + jnp.sum(e, axis=0, keepdims=True)

    carry = (jnp.full((1, CW), -1e30, F32), jnp.zeros((1, CW), F32))
    carry = score_tile(j, carry, True)
    m_fin, l_fin = by_pairs(j, functools.partial(score_tile, masked=False), carry)
    inv_l = 1.0 / l_fin
    lse = m_fin + jnp.log2(l_fin)

    def out_tile(kb, acc, tiles=1):
        parts = []
        for i in range(tiles):
            f = jnp.exp2(m_ref[pl.ds(kb * tiles + i, 1), :] - m_fin) * inv_l
            parts.append((e_ref[rows_of(kb * tiles + i), :] * f).astype(BF16))
        return acc + dot(vt_ref[:, key_rows(kb, tiles)], jnp.concatenate(parts, axis=0))

    acc = by_pairs(j + 1, out_tile, jnp.zeros((DH, CW), F32)).astype(BF16)
    dst = rows_of(stored_block(j))
    for h in range(HEADS):
        ot_ref[DH * h:DH * (h + 1), dst] = acc[:, BLK * h:BLK * (h + 1)]
        lse_ref[h:h + 1, rows_of(j)] = lse[:, BLK * h:BLK * (h + 1)]


def nth_peer(e):
    hp, cp = lax.axis_index('hp'), lax.axis_index('cp')
    m, b = e // 2, e % 2
    px = (hp % 2 + m % 2) % 2
    py = (hp // 2 + m // 2) % 2
    return py * 2 + px, (cp + b) % 2


def attention_kernel(x_own, dy_own, gain_ref, wq_hbm, wk_hbm, wv_hbm, wo_hbm, tab_own,
                     dy_all, ht_out, gq_ref, ot_all,
                     xg, ht, e_ref, m_ref, vt_ref, wq, wk, wv, wkv, stage, q_ref, k_ref, v_ref, ot_ref, lse_ref, tabs,
                     wo, wot, do_ref, kt_ref, dk_ref, dv_ref, give, take,
                     local_sem, dy_sem, t_send, t_recv, x_send, x_recv, dy_send, dy_recv, o_send, o_recv, pair_send, pair_recv):
    hp, cp, xn, yn, dn = neighbours()
    mine = tok_slot(hp, cp)
    hw = HEADS * DH
    loads = [
        pltpu.make_async_copy(x_own, xg.at[mine], local_sem.at[0]),
        pltpu.make_async_copy(wq_hbm.at[:, pl.ds(pl.multiple_of(head_slot(hp, cp) * hw, hw), hw)], wq, local_sem.at[1]),
        pltpu.make_async_copy(wk_hbm.at[:, pl.ds(pl.multiple_of((hp // 2) * 128, 128), 128)], wk, local_sem.at[2]),
        pltpu.make_async_copy(wv_hbm.at[:, pl.ds(pl.multiple_of((hp // 2) * 128, 128), 128)], wv, local_sem.at[3]),
        pltpu.make_async_copy(dy_own, stage, local_sem.at[4]),
        pltpu.make_async_copy(tab_own, tabs.at[mine], local_sem.at[5]),
    ]
    for load in loads:
        load.start()
    wo_load = pltpu.make_async_copy(wo_hbm.at[pl.ds(pl.multiple_of(head_slot(hp, cp) * hw, hw), hw)], wo, local_sem.at[8])
    wo_load.start()
    enter_barrier()
    gx = Gather(x_own, xg, tok_slot, x_send, x_recv, BLK)
    gdy = Gather(dy_own, dy_all, tok_slot, dy_send, dy_recv, BLK)

    gt = Gather(tab_own, tabs, tok_slot, t_send, t_recv, 128)
    gt.start_own()
    gx.start_own()
    for load in loads[1:4]:
        load.wait()
    lane = lax.broadcasted_iota(jnp.int32, wk.shape, 1)
    swap = hp % 2 == 1
    kf, vf = wk[...].astype(F32), wv[...].astype(F32)
    k_sel = jnp.where(swap, pltpu.roll(kf, DH, 1), kf)
    v_sel = jnp.where(swap, vf, pltpu.roll(vf, DH, 1))
    wkv[...] = jnp.where(lane < DH, k_sel, v_sel).astype(BF16)
    wo_load.wait()
    wot[...] = wo[...].T
    for i in (0, 4, 5):
        loads[i].wait()
    dy_mine = pltpu.make_async_copy(stage, dy_all.at[mine], local_sem.at[6])
    dy_mine.start()
    def project(e, _):
        @pl.when(e == 1)
        def _():
            gt.await_sibling(3)
            gx.await_sibling(3)

        @pl.when(e == 2)
        def _():
            gt.relay_near()
            gx.relay_near()
            gdy.start_own()

        @pl.when(e == 3)
        def _():
            gt.await_sibling(4)
            gx.await_sibling(4)

        @pl.when(e == 5)
        def _():
            gt.await_sibling(5)
            gx.await_sibling(5)

        @pl.when(e == 6)
        def _():
            gt.relay_diagonal()
            gx.relay_diagonal()

        @pl.when(e == 7)
        def _():
            gt.await_sibling(6)
            gx.await_sibling(6)

        d = tok_slot(*nth_peer(e))
        project_block(d, xg[d], gain_ref[...], wq, wkv, tabs[d], ht, q_ref, k_ref, v_ref)
        return 0

    lax.fori_loop(0, NB, project, 0)
    ht_copy = pltpu.make_async_copy(ht, ht_out, local_sem.at[7])
    ht_copy.start()
    vt_ref[...] = v_ref[...].T

    def attend(j, _):
        for c in range(CHUNKS):
            @pl.when(j == (2, 4, 6, 7)[c])
            def _():
                gdy.relay_near((c,))

        attend_block(j, q_ref, k_ref, vt_ref, e_ref, m_ref, ot_ref, lse_ref)
        return 0

    lax.fori_loop(0, NB, attend, 0)
    go = Gather(ot_ref, ot_all, head_slot, o_send, o_recv, hw)
    kt_ref[...] = k_ref[...].T
    dk_ref[...] = jnp.zeros_like(dk_ref)
    dv_ref[...] = jnp.zeros_like(dv_ref)
    go.start_own()
    ot_mine = pltpu.make_async_copy(ot_ref, ot_all.at[head_slot(hp, cp)], local_sem.at[9])
    ot_mine.start()
    gx.finish_sends()
    dy_mine.wait()

    def dy_load(e):
        d = tok_slot(*nth_peer(e))
        return pltpu.make_async_copy(dy_all.at[d], xg.at[d], dy_sem.at[e])

    def project_dy(e, _):
        dy_load(e).wait()
        d = tok_slot(*nth_peer(e))
        do = dot(xg[d], wot[...]).astype(BF16)
        dst = rows_of(seq_block(d))
        for h in range(HEADS):
            do_ref[h, dst, :] = do[:, DH * h:DH * (h + 1)]
        return 0

    for number in (3, 4, 5):
        gdy.await_sibling(number)
    for e in range(6):
        dy_load(e).start()
    lax.fori_loop(0, 6, project_dy, 0)
    gdy.relay_diagonal()
    dy_load(6).start()
    gdy.await_sibling(6)
    dy_load(7).start()
    lax.fori_loop(6, NB, project_dy, 0)

    def attend_back(j, _):
        for c in range(CHUNKS):
            @pl.when(j == (2, 4, 5, 6)[c])
            def _():
                go.relay_near((c,))

        slot = stored_block(j)
        src = rows_of(slot)
        q4 = q_ref[:, rows_of(j), :].reshape(CW, DH)
        do4 = do_ref[:, rows_of(j), :].reshape(CW, DH)
        o4t = jnp.concatenate([ot_ref[DH * h:DH * (h + 1), src] for h in range(HEADS)], axis=1)
        lse = jnp.concatenate([lse_ref[h:h + 1, rows_of(j)] for h in range(HEADS)], axis=1)
        delta = jnp.sum(do4.astype(F32).T * o4t.astype(F32), axis=0, keepdims=True)

        def tile(kb, dqt, masked, tiles=1):
            keys = key_rows(kb, tiles)
            p = jnp.exp2(nt_dot(k_ref[keys, :], q4) * EXP2_SCALE - lse)
            if masked:
                p = jnp.where(causal_tile(), p, 0.0)
            dp = nt_dot(v_ref[keys, :], do4)
            dv_ref[keys, :] += dot(p.astype(BF16), do4)
            ds = (p * (dp - delta)).astype(BF16)
            dk_ref[keys, :] += dot(ds, q4)
            return dqt + dot(kt_ref[:, keys], ds)

        dqt = tile(j, jnp.zeros((DH, CW), F32), True)
        dqt = by_pairs(j, functools.partial(tile, masked=False), dqt) * (DH ** -0.5)
        cos_t, sin_t = unpack_table(tabs[slot])
        for p in range(HEADS // 2):
            pair = jnp.concatenate([dqt[:, BLK * (2 * p):BLK * (2 * p + 1)], dqt[:, BLK * (2 * p + 1):BLK * (2 * p + 2)]], axis=0)
            dq = pair.T.astype(BF16).astype(F32)
            gq_ref[src, 128 * p:128 * (p + 1)] = rope_pairs(dq, cos_t, -sin_t).astype(BF16)
        return 0

    lax.fori_loop(0, NB, attend_back, 0)
    give[:, :DH] = (dk_ref[...] * (DH ** -0.5)).astype(BF16)
    give[:, DH:] = dv_ref[...].astype(BF16)
    swap = pltpu.make_async_remote_copy(
        src_ref=give, dst_ref=take, send_sem=pair_send, recv_sem=pair_recv, device_id=(hp, 1 - cp), device_id_type=MESH)
    go.relay_diagonal()
    swap.start()
    for number in (3, 4, 5):
        go.await_sibling(number)
    swap.wait_recv()
    lane = lax.broadcasted_iota(jnp.int32, (BLK, 2 * DH), 1)
    for i in range(NB // 2):
        slot = cp * 4 + i
        src = rows_of(seq_block(slot))
        total = (give[src, :].astype(F32) + take[src, :].astype(F32)).astype(BF16).astype(F32)
        cos_t, sin_t = unpack_table(tabs[slot])
        turned = rope_pairs(total, cos_t, -sin_t)
        gq_ref[NB * BLK + (i % 2) * BLK:NB * BLK + (i % 2 + 1) * BLK, 128 * (i // 2):128 * (i // 2 + 1)] = jnp.where(lane < DH, turned, total).astype(BF16)
    go.await_sibling(6)
    swap.wait_send()
    go.finish_sends()
    ot_mine.wait()
    gt.finish_sends()
    gdy.finish_sends()
    ht_copy.wait()


def flat(a_ref):
    return a_ref[...].reshape(NB * BLK, NB * BLK)


def wo_kernel(info, ot_ref, dy_ref, wo_ref, x_ref, gwo_ref, out_ref, o_mine):
    @pl.when(pl.program_id(0) == 0)
    def _():
        for d in range(NB):
            o_mine[:, BLK * d:BLK * (d + 1)] = ot_ref[d, :, rows_of(info[0])].T

    gwo_ref[...] = dot(flat(ot_ref), dy_ref[...].reshape(NB * BLK, BLK))
    out_ref[...] = (x_ref[...].astype(F32) + dot(o_mine[...], wo_ref[...])).astype(BF16)


def near_kernel(info, ht_ref, own_hbm, sib_hbm, x_hbm, y_hbm, wq_ref, gwq_ref, acc_ref, g_ref, g_sem):
    e = pl.program_id(0)
    toks = NB * BLK
    fetch = [pltpu.make_async_copy(src.at[pl.ds(0, toks)], g_ref.at[i], g_sem.at[i]) for i, src in enumerate((own_hbm, sib_hbm, x_hbm, y_hbm))]

    @pl.when(e == 0)
    def _():
        for load in fetch:
            load.start()

    for i in range(4):
        @pl.when(e == i)
        def _():
            fetch[i].wait()

    g = g_ref.at[e]
    gwq_ref[...] = dot(flat(ht_ref), g[...])
    part = nt_dot(g[rows_of(info[0]), :], wq_ref[...])

    @pl.when(e == 0)
    def _():
        acc_ref[...] = part

    @pl.when(e > 0)
    def _():
        acc_ref[...] += part


def far_kernel(info, ht_ref, own_hbm, sib_hbm, x_hbm, y_hbm, sx_hbm, sy_hbm, da_hbm, db_hbm, sda_hbm, sdb_hbm,
               wq_ref, wk_hbm, wv_hbm, x_hbm_own, dy_hbm_own, gain_ref, acc_hbm, gwq_in,
               gwq_ref, gwk_hbm, gwv_hbm, gh_ref, gg_ref,
               g_ref, kv4, gkvg, bk, bv, gwk, gwv, acc, acc_in, wk, wv, x_own, dy_own, g_sem, kv_sem, late_sem):
    e = pl.program_id(0)
    toks = NB * BLK
    half = da_hbm.shape[0]
    copy = pltpu.make_async_copy
    lo, hi = pl.ds(0, half), pl.ds(half, half)
    fetch = ((copy(sx_hbm, g_ref.at[0], g_sem.at[0]),), (copy(sy_hbm, g_ref.at[1], g_sem.at[1]),),
             (copy(da_hbm, g_ref.at[2, lo], g_sem.at[2]), copy(db_hbm, g_ref.at[2, hi], g_sem.at[3])),
             (copy(sda_hbm, g_ref.at[3, lo], g_sem.at[4]), copy(sdb_hbm, g_ref.at[3, hi], g_sem.at[5])))
    near_kv = [copy(src.at[pl.ds(toks, 2 * BLK)], kv4.at[i], kv_sem.at[i]) for i, src in enumerate((own_hbm, sib_hbm, x_hbm, y_hbm))]
    late = [copy(src, dst, late_sem.at[i]) for i, (src, dst) in enumerate(
        ((acc_hbm, acc_in), (wk_hbm, wk), (wv_hbm, wv), (x_hbm_own, x_own), (dy_hbm_own, dy_own)))]
    give = [copy(gwk, gwk_hbm, late_sem.at[5]), copy(gwv, gwv_hbm, late_sem.at[6])]

    @pl.when(e == 0)
    def _():
        fetch[0][0].start()
        for load in [c for group in fetch[1:] for c in group] + near_kv + late:
            load.start()
        fetch[0][0].wait()

    @pl.when(e == 1)
    def _():
        for load in [c for group in fetch[1:] for c in group] + near_kv:
            load.wait()
        for i in range(4):
            gkvg[info[1 + i]] = kv4[i]
            gkvg[info[5 + i]] = g_ref[i, toks:, :]
        for c in range(2):
            for r in range(2):
                dst = pl.ds((c * 2 + r) * 2 * BLK, 2 * BLK)
                for p in range(2):
                    even = gkvg[4 * p + c, :, 128 * r:128 * (r + 1)]
                    odd = gkvg[4 * p + 2 + c, :, 128 * r:128 * (r + 1)]
                    bk[dst, 128 * p:128 * (p + 1)] = jnp.concatenate([even[:, :DH], odd[:, :DH]], axis=1)
                    bv[dst, 128 * p:128 * (p + 1)] = jnp.concatenate([even[:, DH:], odd[:, DH:]], axis=1)
        gwk[...] = dot(flat(ht_ref), bk[...])
        gwv[...] = dot(flat(ht_ref), bv[...])
        for out in give:
            out.start()

    g = g_ref.at[e]
    part = nt_dot(g[rows_of(info[0]), :], wq_ref[...])

    @pl.when(e == 0)
    def _():
        acc[...] = part

    @pl.when(e > 0)
    def _():
        acc[...] += part

    gwq_ref[...] = dot(flat(ht_ref), g[:toks, :])

    @pl.when(e == 3)
    def _():
        for load in late:
            load.wait()
        mine = rows_of(info[0])
        d_norm = acc[...] + acc_in[...] + nt_dot(bk[mine, :], wk[...]) + nt_dot(bv[mine, :], wv[...])
        x = x_own[...].astype(F32)
        inv = lax.rsqrt(jnp.mean(x * x, axis=-1, keepdims=True) + NORM_EPS)
        x_hat = x * inv
        gg_ref[...] = jnp.sum(d_norm * x_hat, axis=0, keepdims=True)
        d_hat = d_norm * gain_ref[...]
        row_mean = jnp.mean(d_hat * x_hat, axis=-1, keepdims=True)
        gh_ref[...] = (dy_own[...].astype(F32) + inv * (d_hat - x_hat * row_mean)).astype(BF16)
        for out in give:
            out.wait()


def gain_kernel(part_ref, gg_ref, gains, send, recv):
    hp, cp = lax.axis_index('hp'), lax.axis_index('cp')
    mine = tok_slot(hp, cp)
    enter_barrier()

    def gain_copy(m):
        return pltpu.make_async_remote_copy(
            src_ref=part_ref, dst_ref=gains.at[mine], send_sem=send.at[m - 1], recv_sem=recv.at[m - 1],
            device_id=((hp + m // 2) % 4, (cp + m % 2) % 2), device_id_type=MESH)

    for m in range(1, NB):
        gain_copy(m).start()
    gains[mine] = part_ref[...]
    for m in range(1, NB):
        ref = gains.at[tok_slot((hp + 4 - m // 2) % 4, (cp + m % 2) % 2)]
        pltpu.make_async_remote_copy(
            src_ref=ref, dst_ref=ref, send_sem=send.at[m - 1], recv_sem=recv.at[m - 1],
            device_id=(hp, 1 - cp), device_id_type=MESH).wait_recv()
    total = gains[0]
    for d in range(1, NB):
        total = total + gains[d]
    gg_ref[...] = total
    for m in range(1, NB):
        gain_copy(m).wait_send()


VMEM_SPEC = pl.BlockSpec(memory_space=pltpu.VMEM)
ANY_SPEC = pl.BlockSpec(memory_space=pl.ANY)


def run_attention(x_own, dy_own, gain, w_q, w_k, w_v, w_o, tab):
    rows, width = x_own.shape
    toks = rows * NB
    hw = HEADS * DH
    dma = pltpu.SemaphoreType.DMA
    b16 = lambda *shape: pltpu.VMEM(shape, BF16)
    f32 = lambda *shape: pltpu.VMEM(shape, F32)
    return pl.pallas_call(
        attention_kernel,
        out_shape=(
            jax.ShapeDtypeStruct((NB, rows, width), BF16),
            jax.ShapeDtypeStruct((width, toks), BF16),
            jax.ShapeDtypeStruct((toks + 2 * BLK, hw), BF16),
            jax.ShapeDtypeStruct((NB, hw, toks), BF16),
        ),
        in_specs=[ANY_SPEC, ANY_SPEC, VMEM_SPEC] + [ANY_SPEC] * 5,
        out_specs=(ANY_SPEC, ANY_SPEC, VMEM_SPEC, ANY_SPEC),
        scratch_shapes=[
            b16(NB, rows, width), b16(width, toks), f32(toks, CW), f32(NB, CW), b16(DH, toks),
            b16(width, hw), b16(width, 128), b16(width, 128), b16(width, 128), b16(rows, width),
            b16(HEADS, toks, DH), b16(toks, DH), b16(toks, DH), b16(hw, toks), f32(HEADS, toks), f32(NB, 128, 128),
            b16(hw, width), b16(width, hw), b16(HEADS, toks, DH), b16(DH, toks), f32(toks, DH), f32(toks, DH), b16(toks, 2 * DH), b16(toks, 2 * DH),
            dma((10,)), dma((NB,)),
        ] + gather_sems() * 4 + [dma, dma],
        compiler_params=pltpu.CompilerParams(vmem_limit_bytes=60 * 1024 * 1024, collective_id=0, has_side_effects=True),
        cost_estimate=pl.CostEstimate(flops=70_000_000_000, bytes_accessed=40_000_000, transcendentals=0),
        name="attention",
    )(x_own, dy_own, gain, w_q, w_k, w_v, w_o, tab)


def grid_call(kernel, steps, info, args, in_specs, out_shape, out_specs, scratch, flops, name, aliases=None):
    return pl.pallas_call(
        kernel,
        out_shape=out_shape,
        grid_spec=pltpu.PrefetchScalarGridSpec(
            num_scalar_prefetch=1, grid=(steps,), in_specs=in_specs, out_specs=out_specs, scratch_shapes=scratch),
        input_output_aliases=aliases or {},
        compiler_params=pltpu.CompilerParams(vmem_limit_bytes=60 * 1024 * 1024),
        cost_estimate=pl.CostEstimate(flops=flops, bytes_accessed=40_000_000, transcendentals=0),
        name=name,
    )(info, *args)


def whole_block(a):
    return pl.BlockSpec(a.shape, lambda n, info: (0,) * len(a.shape))


def run_wo(info, ot_all, dy_all, w_o, x_own):
    rows, width = x_own.shape
    hw = HEADS * DH
    cols = lambda r: pl.BlockSpec((r, BLK), lambda n, info: (0, n))
    return grid_call(
        wo_kernel, NB, info, (ot_all, dy_all, w_o, x_own),
        [VMEM_SPEC, pl.BlockSpec((NB, rows, BLK), lambda n, info: (0, 0, n)), cols(NB * hw), cols(rows)],
        (jax.ShapeDtypeStruct((NB * hw, width), F32), jax.ShapeDtypeStruct((rows, width), BF16)),
        (cols(NB * hw), cols(rows)),
        [pltpu.VMEM((rows, NB * hw), BF16)], 20_000_000_000, "wo_grad")


def run_near(info, h_t, own, sib, x, y, w_q):
    width, toks = w_q.shape[0], NB * BLK
    cols = pl.BlockSpec((width, BLK), lambda n, info: (0, info[1 + n]))
    acc = jax.ShapeDtypeStruct((BLK, width), F32)
    dma = pltpu.SemaphoreType.DMA
    return grid_call(
        near_kernel, 4, info, (h_t, own, sib, x, y, w_q), [VMEM_SPEC] + [ANY_SPEC] * 4 + [cols],
        (jax.ShapeDtypeStruct((width, NB * BLK), F32), acc), (cols, whole_block(acc)),
        [pltpu.VMEM((4, toks, BLK), BF16), dma((4,))], 10_000_000_000, "wq_near")


def run_far(info, h_t, near, sx, sy, d_a, d_b, sd_a, sd_b, w_q, w_k, w_v, x_own, dy_own, gain, acc, gwq):
    width, toks = w_q.shape[0], NB * BLK
    rows, kv = x_own.shape[0], w_k.shape[1]
    cols = pl.BlockSpec((width, BLK), lambda n, info: (0, info[5 + n]))
    outs = (jax.ShapeDtypeStruct((width, NB * BLK), F32), jax.ShapeDtypeStruct((width, kv), F32), jax.ShapeDtypeStruct((width, kv), F32),
            jax.ShapeDtypeStruct((rows, width), BF16), jax.ShapeDtypeStruct((1, width), F32))
    dma = pltpu.SemaphoreType.DMA
    b16 = lambda *shape: pltpu.VMEM(shape, BF16)
    f32 = lambda *shape: pltpu.VMEM(shape, F32)
    return grid_call(
        far_kernel, 4, info,
        (h_t, *near, sx, sy, d_a, d_b, sd_a, sd_b, w_q, w_k, w_v, x_own, dy_own, gain, acc, gwq),
        [VMEM_SPEC] + [ANY_SPEC] * 10 + [cols] + [ANY_SPEC] * 4 + [VMEM_SPEC] + [ANY_SPEC] * 2,
        outs, (cols, ANY_SPEC, ANY_SPEC, whole_block(outs[3]), whole_block(outs[4])),
        [b16(4, toks + 2 * BLK, BLK), b16(4, 2 * BLK, BLK), b16(NB, 2 * BLK, BLK), b16(toks, kv), b16(toks, kv),
         f32(width, kv), f32(width, kv), f32(rows, width), f32(rows, width), b16(width, kv), b16(width, kv), b16(rows, width), b16(rows, width),
         dma((6,)), dma((4,)), dma((7,))],
        15_000_000_000, "wq_far", aliases={19: 0})


def run_gain(part):
    dma = pltpu.SemaphoreType.DMA
    return pl.pallas_call(
        gain_kernel, out_shape=jax.ShapeDtypeStruct(part.shape, F32), in_specs=[VMEM_SPEC], out_specs=VMEM_SPEC,
        scratch_shapes=[pltpu.VMEM((NB,) + part.shape, F32), dma((7,)), dma((7,))],
        compiler_params=pltpu.CompilerParams(collective_id=2, has_side_effects=True), name="gain_sum")(part)


def solution(mesh):
    def device_step(hidden, grad_out, positions, norm_gain, w_q, w_k, w_v, w_o, inv_freq):
        lane = jnp.arange(128)[None, :]
        pos = positions.reshape(2, 128)
        token = jnp.where(lane < 64, pos[0][:, None], pos[1][:, None]).astype(F32)
        angles = token * jnp.tile(inv_freq, 4)[None, :]
        tab = jnp.where(lane % 64 < 32, jnp.cos(angles), jnp.sin(angles))
        gain = norm_gain.astype(F32)[None, :]
        dy_all, h_t, g, ot_all = run_attention(hidden, grad_out, gain, w_q, w_k, w_v, w_o, tab)
        h_t = h_t.reshape(NB, BLK, -1)
        hp, cp, xn, yn, dn = neighbours()
        slots = [head_slot(a, b) for a, b in ((hp, cp), (hp, 1 - cp), (xn, cp), (yn, cp), (xn, 1 - cp), (yn, 1 - cp), (dn, cp), (dn, 1 - cp))]
        info = jnp.stack([tok_slot(hp, cp)] + slots).astype(jnp.int32)
        along_x = lambda a: lax.ppermute(a, 'hp', [(i, i ^ 1) for i in range(4)])
        along_y = lambda a: lax.ppermute(a, 'hp', [(i, i ^ 2) for i in range(4)])
        to_sib = lambda a: lax.ppermute(a, 'cp', [(0, 1), (1, 0)])
        half = g.shape[0] // 2
        x, y, sib = along_x(g), along_y(g), to_sib(g)
        grad_wo, output = run_wo(info, ot_all, dy_all, w_o, hidden)
        x, y, sib, output = lax.optimization_barrier((x, y, sib, output))
        d_a, d_b = along_y(x[:half]), along_x(y[half:])
        sx, sy = to_sib(x), to_sib(y)
        gwq, acc = run_near(info, h_t, g, sib, x, y, w_q)
        d_a, d_b, acc = lax.optimization_barrier((d_a, d_b, acc))
        sd_a, sd_b = to_sib(d_a), to_sib(d_b)
        grad_wq, grad_wk, grad_wv, grad_hidden, part = run_far(
            info, h_t, (g, sib, x, y), sx, sy, d_a, d_b, sd_a, sd_b, w_q, w_k, w_v, hidden, grad_out, gain, acc, gwq)
        grad_gain = run_gain(part)
        return output, grad_hidden, grad_wq, grad_wk, grad_wv, grad_wo, grad_gain[0]

    seq_spec = P(('cp', 'hp'), None)
    whole = P()
    return jax.shard_map(device_step, mesh=mesh, in_specs=(seq_spec, seq_spec, P(('cp', 'hp')), whole, whole, whole, whole, whole, whole), out_specs=(seq_spec, seq_spec, whole, whole, whole, whole, whole), check_vma=False)
```

```python
import functools
import math

import jax
import jax.numpy as jnp
from jax import lax
from jax.experimental import pallas as pl
from jax.experimental.pallas import tpu as pltpu
from jax.sharding import PartitionSpec as P

NORM_EPS = 1e-5
BLK = 256
HEADS = 4
DH = 64
NB = 8
CW = HEADS * BLK
EXP2_SCALE = (DH ** -0.5) * math.log2(math.e)
F32 = jnp.float32
BF16 = jnp.bfloat16


def seq_block(d):
    cp, half, sub = d // 4, (d // 2) % 2, d % 2
    return 2 * ((1 - half) * cp + half * (3 - cp)) + sub


def stored_block(j):
    b, sub = j // 2, j % 2
    half = b // 2
    cp = (1 - half) * b + half * (3 - b)
    return cp * 4 + half * 2 + sub


def nt_dot(a, b):
    return lax.dot_general(a, b, (((1,), (1,)), ((), ())), preferred_element_type=F32)


def dot(a, b):
    return jnp.dot(a, b, preferred_element_type=F32)


def rope_pairs(t, cos_t, sin_t):
    lane = lax.broadcasted_iota(jnp.int32, t.shape, 1)
    partner = jnp.where(lane % DH < DH // 2, pltpu.roll(t, 128 - DH // 2, 1), pltpu.roll(t, DH // 2, 1))
    return t * cos_t + partner * sin_t


def rows_of(b):
    return pl.ds(pl.multiple_of(b * BLK, BLK), BLK)


def key_rows(kb, tiles):
    return pl.ds(pl.multiple_of(kb * tiles * BLK, tiles * BLK), tiles * BLK)


def by_pairs(count, tile, carry):
    carry = lax.fori_loop(0, count // 2, functools.partial(tile, tiles=2), carry)
    return lax.fori_loop(count - count % 2, count, tile, carry)


def causal_tile():
    row = lax.broadcasted_iota(jnp.int32, (BLK, CW), 0)
    col = lax.broadcasted_iota(jnp.int32, (BLK, CW), 1)
    return row <= col % BLK


MESH = pl.DeviceIdType.MESH
CHUNKS = 4


def neighbours():
    hp, cp = lax.axis_index('hp'), lax.axis_index('cp')
    flip = 1 - 2 * (hp % 2)
    y_hp = (hp + 2) % 4
    return hp, cp, hp + flip, y_hp, y_hp + flip


def tok_slot(hp, cp):
    return cp * 4 + hp


def head_slot(hp, cp):
    return hp * 2 + cp


def enter_barrier():
    hp, cp = lax.axis_index('hp'), lax.axis_index('cp')
    barrier = pltpu.get_barrier_semaphore()
    for m in range(1, 8):
        pl.semaphore_signal(barrier, inc=1, device_id=((hp + m // 2) % 4, (cp + m % 2) % 2), device_id_type=MESH)
    pl.semaphore_wait(barrier, 7)


class Gather:
    def __init__(self, src, dst, slot, send, recv, rows):
        self.src, self.dst, self.slot, self.send, self.recv = src, dst, slot, send, recv
        self.step = rows // CHUNKS
        self.hp, self.cp, self.xn, self.yn, self.dn = neighbours()

    def part(self, ref, c):
        return ref.at[pl.ds(c * self.step, self.step)]

    def place(self, hp, cp, c):
        return self.part(self.dst.at[self.slot(hp, cp)], c)

    def copy(self, kind, c):
        hp, cp, xn, yn, dn = self.hp, self.cp, self.xn, self.yn, self.dn
        origin, lands, to = {
            'own_x': (hp, 0, (xn, cp)), 'own_y': (hp, 1, (yn, cp)), 'own_s': (hp, 3, (hp, 1 - cp)),
            'x_s': (xn, 4, (hp, 1 - cp)), 'y_s': (yn, 5, (hp, 1 - cp)), 'd_s': (dn, 6, (hp, 1 - cp)),
            'x_y': (xn, 2, (yn, cp)), 'y_x': (yn, 2, (xn, cp)),
        }[kind]
        number = ('own_x', 'own_y', 'own_s', 'x_s', 'y_s', 'd_s', 'x_y', 'y_x').index(kind)
        src = self.part(self.src, c) if kind.startswith('own') else self.place(origin, cp, c)
        return pltpu.make_async_remote_copy(
            src_ref=src, dst_ref=self.place(origin, cp, c), send_sem=self.send.at[number, c],
            recv_sem=self.recv.at[lands, c], device_id=to, device_id_type=MESH)

    def await_from(self, number, c):
        hp, cp = ((self.xn, self.cp), (self.yn, self.cp), (self.dn, self.cp), (self.hp, 1 - self.cp),
                  (self.xn, 1 - self.cp), (self.yn, 1 - self.cp), (self.dn, 1 - self.cp))[number]
        ref = self.place(hp, cp, c)
        pltpu.make_async_remote_copy(
            src_ref=ref, dst_ref=ref, send_sem=self.send.at[0, c], recv_sem=self.recv.at[number, c],
            device_id=(self.hp, 1 - self.cp), device_id_type=MESH).wait_recv()

    def start_own(self):
        for c in range(CHUNKS):
            for kind in ('own_x', 'own_y', 'own_s'):
                self.copy(kind, c).start()

    def relay_near(self, chunks=range(CHUNKS)):
        for c in chunks:
            self.await_from(0, c)
            self.copy('x_s', c).start()
            if c < CHUNKS // 2:
                self.copy('x_y', c).start()
            self.await_from(1, c)
            self.copy('y_s', c).start()
            if c >= CHUNKS // 2:
                self.copy('y_x', c).start()

    def relay_diagonal(self):
        for c in range(CHUNKS):
            self.await_from(2, c)
            self.copy('d_s', c).start()

    def await_sibling(self, number):
        for c in range(CHUNKS):
            self.await_from(number, c)

    def finish_sends(self):
        for c in range(CHUNKS):
            for kind in ('own_x', 'own_y', 'own_s', 'x_s', 'y_s', 'd_s'):
                self.copy(kind, c).wait_send()
            self.copy('x_y' if c < CHUNKS // 2 else 'y_x', c).wait_send()


def gather_sems():
    return [pltpu.SemaphoreType.DMA((8, CHUNKS)), pltpu.SemaphoreType.DMA((7, CHUNKS))]


def unpack_table(tab):
    group = lax.broadcasted_iota(jnp.int32, tab.shape, 1) // (DH // 2)
    turned = [tab] + [pltpu.roll(tab, 32 * i, 1) for i in (1, 2, 3)]

    def pick(order):
        out = turned[order[3]]
        for g in range(3):
            out = jnp.where(group == g, turned[order[g]], out)
        return out

    sign = jnp.where(group % 2 == 0, -1.0, 1.0)
    cos_t = jnp.concatenate([pick((0, 1, 2, 3)), pick((2, 3, 0, 1))], axis=0)
    sin_t = jnp.concatenate([pick((3, 0, 1, 2)) * sign, pick((1, 2, 3, 0)) * sign], axis=0)
    return cos_t, sin_t


def project_block(d, x, gain, wq_ref, wkv_ref, tab, ht_ref, q_ref, k_ref, v_ref):
    xf = x.astype(F32)
    inv = lax.rsqrt(jnp.mean(xf * xf, axis=-1, keepdims=True) + NORM_EPS)
    h = (xf * inv * gain).astype(BF16)
    ht_ref[:, rows_of(d)] = h.T
    dst = rows_of(seq_block(d))
    cos_t, sin_t = unpack_table(tab)
    y = dot(h, wq_ref[...])
    for p in range(HEADS // 2):
        qr = rope_pairs(y[:, 128 * p:128 * (p + 1)], cos_t, sin_t).astype(BF16)
        q_ref[2 * p, dst, :] = qr[:, :DH]
        q_ref[2 * p + 1, dst, :] = qr[:, DH:]
    kv = dot(h, wkv_ref[...])
    k_ref[dst, :] = rope_pairs(kv, cos_t, sin_t).astype(BF16)[:, :DH]
    v_ref[dst, :] = kv.astype(BF16)[:, DH:]


def attend_block(j, q_ref, k_ref, vt_ref, e_ref, m_ref, ot_ref, lse_ref):
    q4 = q_ref[:, rows_of(j), :].reshape(CW, DH)

    def score_tile(kb, carry, masked, tiles=1):
        m_old, l_old = carry
        keys = key_rows(kb, tiles)
        s = nt_dot(k_ref[keys, :], q4) * EXP2_SCALE
        if masked:
            s = jnp.where(causal_tile(), s, -1e30)
        m_new = jnp.maximum(m_old, jnp.max(s, axis=0, keepdims=True))
        e = jnp.exp2(s - m_new)
        e_ref[keys, :] = e
        for i in range(tiles):
            m_ref[pl.ds(kb * tiles + i, 1), :] = m_new
        return m_new, l_old * jnp.exp2(m_old - m_new) + jnp.sum(e, axis=0, keepdims=True)

    carry = (jnp.full((1, CW), -1e30, F32), jnp.zeros((1, CW), F32))
    carry = score_tile(j, carry, True)
    m_fin, l_fin = by_pairs(j, functools.partial(score_tile, masked=False), carry)
    inv_l = 1.0 / l_fin
    lse = m_fin + jnp.log2(l_fin)

    def out_tile(kb, acc, tiles=1):
        parts = []
        for i in range(tiles):
            f = jnp.exp2(m_ref[pl.ds(kb * tiles + i, 1), :] - m_fin) * inv_l
            parts.append((e_ref[rows_of(kb * tiles + i), :] * f).astype(BF16))
        return acc + dot(vt_ref[:, key_rows(kb, tiles)], jnp.concatenate(parts, axis=0))

    acc = by_pairs(j + 1, out_tile, jnp.zeros((DH, CW), F32)).astype(BF16)
    dst = rows_of(stored_block(j))
    for h in range(HEADS):
        ot_ref[DH * h:DH * (h + 1), dst] = acc[:, BLK * h:BLK * (h + 1)]
        lse_ref[h:h + 1, rows_of(j)] = lse[:, BLK * h:BLK * (h + 1)]


def nth_peer(e):
    hp, cp = lax.axis_index('hp'), lax.axis_index('cp')
    m, b = e // 2, e % 2
    px = (hp % 2 + m % 2) % 2
    py = (hp // 2 + m // 2) % 2
    return py * 2 + px, (cp + b) % 2


def attention_kernel(x_own, dy_own, gain_ref, wq_hbm, wk_hbm, wv_hbm, wo_hbm, tab_own,
                     dy_all, ht_out, gq_ref, ot_all,
                     xg, ht, e_ref, m_ref, vt_ref, wq, wk, wv, wkv, stage, q_ref, k_ref, v_ref, ot_ref, lse_ref, tabs,
                     wo, wot, do_ref, kt_ref, dk_ref, dv_ref, give, take,
                     local_sem, dy_sem, t_send, t_recv, x_send, x_recv, dy_send, dy_recv, o_send, o_recv, pair_send, pair_recv):
    hp, cp, xn, yn, dn = neighbours()
    mine = tok_slot(hp, cp)
    hw = HEADS * DH
    loads = [
        pltpu.make_async_copy(x_own, xg.at[mine], local_sem.at[0]),
        pltpu.make_async_copy(wq_hbm.at[:, pl.ds(pl.multiple_of(head_slot(hp, cp) * hw, hw), hw)], wq, local_sem.at[1]),
        pltpu.make_async_copy(wk_hbm.at[:, pl.ds(pl.multiple_of((hp // 2) * 128, 128), 128)], wk, local_sem.at[2]),
        pltpu.make_async_copy(wv_hbm.at[:, pl.ds(pl.multiple_of((hp // 2) * 128, 128), 128)], wv, local_sem.at[3]),
        pltpu.make_async_copy(dy_own, stage, local_sem.at[4]),
        pltpu.make_async_copy(tab_own, tabs.at[mine], local_sem.at[5]),
    ]
    for load in loads:
        load.start()
    wo_load = pltpu.make_async_copy(wo_hbm.at[pl.ds(pl.multiple_of(head_slot(hp, cp) * hw, hw), hw)], wo, local_sem.at[8])
    wo_load.start()
    enter_barrier()
    gx = Gather(x_own, xg, tok_slot, x_send, x_recv, BLK)
    gdy = Gather(dy_own, dy_all, tok_slot, dy_send, dy_recv, BLK)

    gt = Gather(tab_own, tabs, tok_slot, t_send, t_recv, 128)
    gt.start_own()
    gx.start_own()
    for load in loads[1:4]:
        load.wait()
    lane = lax.broadcasted_iota(jnp.int32, wk.shape, 1)
    swap = hp % 2 == 1
    kf, vf = wk[...].astype(F32), wv[...].astype(F32)
    k_sel = jnp.where(swap, pltpu.roll(kf, DH, 1), kf)
    v_sel = jnp.where(swap, vf, pltpu.roll(vf, DH, 1))
    wkv[...] = jnp.where(lane < DH, k_sel, v_sel).astype(BF16)
    wo_load.wait()
    wot[...] = wo[...].T
    for i in (0, 4, 5):
        loads[i].wait()
    dy_mine = pltpu.make_async_copy(stage, dy_all.at[mine], local_sem.at[6])
    dy_mine.start()
    def project(e, _):
        @pl.when(e == 1)
        def _():
            gt.await_sibling(3)
            gx.await_sibling(3)

        @pl.when(e == 2)
        def _():
            gt.relay_near()
            gx.relay_near()
            gdy.start_own()

        @pl.when(e == 3)
        def _():
            gt.await_sibling(4)
            gx.await_sibling(4)

        @pl.when(e == 5)
        def _():
            gt.await_sibling(5)
            gx.await_sibling(5)

        @pl.when(e == 6)
        def _():
            gt.relay_diagonal()
            gx.relay_diagonal()

        @pl.when(e == 7)
        def _():
            gt.await_sibling(6)
            gx.await_sibling(6)

        d = tok_slot(*nth_peer(e))
        project_block(d, xg[d], gain_ref[...].astype(F32), wq, wkv, tabs[d], ht, q_ref, k_ref, v_ref)
        return 0

    lax.fori_loop(0, NB, project, 0)
    ht_copy = pltpu.make_async_copy(ht, ht_out, local_sem.at[7])
    ht_copy.start()
    vt_ref[...] = v_ref[...].T

    def attend(j, _):
        for c in range(CHUNKS):
            @pl.when(j == (2, 4, 6, 7)[c])
            def _():
                gdy.relay_near((c,))

        attend_block(j, q_ref, k_ref, vt_ref, e_ref, m_ref, ot_ref, lse_ref)
        return 0

    lax.fori_loop(0, NB, attend, 0)
    go = Gather(ot_ref, ot_all, head_slot, o_send, o_recv, hw)
    kt_ref[...] = k_ref[...].T
    dk_ref[...] = jnp.zeros_like(dk_ref)
    dv_ref[...] = jnp.zeros_like(dv_ref)
    go.start_own()
    ot_mine = pltpu.make_async_copy(ot_ref, ot_all.at[head_slot(hp, cp)], local_sem.at[9])
    ot_mine.start()
    gx.finish_sends()
    dy_mine.wait()

    def dy_load(e):
        d = tok_slot(*nth_peer(e))
        return pltpu.make_async_copy(dy_all.at[d], xg.at[d], dy_sem.at[e])

    def project_dy(e, _):
        dy_load(e).wait()
        d = tok_slot(*nth_peer(e))
        do = dot(xg[d], wot[...]).astype(BF16)
        dst = rows_of(seq_block(d))
        for h in range(HEADS):
            do_ref[h, dst, :] = do[:, DH * h:DH * (h + 1)]
        return 0

    for number in (3, 4, 5):
        gdy.await_sibling(number)
    for e in range(6):
        dy_load(e).start()
    lax.fori_loop(0, 6, project_dy, 0)
    gdy.relay_diagonal()
    dy_load(6).start()
    gdy.await_sibling(6)
    dy_load(7).start()
    lax.fori_loop(6, NB, project_dy, 0)

    def attend_back(j, _):
        for c in range(CHUNKS):
            @pl.when(j == (2, 4, 5, 6)[c])
            def _():
                go.relay_near((c,))

        slot = stored_block(j)
        src = rows_of(slot)
        q4 = q_ref[:, rows_of(j), :].reshape(CW, DH)
        do4 = do_ref[:, rows_of(j), :].reshape(CW, DH)
        o4t = jnp.concatenate([ot_ref[DH * h:DH * (h + 1), src] for h in range(HEADS)], axis=1)
        lse = jnp.concatenate([lse_ref[h:h + 1, rows_of(j)] for h in range(HEADS)], axis=1)
        delta = jnp.sum(do4.astype(F32).T * o4t.astype(F32), axis=0, keepdims=True)

        def tile(kb, dqt, masked, tiles=1):
            keys = key_rows(kb, tiles)
            p = jnp.exp2(nt_dot(k_ref[keys, :], q4) * EXP2_SCALE - lse)
            if masked:
                p = jnp.where(causal_tile(), p, 0.0)
            dp = nt_dot(v_ref[keys, :], do4)
            dv_ref[keys, :] += dot(p.astype(BF16), do4)
            ds = (p * (dp - delta)).astype(BF16)
            dk_ref[keys, :] += dot(ds, q4)
            return dqt + dot(kt_ref[:, keys], ds)

        dqt = tile(j, jnp.zeros((DH, CW), F32), True)
        dqt = by_pairs(j, functools.partial(tile, masked=False), dqt) * (DH ** -0.5)
        cos_t, sin_t = unpack_table(tabs[slot])
        for p in range(HEADS // 2):
            pair = jnp.concatenate([dqt[:, BLK * (2 * p):BLK * (2 * p + 1)], dqt[:, BLK * (2 * p + 1):BLK * (2 * p + 2)]], axis=0)
            dq = pair.T.astype(BF16).astype(F32)
            gq_ref[src, 128 * p:128 * (p + 1)] = rope_pairs(dq, cos_t, -sin_t).astype(BF16)
        return 0

    lax.fori_loop(0, NB, attend_back, 0)
    give[:, :DH] = (dk_ref[...] * (DH ** -0.5)).astype(BF16)
    give[:, DH:] = dv_ref[...].astype(BF16)
    swap = pltpu.make_async_remote_copy(
        src_ref=give, dst_ref=take, send_sem=pair_send, recv_sem=pair_recv, device_id=(hp, 1 - cp), device_id_type=MESH)
    go.relay_diagonal()
    swap.start()
    for number in (3, 4, 5):
        go.await_sibling(number)
    swap.wait_recv()
    lane = lax.broadcasted_iota(jnp.int32, (BLK, 2 * DH), 1)
    for i in range(NB // 2):
        slot = cp * 4 + i
        src = rows_of(seq_block(slot))
        total = (give[src, :].astype(F32) + take[src, :].astype(F32)).astype(BF16).astype(F32)
        cos_t, sin_t = unpack_table(tabs[slot])
        turned = rope_pairs(total, cos_t, -sin_t)
        gq_ref[NB * BLK + (i % 2) * BLK:NB * BLK + (i % 2 + 1) * BLK, 128 * (i // 2):128 * (i // 2 + 1)] = jnp.where(lane < DH, turned, total).astype(BF16)
    go.await_sibling(6)
    swap.wait_send()
    go.finish_sends()
    ot_mine.wait()
    gt.finish_sends()
    gdy.finish_sends()
    ht_copy.wait()


def flat(a_ref):
    return a_ref[...].reshape(NB * BLK, NB * BLK)


def wo_kernel(info, ot_ref, dy_ref, wo_ref, x_ref, gwo_ref, out_ref, o_mine):
    @pl.when(pl.program_id(0) == 0)
    def _():
        for d in range(NB):
            o_mine[:, BLK * d:BLK * (d + 1)] = ot_ref[d, :, rows_of(info[0])].T

    gwo_ref[...] = dot(flat(ot_ref), dy_ref[...].reshape(NB * BLK, BLK))
    out_ref[...] = (x_ref[...].astype(F32) + dot(o_mine[...], wo_ref[...])).astype(BF16)


def near_kernel(info, ht_ref, own_hbm, sib_hbm, x_hbm, y_hbm, wq_ref, gwq_ref, acc_ref, g_ref, g_sem):
    e = pl.program_id(0)
    toks = NB * BLK
    fetch = [pltpu.make_async_copy(src.at[pl.ds(0, toks)], g_ref.at[i], g_sem.at[i]) for i, src in enumerate((own_hbm, sib_hbm, x_hbm, y_hbm))]

    @pl.when(e == 0)
    def _():
        for load in fetch:
            load.start()

    for i in range(4):
        @pl.when(e == i)
        def _():
            fetch[i].wait()

    g = g_ref.at[e]
    gwq_ref[...] = dot(flat(ht_ref), g[...])
    part = nt_dot(g[rows_of(info[0]), :], wq_ref[...])

    @pl.when(e == 0)
    def _():
        acc_ref[...] = part

    @pl.when(e > 0)
    def _():
        acc_ref[...] += part


def far_kernel(info, ht_ref, own_hbm, sib_hbm, x_hbm, y_hbm, sx_hbm, sy_hbm, da_hbm, db_hbm, sda_hbm, sdb_hbm,
               wq_ref, wk_hbm, wv_hbm, x_hbm_own, dy_hbm_own, gain_ref, acc_hbm, gwq_in,
               gwq_ref, gwk_hbm, gwv_hbm, gh_ref, gg_ref,
               g_ref, kv4, gkvg, bk, bv, gwk, gwv, acc, acc_in, wk, wv, x_own, dy_own, g_sem, kv_sem, late_sem):
    e = pl.program_id(0)
    toks = NB * BLK
    half = da_hbm.shape[0]
    copy = pltpu.make_async_copy
    lo, hi = pl.ds(0, half), pl.ds(half, half)
    fetch = ((copy(sx_hbm, g_ref.at[0], g_sem.at[0]),), (copy(sy_hbm, g_ref.at[1], g_sem.at[1]),),
             (copy(da_hbm, g_ref.at[2, lo], g_sem.at[2]), copy(db_hbm, g_ref.at[2, hi], g_sem.at[3])),
             (copy(sda_hbm, g_ref.at[3, lo], g_sem.at[4]), copy(sdb_hbm, g_ref.at[3, hi], g_sem.at[5])))
    near_kv = [copy(src.at[pl.ds(toks, 2 * BLK)], kv4.at[i], kv_sem.at[i]) for i, src in enumerate((own_hbm, sib_hbm, x_hbm, y_hbm))]
    late = [copy(src, dst, late_sem.at[i]) for i, (src, dst) in enumerate(
        ((acc_hbm, acc_in), (wk_hbm, wk), (wv_hbm, wv), (x_hbm_own, x_own), (dy_hbm_own, dy_own)))]
    give = [copy(gwk, gwk_hbm, late_sem.at[5]), copy(gwv, gwv_hbm, late_sem.at[6])]

    @pl.when(e == 0)
    def _():
        fetch[0][0].start()
        for load in [c for group in fetch[1:] for c in group] + near_kv + late:
            load.start()
        fetch[0][0].wait()

    @pl.when(e == 1)
    def _():
        for load in [c for group in fetch[1:] for c in group] + near_kv:
            load.wait()
        for i in range(4):
            gkvg[info[1 + i]] = kv4[i]
            gkvg[info[5 + i]] = g_ref[i, toks:, :]
        for c in range(2):
            for r in range(2):
                dst = pl.ds((c * 2 + r) * 2 * BLK, 2 * BLK)
                for p in range(2):
                    even = gkvg[4 * p + c, :, 128 * r:128 * (r + 1)]
                    odd = gkvg[4 * p + 2 + c, :, 128 * r:128 * (r + 1)]
                    bk[dst, 128 * p:128 * (p + 1)] = jnp.concatenate([even[:, :DH], odd[:, :DH]], axis=1)
                    bv[dst, 128 * p:128 * (p + 1)] = jnp.concatenate([even[:, DH:], odd[:, DH:]], axis=1)
        gwk[...] = dot(flat(ht_ref), bk[...])
        gwv[...] = dot(flat(ht_ref), bv[...])
        for out in give:
            out.start()

    g = g_ref.at[e]
    part = nt_dot(g[rows_of(info[0]), :], wq_ref[...])

    @pl.when(e == 0)
    def _():
        acc[...] = part

    @pl.when(e > 0)
    def _():
        acc[...] += part

    gwq_ref[...] = dot(flat(ht_ref), g[:toks, :])

    @pl.when(e == 3)
    def _():
        for load in late:
            load.wait()
        mine = rows_of(info[0])
        d_norm = acc[...] + acc_in[...] + nt_dot(bk[mine, :], wk[...]) + nt_dot(bv[mine, :], wv[...])
        x = x_own[...].astype(F32)
        inv = lax.rsqrt(jnp.mean(x * x, axis=-1, keepdims=True) + NORM_EPS)
        x_hat = x * inv
        gg_ref[...] = jnp.sum(d_norm * x_hat, axis=0, keepdims=True)
        d_hat = d_norm * gain_ref[...].astype(F32)
        row_mean = jnp.mean(d_hat * x_hat, axis=-1, keepdims=True)
        gh_ref[...] = (dy_own[...].astype(F32) + inv * (d_hat - x_hat * row_mean)).astype(BF16)
        for out in give:
            out.wait()


def gain_kernel(part_ref, gg_ref, gains, send, recv):
    hp, cp = lax.axis_index('hp'), lax.axis_index('cp')
    mine = tok_slot(hp, cp)
    enter_barrier()

    def gain_copy(m):
        return pltpu.make_async_remote_copy(
            src_ref=part_ref, dst_ref=gains.at[mine], send_sem=send.at[m - 1], recv_sem=recv.at[m - 1],
            device_id=((hp + m // 2) % 4, (cp + m % 2) % 2), device_id_type=MESH)

    for m in range(1, NB):
        gain_copy(m).start()
    gains[mine] = part_ref[...]
    for m in range(1, NB):
        ref = gains.at[tok_slot((hp + 4 - m // 2) % 4, (cp + m % 2) % 2)]
        pltpu.make_async_remote_copy(
            src_ref=ref, dst_ref=ref, send_sem=send.at[m - 1], recv_sem=recv.at[m - 1],
            device_id=(hp, 1 - cp), device_id_type=MESH).wait_recv()
    total = gains[0]
    for d in range(1, NB):
        total = total + gains[d]
    gg_ref[...] = total
    for m in range(1, NB):
        gain_copy(m).wait_send()


VMEM_SPEC = pl.BlockSpec(memory_space=pltpu.VMEM)
ANY_SPEC = pl.BlockSpec(memory_space=pl.ANY)


def run_attention(x_own, dy_own, gain, w_q, w_k, w_v, w_o, tab):
    rows, width = x_own.shape
    toks = rows * NB
    hw = HEADS * DH
    dma = pltpu.SemaphoreType.DMA
    b16 = lambda *shape: pltpu.VMEM(shape, BF16)
    f32 = lambda *shape: pltpu.VMEM(shape, F32)
    return pl.pallas_call(
        attention_kernel,
        out_shape=(
            jax.ShapeDtypeStruct((NB, rows, width), BF16),
            jax.ShapeDtypeStruct((width, toks), BF16),
            jax.ShapeDtypeStruct((toks + 2 * BLK, hw), BF16),
            jax.ShapeDtypeStruct((NB, hw, toks), BF16),
        ),
        in_specs=[ANY_SPEC, ANY_SPEC, VMEM_SPEC] + [ANY_SPEC] * 5,
        out_specs=(ANY_SPEC, ANY_SPEC, VMEM_SPEC, ANY_SPEC),
        scratch_shapes=[
            b16(NB, rows, width), b16(width, toks), f32(toks, CW), f32(NB, CW), b16(DH, toks),
            b16(width, hw), b16(width, 128), b16(width, 128), b16(width, 128), b16(rows, width),
            b16(HEADS, toks, DH), b16(toks, DH), b16(toks, DH), b16(hw, toks), f32(HEADS, toks), f32(NB, 128, 128),
            b16(hw, width), b16(width, hw), b16(HEADS, toks, DH), b16(DH, toks), f32(toks, DH), f32(toks, DH), b16(toks, 2 * DH), b16(toks, 2 * DH),
            dma((10,)), dma((NB,)),
        ] + gather_sems() * 4 + [dma, dma],
        compiler_params=pltpu.CompilerParams(vmem_limit_bytes=60 * 1024 * 1024, collective_id=0, has_side_effects=True),
        cost_estimate=pl.CostEstimate(flops=70_000_000_000, bytes_accessed=40_000_000, transcendentals=0),
        name="attention",
    )(x_own, dy_own, gain, w_q, w_k, w_v, w_o, tab)


def grid_call(kernel, steps, info, args, in_specs, out_shape, out_specs, scratch, flops, name, aliases=None):
    return pl.pallas_call(
        kernel,
        out_shape=out_shape,
        grid_spec=pltpu.PrefetchScalarGridSpec(
            num_scalar_prefetch=1, grid=(steps,), in_specs=in_specs, out_specs=out_specs, scratch_shapes=scratch),
        input_output_aliases=aliases or {},
        compiler_params=pltpu.CompilerParams(vmem_limit_bytes=60 * 1024 * 1024),
        cost_estimate=pl.CostEstimate(flops=flops, bytes_accessed=40_000_000, transcendentals=0),
        name=name,
    )(info, *args)


def whole_block(a):
    return pl.BlockSpec(a.shape, lambda n, info: (0,) * len(a.shape))


def run_wo(info, ot_all, dy_all, w_o, x_own):
    rows, width = x_own.shape
    hw = HEADS * DH
    cols = lambda r: pl.BlockSpec((r, BLK), lambda n, info: (0, n))
    return grid_call(
        wo_kernel, NB, info, (ot_all, dy_all, w_o, x_own),
        [VMEM_SPEC, pl.BlockSpec((NB, rows, BLK), lambda n, info: (0, 0, n)), cols(NB * hw), cols(rows)],
        (jax.ShapeDtypeStruct((NB * hw, width), F32), jax.ShapeDtypeStruct((rows, width), BF16)),
        (cols(NB * hw), cols(rows)),
        [pltpu.VMEM((rows, NB * hw), BF16)], 20_000_000_000, "wo_grad")


def run_near(info, h_t, own, sib, x, y, w_q):
    width, toks = w_q.shape[0], NB * BLK
    cols = pl.BlockSpec((width, BLK), lambda n, info: (0, info[1 + n]))
    acc = jax.ShapeDtypeStruct((BLK, width), F32)
    dma = pltpu.SemaphoreType.DMA
    return grid_call(
        near_kernel, 4, info, (h_t, own, sib, x, y, w_q), [VMEM_SPEC] + [ANY_SPEC] * 4 + [cols],
        (jax.ShapeDtypeStruct((width, NB * BLK), F32), acc), (cols, whole_block(acc)),
        [pltpu.VMEM((4, toks, BLK), BF16), dma((4,))], 10_000_000_000, "wq_near")


def run_far(info, h_t, near, sx, sy, d_a, d_b, sd_a, sd_b, w_q, w_k, w_v, x_own, dy_own, gain, acc, gwq):
    width, toks = w_q.shape[0], NB * BLK
    rows, kv = x_own.shape[0], w_k.shape[1]
    cols = pl.BlockSpec((width, BLK), lambda n, info: (0, info[5 + n]))
    outs = (jax.ShapeDtypeStruct((width, NB * BLK), F32), jax.ShapeDtypeStruct((width, kv), F32), jax.ShapeDtypeStruct((width, kv), F32),
            jax.ShapeDtypeStruct((rows, width), BF16), jax.ShapeDtypeStruct((1, width), F32))
    dma = pltpu.SemaphoreType.DMA
    b16 = lambda *shape: pltpu.VMEM(shape, BF16)
    f32 = lambda *shape: pltpu.VMEM(shape, F32)
    return grid_call(
        far_kernel, 4, info,
        (h_t, *near, sx, sy, d_a, d_b, sd_a, sd_b, w_q, w_k, w_v, x_own, dy_own, gain, acc, gwq),
        [VMEM_SPEC] + [ANY_SPEC] * 10 + [cols] + [ANY_SPEC] * 4 + [VMEM_SPEC] + [ANY_SPEC] * 2,
        outs, (cols, ANY_SPEC, ANY_SPEC, whole_block(outs[3]), whole_block(outs[4])),
        [b16(4, toks + 2 * BLK, BLK), b16(4, 2 * BLK, BLK), b16(NB, 2 * BLK, BLK), b16(toks, kv), b16(toks, kv),
         f32(width, kv), f32(width, kv), f32(rows, width), f32(rows, width), b16(width, kv), b16(width, kv), b16(rows, width), b16(rows, width),
         dma((6,)), dma((4,)), dma((7,))],
        15_000_000_000, "wq_far", aliases={19: 0})


def run_gain(part):
    dma = pltpu.SemaphoreType.DMA
    return pl.pallas_call(
        gain_kernel, out_shape=jax.ShapeDtypeStruct(part.shape, F32), in_specs=[VMEM_SPEC], out_specs=VMEM_SPEC,
        scratch_shapes=[pltpu.VMEM((NB,) + part.shape, F32), dma((7,)), dma((7,))],
        compiler_params=pltpu.CompilerParams(collective_id=2, has_side_effects=True), name="gain_sum")(part)


def solution(mesh):
    def device_step(hidden, grad_out, positions, norm_gain, w_q, w_k, w_v, w_o, inv_freq):
        lane = jnp.arange(128)[None, :]
        pos = positions.reshape(2, 128)
        token = jnp.where(lane < 64, pos[0][:, None], pos[1][:, None]).astype(F32)
        angles = token * jnp.tile(inv_freq, 4)[None, :]
        tab = jnp.where(lane % 64 < 32, jnp.cos(angles), jnp.sin(angles))
        gain = norm_gain[None, :]
        dy_all, h_t, g, ot_all = run_attention(hidden, grad_out, gain, w_q, w_k, w_v, w_o, tab)
        h_t = h_t.reshape(NB, BLK, -1)
        hp, cp, xn, yn, dn = neighbours()
        slots = [head_slot(a, b) for a, b in ((hp, cp), (hp, 1 - cp), (xn, cp), (yn, cp), (xn, 1 - cp), (yn, 1 - cp), (dn, cp), (dn, 1 - cp))]
        info = jnp.stack([tok_slot(hp, cp)] + slots).astype(jnp.int32)
        along_x = lambda a: lax.ppermute(a, 'hp', [(i, i ^ 1) for i in range(4)])
        along_y = lambda a: lax.ppermute(a, 'hp', [(i, i ^ 2) for i in range(4)])
        to_sib = lambda a: lax.ppermute(a, 'cp', [(0, 1), (1, 0)])
        half = g.shape[0] // 2
        x, y, sib = along_x(g), along_y(g), to_sib(g)
        grad_wo, output = run_wo(info, ot_all, dy_all, w_o, hidden)
        x, y, sib, output = lax.optimization_barrier((x, y, sib, output))
        d_a, d_b = along_y(x[:half]), along_x(y[half:])
        sx, sy = to_sib(x), to_sib(y)
        gwq, acc = run_near(info, h_t, g, sib, x, y, w_q)
        d_a, d_b, acc = lax.optimization_barrier((d_a, d_b, acc))
        sd_a, sd_b = to_sib(d_a), to_sib(d_b)
        grad_wq, grad_wk, grad_wv, grad_hidden, part = run_far(
            info, h_t, (g, sib, x, y), sx, sy, d_a, d_b, sd_a, sd_b, w_q, w_k, w_v, hidden, grad_out, gain, acc, gwq)
        grad_gain = run_gain(part)
        return output, grad_hidden, grad_wq, grad_wk, grad_wv, grad_wo, grad_gain[0]

    seq_spec = P(('cp', 'hp'), None)
    whole = P()
    return jax.shard_map(device_step, mesh=mesh, in_specs=(seq_spec, seq_spec, P(('cp', 'hp')), whole, whole, whole, whole, whole, whole), out_specs=(seq_spec, seq_spec, whole, whole, whole, whole, whole), check_vma=False)
```
